32 devices in a mesh: dp: 8 (over z, x), tensor: 4 (over y, core).
Axes of the slice: x: 2, y: 2, z: 4, core: 2. Of those that a mesh axis runs over, the one named last changes fastest.
Arguments:
- tokens: bfloat16 [2, 8, 1024, 1024], P(None, 'dp', 'tensor'), may hold values from -6 to 6
- segment_ids: int32 [2, 8, 1024], P(None, 'dp'), may hold values from 0 to 2, as said below
- attn_gain: float32 [1024], replicated, may hold values from 0.1 to 1.9
- query_gain: float32 [64], replicated, may hold values from 0.1 to 1.9
- key_gain: float32 [64], replicated, may hold values from 0.1 to 1.9
- w_query: bfloat16 [1024, 1024], P('dp', 'tensor'), may hold values from -0.1875 to 0.1875
- w_key: bfloat16 [1024, 512], P('dp', 'tensor'), may hold values from -0.1875 to 0.1875
- w_value: bfloat16 [1024, 512], P('dp', 'tensor'), may hold values from -0.1875 to 0.1875
- w_out: bfloat16 [1024, 1024], P('tensor', 'dp'), may hold values from -1.5 to 1.5
- ffn_gain: float32 [1024], replicated, may hold values from 0.1 to 1.9
- w_gate: bfloat16 [1024, 4608], P('dp', 'tensor'), may hold values from -0.1875 to 0.1875
- w_up: bfloat16 [1024, 4608], P('dp', 'tensor'), may hold values from -0.1875 to 0.1875
- w_down: bfloat16 [4608, 1024], P('tensor', 'dp'), may hold values from -0.09375 to 0.09375
- cotangent: bfloat16 [2, 8, 1024, 1024], P(None, 'dp', 'tensor'), may hold values from -6 to 6
Outputs:
- mixed: bfloat16 [2, 8, 1024, 1024], P(None, 'dp', 'tensor')
- grad_tokens: float32 [2, 8, 1024, 1024], P(None, 'dp', 'tensor')
- grad_attn_gain: float32 [1024], replicated
- grad_query_gain: float32 [64], replicated
- grad_key_gain: float32 [64], replicated
- grad_query: float32 [1024, 1024], P('dp', 'tensor')
- grad_key: float32 [1024, 512], P('dp', 'tensor')
- grad_value: float32 [1024, 512], P('dp', 'tensor')
- grad_out: float32 [1024, 1024], P('tensor', 'dp')
- grad_ffn_gain: float32 [1024], replicated
- grad_gate: float32 [1024, 4608], P('dp', 'tensor')
- grad_up: float32 [1024, 4608], P('dp', 'tensor')
- grad_down: float32 [4608, 1024], P('tensor', 'dp')
The draws below stay inside these ranges and needn't reach their ends.
Inputs may be any that keep to these rules, and one draw needn't show every extreme that they name: `segment_ids`: ids never fall along a sequence and every sequence holds documents 0, 1 and 2; document 0 has 204 to 408 tokens, document 1 has 204 to 511 tokens.
All inputs are finite; a program needn't handle non-finite values.
Results may differ from the reference program's by a relative error of at most 0.017.
Values may be sent and summed in bfloat16 or wider, within the bound.
A program may use at most 112 MiB of HBM per device.

```python
import jax
import jax.numpy as jnp
from jax import lax

D = 1024
H = 16
KV = 8
DH = 64
FF = 4608
LEN = 1024
MICRO = 2
SEQS = 8


def draw_segment_ids(key, part):
    first_key = jax.random.fold_in(key, 11)
    second_key = jax.random.fold_in(key, 12)
    first_end = jax.random.randint(first_key, (MICRO, SEQS, 1), LEN // 5, 2 * LEN // 5)
    second_end = first_end + jax.random.randint(second_key, (MICRO, SEQS, 1), LEN // 5, LEN // 2)
    positions = jnp.arange(LEN, dtype=jnp.int32)[None, None, :]
    return (positions >= first_end).astype(jnp.int32) + (positions >= second_end).astype(jnp.int32)


def spiked(values, own_key, source, target, blocks, factor):
    def block_of(position):
        return (jnp.arange(values.shape[position]) // (values.shape[position] // blocks)).reshape((-1,) + (1,) * (values.ndim - 1 - position))

    near = jax.random.permutation(own_key, blocks)[block_of(target)]
    far = (block_of(target) + blocks // 2) % blocks
    return jnp.where((block_of(source) == near) | (block_of(source) == far), factor * values, values)


def shard_levels(own_key, dims, shards, low, largest):
    def one(axis_at, blocks):
        heights = jax.random.uniform(jax.random.fold_in(jax.random.fold_in(own_key, 6), axis_at), (blocks,), jnp.float32, low / len(shards), largest / len(shards))
        return jnp.repeat(jnp.exp(heights), dims[axis_at] // blocks).reshape((-1,) + (1,) * (len(dims) - axis_at - 1))

    gain = one(*shards[0])
    for cut in shards[1:]:
        gain = gain * one(*cut)
    return gain


def scatter_about(key, dims, scale, bound, shards=(), kind=jnp.bfloat16):
    array = jax.random.normal(key, dims, jnp.float32) * scale
    if len(shards) > 0:
        array = shard_levels(key, dims, shards, -0.22, 0.18) * array
    return jnp.clip(array, min=-bound, max=bound).astype(kind)


def heavy_noise(stream_key, extent, scale, limit, shards, heavy, kind=jnp.bfloat16):
    values = scale * jax.random.normal(stream_key, extent, jnp.float32)
    if shards:
        values = values * shard_levels(stream_key, extent, shards, -0.22, 0.18)
    return jnp.clip(spiked(values, jax.random.fold_in(stream_key, 3), *heavy), -limit, limit).astype(kind)


def setup_inputs(seed: int = 0) -> dict:
    arg_keys = jax.random.split(jax.random.key(seed), 15)
    tokens = heavy_noise(arg_keys[0], (MICRO, SEQS, LEN, D), 1.0, 6.0, ((1, 8), (2, 4)), (1, 3, 8, 2.0))
    segment_ids = draw_segment_ids(jax.random.fold_in(arg_keys[14], 71), 0)
    attn_gain = jnp.clip(1.0 + 0.18 * jax.random.normal(arg_keys[2], (D,), jnp.float32), 0.1, 1.9)
    query_gain = jnp.clip(1.0 + 0.18 * jax.random.normal(arg_keys[3], (DH,), jnp.float32), 0.1, 1.9)
    key_gain = jnp.clip(1.0 + 0.18 * jax.random.normal(arg_keys[4], (DH,), jnp.float32), 0.1, 1.9)
    w_query = scatter_about(arg_keys[5], (D, H * DH), D ** -0.5, 0.1875, ((0, 8), (1, 4)))
    w_key = scatter_about(arg_keys[6], (D, KV * DH), D ** -0.5, 0.1875, ((0, 8), (1, 4)))
    w_value = scatter_about(arg_keys[7], (D, KV * DH), D ** -0.5, 0.1875, ((0, 8), (1, 4)))
    w_out = scatter_about(arg_keys[8], (H * DH, D), (H * DH // 64) ** -0.5, 1.5, ((0, 4), (1, 8)))
    ffn_gain = jnp.clip(1.0 + 0.18 * jax.random.normal(arg_keys[9], (D,), jnp.float32), 0.1, 1.9)
    w_gate = scatter_about(arg_keys[10], (D, FF), D ** -0.5, 0.1875, ((0, 8), (1, 4)))
    w_up = scatter_about(arg_keys[11], (D, FF), D ** -0.5, 0.1875, ((0, 8), (1, 4)))
    w_down = scatter_about(arg_keys[12], (FF, D), FF ** -0.5, 0.09375, ((0, 4), (1, 8)))
    cotangent = scatter_about(arg_keys[13], (MICRO, SEQS, LEN, D), 1.0, 6.0, ((1, 8), (2, 4)))
    return {"tokens": tokens, "segment_ids": segment_ids, "attn_gain": attn_gain, "query_gain": query_gain, "key_gain": key_gain, "w_query": w_query, "w_key": w_key, "w_value": w_value, "w_out": w_out, "ffn_gain": ffn_gain, "w_gate": w_gate, "w_up": w_up, "w_down": w_down, "cotangent": cotangent}


NORM_EPS = 1e-05
ROPE_BASE = 1000000.0
PRECISE = lax.Precision.HIGHEST

@jax.custom_vjp
def low(v):
    return lax.optimization_barrier(v.astype(jnp.bfloat16)).astype(jnp.float32)

@jax.custom_vjp
def low_back(v):
    return v

def low_keep(v):
    return (low(v), None)

def low_pass(kept, grad):
    return (grad,)

def back_keep(v):
    return (v, None)

def back_low(kept, grad):
    return (low(grad),)
low.defvjp(low_keep, low_pass)
low_back.defvjp(back_keep, back_low)

def rms_scale(values, gain_vector):
    inverse = lax.rsqrt(lax.optimization_barrier(jnp.mean(values * values, axis=-1, keepdims=True)) + NORM_EPS)
    return values * inverse * gain_vector

def rope_tables(length, head_width):
    freq_index = jnp.arange(head_width // 2, dtype=jnp.float32)
    inverse_freq = ROPE_BASE ** (-2.0 * freq_index / head_width)
    angles = jnp.arange(length, dtype=jnp.float32)[:, None] * inverse_freq[None, :]
    return (jnp.cos(angles), jnp.sin(angles))

def rotate(values, cosine_table, sine_table):
    half_width = values.shape[-1] // 2
    front_half = values[..., :half_width]
    back_half = values[..., half_width:]
    return jnp.concatenate([front_half * cosine_table - back_half * sine_table, back_half * cosine_table + front_half * sine_table], axis=-1)

def layer(rows_in, segments, params):
    attn_gain, query_gain, key_gain, w_query, w_key, w_value, w_out, ffn_gain, w_gate, w_up, w_down = params
    length = rows_in.shape[0]
    normed = low(rms_scale(rows_in, attn_gain))
    query_proj = low_back(jnp.dot(normed, w_query, precision=PRECISE))
    key_proj = low_back(jnp.dot(normed, w_key, precision=PRECISE))
    value_low = low(low_back(jnp.dot(normed, w_value, precision=PRECISE)))
    cosine_table, sine_table = rope_tables(length, DH)
    query_heads = query_proj.reshape(length, H, DH).transpose(1, 0, 2)
    key_heads = key_proj.reshape(length, KV, DH).transpose(1, 0, 2)
    value_heads = value_low.reshape(length, KV, DH).transpose(1, 0, 2)
    query_rot = low(rotate(rms_scale(query_heads, query_gain), cosine_table, sine_table) * DH ** (-0.5))
    key_rot = low(rotate(rms_scale(key_heads, key_gain), cosine_table, sine_table))
    key_repeat = jnp.repeat(key_rot, H // KV, axis=0)
    value_repeat = jnp.repeat(value_heads, H // KV, axis=0)
    scores = low_back(jnp.einsum('hqd,hkd->hqk', query_rot, key_repeat, precision=PRECISE))
    positions = jnp.arange(length)
    allowed = (positions[:, None] >= positions[None, :]) & (segments[:, None] == segments[None, :])
    scores = jnp.where(allowed[None], scores, -1e+30)
    row_top = lax.optimization_barrier(jnp.max(scores, axis=-1, keepdims=True))
    weights = jnp.exp(scores - row_top)
    probabilities = weights / lax.optimization_barrier(jnp.sum(weights, axis=-1, keepdims=True))
    attended = jnp.einsum('hqk,hkd->hqd', low(probabilities), value_repeat, precision=PRECISE)
    attended = low(low_back(attended.transpose(1, 0, 2).reshape(length, H * DH)))
    branch = low_back(jnp.dot(attended, w_out, precision=PRECISE))
    middle = rows_in + branch
    ffn_normed = low(rms_scale(middle, ffn_gain))
    gate_proj = low_back(jnp.dot(ffn_normed, w_gate, precision=PRECISE))
    up_proj = low_back(jnp.dot(ffn_normed, w_up, precision=PRECISE))
    hidden = low(jax.nn.silu(gate_proj) * up_proj)
    return middle + low_back(jnp.dot(hidden, w_down, precision=PRECISE))

def reference(tokens, segment_ids, attn_gain, query_gain, key_gain, w_query, w_key, w_value, w_out, ffn_gain, w_gate, w_up, w_down, cotangent):
    params = (attn_gain.astype(jnp.float32), query_gain.astype(jnp.float32), key_gain.astype(jnp.float32), w_query.astype(jnp.float32), w_key.astype(jnp.float32), w_value.astype(jnp.float32), w_out.astype(jnp.float32), ffn_gain.astype(jnp.float32), w_gate.astype(jnp.float32), w_up.astype(jnp.float32), w_down.astype(jnp.float32))
    flat_tokens = tokens.astype(jnp.float32).reshape(MICRO * SEQS, LEN, D)
    flat_segments = segment_ids.reshape(MICRO * SEQS, LEN)
    checked = jax.checkpoint(layer)

    def forward(all_tokens, all_params):

        def one_sequence(carry_state, pair_item):
            return (carry_state, checked(pair_item[0], pair_item[1], all_params))
        _, outputs = lax.scan(one_sequence, jnp.zeros((), jnp.float32), (all_tokens, flat_segments))
        return outputs
    outputs, pull = jax.vjp(forward, flat_tokens, params)
    token_grad, param_grads = pull(cotangent.astype(jnp.float32).reshape(MICRO * SEQS, LEN, D))
    mixed = outputs.reshape(MICRO, SEQS, LEN, D).astype(jnp.bfloat16)
    return (mixed, token_grad.reshape(MICRO, SEQS, LEN, D), param_grads[0], param_grads[1], param_grads[2], param_grads[3], param_grads[4], param_grads[5], param_grads[6], param_grads[7], param_grads[8], param_grads[9], param_grads[10])
```

```python
import functools

import jax
import jax.numpy as jnp
from jax import lax
from jax.experimental import pallas as pl
from jax.experimental.pallas import tpu as pltpu
from jax.sharding import PartitionSpec as P

D = 1024
DH = 64
BLOCK = 512
MESH = pl.DeviceIdType.MESH
VMEM_LIMIT = 64000 * 1024
PIECES = 4


def remote(src, dst, send_sem, recv_sem, dp, tensor):
    return pltpu.make_async_remote_copy(
        src_ref=src,
        dst_ref=dst,
        send_sem=send_sem,
        recv_sem=recv_sem,
        device_id=(dp, tensor),
        device_id_type=MESH,
    )


def place(dp_size):
    dp = lax.axis_index("dp")
    tensor = lax.axis_index("tensor")
    return dp, tensor, dp // 2, lax.rem(dp, 2), dp_size // 2


def greet(dp_size):
    dp, tensor, outer, inner, outer_size = place(dp_size)
    barrier = pltpu.get_barrier_semaphore()

    @pl.loop(1, outer_size)
    def _(shift):
        peer = lax.rem(outer + shift, outer_size) * 2 + inner
        pl.semaphore_signal(barrier, inc=1, device_id=(peer, tensor), device_id_type=MESH)

    pl.semaphore_signal(
        barrier, inc=1, device_id=(outer * 2 + 1 - inner, tensor), device_id_type=MESH
    )
    pl.semaphore_wait(barrier, outer_size)


def gather_kernel(dp_size, *refs):
    shards = refs[:PIECES]
    fulls = refs[PIECES : 2 * PIECES]
    outer_send, outer_recv, inner_send, inner_recv = refs[2 * PIECES :]
    dp, tensor, outer, inner, outer_size = place(dp_size)
    rows = shards[0].shape[0]
    other = outer * 2 + 1 - inner
    greet(dp_size)

    def at(full, index):
        return full.at[pl.ds(pl.multiple_of(index * rows, rows), rows), :]

    def outer_copy(piece, shift):
        peer = lax.rem(outer + shift, outer_size) * 2 + inner
        return remote(
            shards[piece],
            at(fulls[piece], dp),
            outer_send.at[piece, shift],
            outer_recv.at[piece, shift],
            peer,
            tensor,
        )

    def inner_copy(piece, shift):
        source = lax.rem(outer - shift + outer_size, outer_size) * 2 + inner
        return remote(
            at(fulls[piece], source),
            at(fulls[piece], source),
            inner_send.at[piece, shift],
            inner_recv.at[piece, shift],
            other,
            tensor,
        )

    for piece in range(PIECES):
        at(fulls[piece], dp)[...] = shards[piece][...]

        @pl.loop(1, outer_size)
        def _(shift):
            outer_copy(piece, shift).start()

        remote(
            shards[piece],
            at(fulls[piece], dp),
            inner_send.at[piece, 0],
            inner_recv.at[piece, 0],
            other,
            tensor,
        ).start()
    for piece in range(PIECES):

        @pl.loop(1, outer_size)
        def _(shift):
            outer_copy(piece, shift).wait_recv()
            inner_copy(piece, shift).start()

    for piece in range(PIECES):
        inner_copy(piece, 0).wait()

        @pl.loop(1, outer_size)
        def _(shift):
            outer_copy(piece, shift).wait_send()
            inner_copy(piece, shift).wait()


def gather_weights(dp_size, shards):
    whole = pl.BlockSpec(memory_space=pltpu.VMEM)
    sems = pltpu.SemaphoreType.DMA((PIECES, dp_size // 2))
    return pl.pallas_call(
        functools.partial(gather_kernel, dp_size),
        out_shape=[
            jax.ShapeDtypeStruct((s.shape[0] * dp_size, s.shape[1]), s.dtype) for s in shards
        ],
        in_specs=[whole] * PIECES,
        out_specs=[whole] * PIECES,
        scratch_shapes=[sems] * 4,
        compiler_params=pltpu.CompilerParams(
            collective_id=0, has_side_effects=True, vmem_limit_bytes=VMEM_LIMIT
        ),
        name="gather_weights",
    )(*shards)


def scatter_kernel(dp_size, *refs):
    partials = refs[:PIECES]
    outs = refs[PIECES : 2 * PIECES]
    inner_bufs = refs[2 * PIECES : 3 * PIECES]
    outer_out = refs[3 * PIECES : 4 * PIECES]
    outer_in = refs[4 * PIECES : 5 * PIECES]
    outer_send, outer_recv, inner_send, inner_recv = refs[5 * PIECES :]
    dp, tensor, outer, inner, outer_size = place(dp_size)
    rows = outs[0].shape[0]
    other = outer * 2 + 1 - inner
    greet(dp_size)

    def at(full, index):
        return full.at[pl.ds(pl.multiple_of(index * rows, rows), rows), :]

    def inner_copy(piece, shift):
        target = lax.rem(outer + shift, outer_size) * 2 + 1 - inner
        return remote(
            at(partials[piece], target),
            inner_bufs[piece].at[shift],
            inner_send.at[piece, shift],
            inner_recv.at[piece, shift],
            other,
            tensor,
        )

    def outer_copy(piece, shift):
        peer = lax.rem(outer + shift, outer_size) * 2 + inner
        return remote(
            outer_out[piece].at[shift],
            outer_in[piece].at[shift],
            outer_send.at[piece, shift],
            outer_recv.at[piece, shift],
            peer,
            tensor,
        )

    for piece in range(PIECES):

        @pl.loop(1, outer_size)
        def _(shift):
            inner_copy(piece, shift).start()

        inner_copy(piece, 0).start()
    for piece in range(PIECES):

        @pl.loop(1, outer_size)
        def _(shift):
            inner_copy(piece, shift).wait_recv()
            target = lax.rem(outer + shift, outer_size) * 2 + inner
            outer_out[piece][shift] = (
                at(partials[piece], target)[...].astype(jnp.float32)
                + inner_bufs[piece][shift].astype(jnp.float32)
            ).astype(jnp.bfloat16)
            outer_copy(piece, shift).start()

        inner_copy(piece, 0).wait_recv()
        outs[piece][...] = at(partials[piece], dp)[...].astype(jnp.float32) + inner_bufs[piece][
            0
        ].astype(jnp.float32)
    for piece in range(PIECES):

        @pl.loop(1, outer_size)
        def _(shift):
            outer_copy(piece, shift).wait_recv()
            outs[piece][...] += outer_in[piece][shift].astype(jnp.float32)

    for piece in range(PIECES):
        inner_copy(piece, 0).wait_send()

        @pl.loop(1, outer_size)
        def _(shift):
            inner_copy(piece, shift).wait_send()
            outer_copy(piece, shift).wait_send()


def scatter_grads(dp_size, partials):
    whole = pl.BlockSpec(memory_space=pltpu.VMEM)
    sems = pltpu.SemaphoreType.DMA((PIECES, dp_size // 2))
    bufs = [
        pltpu.VMEM((dp_size // 2, p.shape[0] // dp_size, p.shape[1]), jnp.bfloat16)
        for p in partials
    ]
    return pl.pallas_call(
        functools.partial(scatter_kernel, dp_size),
        out_shape=[
            jax.ShapeDtypeStruct((p.shape[0] // dp_size, p.shape[1]), jnp.float32)
            for p in partials
        ],
        in_specs=[whole] * PIECES,
        out_specs=[whole] * PIECES,
        scratch_shapes=bufs * 3 + [sems] * 4,
        compiler_params=pltpu.CompilerParams(
            collective_id=1, has_side_effects=True, vmem_limit_bytes=VMEM_LIMIT
        ),
        name="scatter_grads",
    )(*partials)


NORM_EPS = 1e-05
ROPE_BASE = 1000000.0


def rope_tables(length, head_width):
    freq_index = jnp.arange(head_width // 2, dtype=jnp.float32)
    inverse_freq = ROPE_BASE ** (-2.0 * freq_index / head_width)
    angles = jnp.arange(length, dtype=jnp.float32)[:, None] * inverse_freq[None, :]
    return (jnp.cos(angles), jnp.sin(angles))


def rotate(values, cosine_table, sine_table):
    half_width = values.shape[-1] // 2
    front_half = values[..., :half_width]
    back_half = values[..., half_width:]
    return jnp.concatenate(
        [
            front_half * cosine_table - back_half * sine_table,
            back_half * cosine_table + front_half * sine_table,
        ],
        axis=-1,
    )


def norm_forward(values, gain_vector):
    inverse = lax.rsqrt(jnp.mean(values * values, axis=-1, keepdims=True) + NORM_EPS)
    return (values * inverse * gain_vector, inverse)


def norm_backward(values, inverse, gain_vector, upstream):
    scaled = values * inverse
    weighted = upstream * gain_vector
    back_grad = inverse * (weighted - scaled * jnp.mean(weighted * scaled, axis=-1, keepdims=True))
    return (back_grad, upstream * scaled)


def product(left_side, right_side):
    return jnp.dot(left_side, right_side, preferred_element_type=jnp.float32)


def times_transposed(left_side, right_side):
    return lax.dot_general(
        left_side, right_side, (((1,), (1,)), ((), ())), preferred_element_type=jnp.float32
    )


def transposed_times(left_side, right_side):
    return lax.dot_general(
        left_side, right_side, (((0,), (0,)), ((), ())), preferred_element_type=jnp.float32
    )


def shards(
    dp_size,
    tokens,
    segment_ids,
    attn_gain,
    query_gain,
    key_gain,
    w_query,
    w_key,
    w_value,
    w_out,
    ffn_gain,
    w_gate,
    w_up,
    w_down,
    cotangent,
):
    micro_count = tokens.shape[0]
    length = segment_ids.shape[2]
    block_count = length // BLOCK
    head_count = w_query.shape[1] // DH
    group_count = w_key.shape[1] // DH
    group_size = head_count // group_count
    score_scale = DH ** (-0.5)
    cosine_table, sine_table = rope_tables(length, DH)
    cosine_heads = cosine_table[:, None, :]
    sine_heads = sine_table[:, None, :]
    positions = jnp.arange(length)
    attn_full, gate_kept, up_kept, down_kept = gather_weights(
        dp_size,
        (jnp.concatenate([w_query, w_key, w_value, w_out.T], axis=1), w_gate, w_up, w_down.T),
    )
    query_end = w_query.shape[1]
    key_end = query_end + w_key.shape[1]
    value_end = key_end + w_value.shape[1]
    attn_kept = (
        attn_full[:, :query_end],
        attn_full[:, query_end:key_end],
        attn_full[:, key_end:value_end],
        attn_full[:, value_end:],
    )
    ffn_kept = (gate_kept, up_kept, down_kept)

    def attn_source():
        return attn_kept

    def ffn_source():
        return ffn_kept

    def heads_major(values):
        return values.reshape(length, group_count, group_size, DH).transpose(1, 2, 0, 3)

    def block_mask(block_index, segments):
        row_start = block_index * BLOCK
        row_end = row_start + BLOCK
        row_pos = positions[row_start:row_end]
        return (row_pos[:, None] >= positions[None, :row_end]) & (
            segments[row_start:row_end, None] == segments[None, :row_end]
        )

    def attention_backward(query_major, key_major, value_major, log_totals, grad_major, segments):
        query_grads = []
        key_grad = jnp.zeros((group_count, length, DH), jnp.float32)
        value_grad = jnp.zeros((group_count, length, DH), jnp.float32)
        for block_index in range(block_count):
            row_start = block_index * BLOCK
            row_end = row_start + BLOCK
            query_block = query_major[:, :, row_start:row_end]
            grad_block = grad_major[:, :, row_start:row_end]
            allowed = block_mask(block_index, segments)
            scores = jnp.einsum(
                "gjqd,gkd->gjqk",
                query_block,
                key_major[:, :row_end],
                preferred_element_type=jnp.float32,
            )
            probabilities = jnp.where(allowed, jnp.exp(scores - log_totals[block_index]), 0.0)
            prob_grad = jnp.einsum(
                "gjqd,gkd->gjqk",
                grad_block,
                value_major[:, :row_end],
                preferred_element_type=jnp.float32,
            )
            row_delta = jnp.sum(probabilities * prob_grad, axis=-1, keepdims=True)
            score_grad = (probabilities * (prob_grad - row_delta)).astype(jnp.bfloat16)
            query_grads.append(
                jnp.einsum(
                    "gjqk,gkd->gjqd",
                    score_grad,
                    key_major[:, :row_end],
                    preferred_element_type=jnp.float32,
                )
            )
            key_part = jnp.einsum(
                "gjqk,gjqd->gkd", score_grad, query_block, preferred_element_type=jnp.float32
            )
            value_part = jnp.einsum(
                "gjqk,gjqd->gkd",
                probabilities.astype(jnp.bfloat16),
                grad_block,
                preferred_element_type=jnp.float32,
            )
            key_grad = key_grad.at[:, :row_end].add(key_part)
            value_grad = value_grad.at[:, :row_end].add(value_part)
        query_grad_all = (
            jnp.concatenate(query_grads, axis=2)
            .transpose(2, 0, 1, 3)
            .reshape(length, head_count, DH)
        )
        return (query_grad_all, key_grad.transpose(1, 0, 2), value_grad.transpose(1, 0, 2))

    grad_accs = (
        jnp.zeros((D, w_query.shape[1]), jnp.float32),
        jnp.zeros((D, w_key.shape[1]), jnp.float32),
        jnp.zeros((D, w_value.shape[1]), jnp.float32),
        jnp.zeros((D, w_out.shape[0]), jnp.float32),
        jnp.zeros((D, w_gate.shape[1]), jnp.float32),
        jnp.zeros((D, w_up.shape[1]), jnp.float32),
        jnp.zeros((D, w_down.shape[0]), jnp.float32),
    )
    shard_sums = None
    attn_gain_acc = jnp.zeros((D,), jnp.float32)
    ffn_gain_acc = jnp.zeros((D,), jnp.float32)
    query_gain_acc = jnp.zeros((DH,), jnp.float32)
    key_gain_acc = jnp.zeros((DH,), jnp.float32)
    mixed_rows = []
    input_grads = []
    for micro_index in range(micro_count):
        rows_in = tokens[micro_index, 0].astype(jnp.float32)
        segments = segment_ids[micro_index, 0]
        query_full, key_full, value_full, out_full = attn_source()
        normed, inverse_one = norm_forward(rows_in, attn_gain)
        normed_all = lax.all_gather(normed.astype(jnp.bfloat16), "tensor", axis=0, tiled=True)
        query_heads = product(normed_all, query_full).reshape(length, head_count, DH)
        key_heads = product(normed_all, key_full).reshape(length, group_count, DH)
        value_low = (
            product(normed_all, value_full).astype(jnp.bfloat16).reshape(length, group_count, DH)
        )
        query_normed, query_inverse = norm_forward(query_heads, query_gain)
        query_rot = (rotate(query_normed, cosine_heads, sine_heads) * score_scale).astype(
            jnp.bfloat16
        )
        key_normed, key_inverse = norm_forward(key_heads, key_gain)
        key_rot = rotate(key_normed, cosine_heads, sine_heads).astype(jnp.bfloat16)
        query_major = heads_major(query_rot)
        key_major = key_rot.transpose(1, 0, 2)
        value_major = value_low.transpose(1, 0, 2)
        outputs = []
        attention_log_totals = []
        for attention_block_index in range(block_count):
            attention_row_start = attention_block_index * BLOCK
            attention_row_end = attention_row_start + BLOCK
            attention_query_block = query_major[:, :, attention_row_start:attention_row_end]
            attention_allowed = block_mask(attention_block_index, segments)
            attention_scores = jnp.einsum(
                "gjqd,gkd->gjqk",
                attention_query_block,
                key_major[:, :attention_row_end],
                preferred_element_type=jnp.float32,
            )
            attention_scores = jnp.where(attention_allowed, attention_scores, -1e30)
            row_top = jnp.max(attention_scores, axis=-1, keepdims=True)
            weights = jnp.exp(attention_scores - row_top)
            row_total = jnp.sum(weights, axis=-1, keepdims=True)
            attention_probabilities = (weights / row_total).astype(jnp.bfloat16)
            outputs.append(
                jnp.einsum(
                    "gjqk,gkd->gjqd",
                    attention_probabilities,
                    value_major[:, :attention_row_end],
                    preferred_element_type=jnp.float32,
                )
            )
            attention_log_totals.append(row_top + jnp.log(row_total))
        attended = (
            jnp.concatenate(outputs, axis=2).transpose(2, 0, 1, 3).reshape(length, head_count * DH)
        )
        log_totals = attention_log_totals
        attended_low = attended.astype(jnp.bfloat16)
        branch = lax.psum_scatter(
            times_transposed(attended_low, out_full), "tensor", scatter_dimension=0, tiled=True
        )
        middle = rows_in + branch
        ffn_normed, inverse_two = norm_forward(middle, ffn_gain)
        ffn_all = lax.all_gather(ffn_normed.astype(jnp.bfloat16), "tensor", axis=0, tiled=True)
        gate_full, up_full, down_full = ffn_source()
        gate_proj = product(ffn_all, gate_full)
        up_proj = product(ffn_all, up_full)
        gate_sig = jax.nn.sigmoid(gate_proj)
        gate_act = gate_proj * gate_sig
        hidden = (gate_act * up_proj).astype(jnp.bfloat16)
        ffn_out = lax.psum_scatter(
            times_transposed(hidden, down_full).astype(jnp.bfloat16),
            "tensor",
            scatter_dimension=0,
            tiled=True,
        ).astype(jnp.float32)
        mixed_rows.append((middle + ffn_out).astype(jnp.bfloat16))
        upstream = cotangent[micro_index, 0].astype(jnp.float32)
        gate_full, up_full, down_full = ffn_source()
        ffn_upstream = lax.all_gather(upstream.astype(jnp.bfloat16), "tensor", axis=0, tiled=True)
        hidden_grad = product(ffn_upstream, down_full)
        gate_grad = (
            hidden_grad * up_proj * gate_sig * (1.0 + gate_proj * (1.0 - gate_sig))
        ).astype(jnp.bfloat16)
        up_grad = (hidden_grad * gate_act).astype(jnp.bfloat16)
        ffn_part = times_transposed(gate_grad, gate_full) + times_transposed(up_grad, up_full)
        ffn_normed_grad = lax.psum_scatter(
            ffn_part.astype(jnp.bfloat16), "tensor", scatter_dimension=0, tiled=True
        ).astype(jnp.float32)
        middle_back, ffn_term = norm_backward(middle, inverse_two, ffn_gain, ffn_normed_grad)
        ffn_gain_acc = ffn_gain_acc + jnp.sum(ffn_term, axis=0)
        middle_grad = upstream + middle_back
        attn_upstream = lax.all_gather(
            middle_grad.astype(jnp.bfloat16), "tensor", axis=0, tiled=True
        )
        query_full, key_full, value_full, out_full = attn_source()
        attended_grad = product(attn_upstream, out_full).astype(jnp.bfloat16)
        rot_query_grad, key_rot_grad, value_grad = attention_backward(
            query_major, key_major, value_major, log_totals, heads_major(attended_grad), segments
        )
        query_normed_grad = rotate(rot_query_grad * score_scale, cosine_heads, -sine_heads)
        query_back, query_term = norm_backward(
            query_heads, query_inverse, query_gain, query_normed_grad
        )
        query_gain_acc = query_gain_acc + jnp.sum(query_term, axis=(0, 1))
        query_grad = query_back.reshape(length, head_count * DH).astype(jnp.bfloat16)
        key_normed_grad = rotate(key_rot_grad, cosine_heads, -sine_heads)
        key_back, key_term = norm_backward(key_heads, key_inverse, key_gain, key_normed_grad)
        key_gain_acc = key_gain_acc + jnp.sum(key_term, axis=(0, 1))
        key_grad = key_back.reshape(length, group_count * DH).astype(jnp.bfloat16)
        value_grad_low = value_grad.reshape(length, group_count * DH).astype(jnp.bfloat16)
        attn_part = (
            times_transposed(query_grad, query_full)
            + times_transposed(key_grad, key_full)
            + times_transposed(value_grad_low, value_full)
        )
        normed_grad = lax.psum_scatter(
            attn_part.astype(jnp.bfloat16), "tensor", scatter_dimension=0, tiled=True
        ).astype(jnp.float32)
        token_back, attn_term = norm_backward(rows_in, inverse_one, attn_gain, normed_grad)
        attn_gain_acc = attn_gain_acc + jnp.sum(attn_term, axis=0)
        input_grads.append(middle_grad + token_back)
        grad_accs = (
            grad_accs[0] + transposed_times(normed_all, query_grad),
            grad_accs[1] + transposed_times(normed_all, key_grad),
            grad_accs[2] + transposed_times(normed_all, value_grad_low),
            grad_accs[3] + transposed_times(attn_upstream, attended_low),
            grad_accs[4] + transposed_times(ffn_all, gate_grad),
            grad_accs[5] + transposed_times(ffn_all, up_grad),
            grad_accs[6] + transposed_times(ffn_upstream, hidden),
        )
    low_accs = [acc.astype(jnp.bfloat16) for acc in grad_accs]
    attn_sum, gate_sum, up_sum, down_sum = scatter_grads(
        dp_size, (jnp.concatenate(low_accs[:4], axis=1), *low_accs[4:])
    )
    shard_sums = (
        attn_sum[:, :query_end],
        attn_sum[:, query_end:key_end],
        attn_sum[:, key_end:value_end],
        attn_sum[:, value_end:].T,
        gate_sum,
        up_sum,
        down_sum.T,
    )
    gain_sums = lax.psum(
        (attn_gain_acc, query_gain_acc, key_gain_acc, ffn_gain_acc), ("dp", "tensor")
    )
    mixed = jnp.stack(mixed_rows, axis=0)[:, None]
    grad_tokens = jnp.stack(input_grads, axis=0)[:, None]
    return (
        mixed,
        grad_tokens,
        gain_sums[0],
        gain_sums[1],
        gain_sums[2],
        shard_sums[0],
        shard_sums[1],
        shard_sums[2],
        shard_sums[3],
        gain_sums[3],
        shard_sums[4],
        shard_sums[5],
        shard_sums[6],
    )


def solution(mesh):
    placed = (
        P(None, "dp", "tensor", None),
        P(None, "dp", None),
        P(),
        P(),
        P(),
        P("dp", "tensor"),
        P("dp", "tensor"),
        P("dp", "tensor"),
        P("tensor", "dp"),
        P(),
        P("dp", "tensor"),
        P("dp", "tensor"),
        P("tensor", "dp"),
        P(None, "dp", "tensor", None),
    )
    return jax.shard_map(
        functools.partial(shards, mesh.shape["dp"]),
        mesh=mesh,
        in_specs=placed,
        out_specs=(
            P(None, "dp", "tensor", None),
            P(None, "dp", "tensor", None),
            P(),
            P(),
            P(),
            P("dp", "tensor"),
            P("dp", "tensor"),
            P("dp", "tensor"),
            P("tensor", "dp"),
            P(),
            P("dp", "tensor"),
            P("dp", "tensor"),
            P("tensor", "dp"),
        ),
        check_vma=False,
    )
```

```python
import functools
import math

import jax
import jax.numpy as jnp
from jax import lax
from jax.experimental import pallas as pl
from jax.experimental.pallas import tpu as pltpu
from jax.sharding import PartitionSpec as P

MESH = pl.DeviceIdType.MESH
VMEM_LIMIT = 65000 * 1024
NORM_EPS = 1e-05
ROPE_BASE = 1000000.0
DH = 64
TILE = 256
LN2 = math.log(2.0)
APART = -32768.0
BF16 = jnp.bfloat16
F32 = jnp.float32


def nn(left, right):
    return lax.dot_general(left, right, (((1,), (0,)), ((), ())), preferred_element_type=F32)


def nt(left, right):
    return lax.dot_general(left, right, (((1,), (1,)), ((), ())), preferred_element_type=F32)


def tn(left, right):
    return lax.dot_general(left, right, (((0,), (0,)), ((), ())), preferred_element_type=F32)


def tile(index, size=TILE):
    return pl.ds(pl.multiple_of(index * size, size), size)


def low_parts(values):
    high = values.astype(BF16)
    return high, (values - high.astype(F32)).astype(BF16)


def head_mean(values, mixer):
    high, rest = low_parts(values)
    return nn(high, mixer) + nn(rest, mixer)


def swap_halves(values):
    lane = lax.broadcasted_iota(jnp.int32, values.shape, 1)
    ahead = pltpu.roll(values, 96, 1)
    behind = pltpu.roll(values, 32, 1)
    return jnp.where(lax.rem(lane, 64) < 32, ahead, behind)


def norm_rows(values, gain):
    inverse = lax.rsqrt(jnp.mean(values * values, axis=-1, keepdims=True) + NORM_EPS)
    return values * inverse * gain


def norm_rows_back(values, gain, upstream):
    inverse = lax.rsqrt(jnp.mean(values * values, axis=-1, keepdims=True) + NORM_EPS)
    scaled = values * inverse
    weighted = upstream * gain
    back = inverse * (weighted - scaled * jnp.mean(weighted * scaled, axis=-1, keepdims=True))
    return back, jnp.sum(upstream * scaled, axis=0, keepdims=True)


class Place:
    def __init__(self, dp_size):
        self.dp_size = dp_size
        self.dp = lax.axis_index("dp")
        self.tensor = lax.axis_index("tensor")
        self.outer_size = dp_size // 2
        self.outer = self.dp // 2
        self.inner = lax.rem(self.dp, 2)
        self.other = self.outer * 2 + 1 - self.inner
        self.side = self.tensor // 2
        self.core = lax.rem(self.tensor, 2)
        self.across = (1 - self.side) * 2 + self.core
        self.twin = self.side * 2 + 1 - self.core

    def ahead(self, shift, inner=None):
        inner = self.inner if inner is None else inner
        return lax.rem(self.outer + shift, self.outer_size) * 2 + inner

    def behind(self, shift):
        return lax.rem(self.outer - shift + self.outer_size, self.outer_size) * 2 + self.inner

    def block(self, step):
        side = 1 - self.side if step < 2 else self.side
        core = 1 - self.core if step % 2 == 0 else self.core
        return side * 2 + core

    def copy(self, src, dst, sems, index, dp=None, tensor=None):
        return pltpu.make_async_remote_copy(
            src_ref=src,
            dst_ref=dst,
            send_sem=sems[0].at[index],
            recv_sem=sems[1].at[index],
            device_id=(
                self.dp if dp is None else dp,
                self.tensor if tensor is None else tensor,
            ),
            device_id_type=MESH,
        )

    def greet(self, everyone):
        barrier = pltpu.get_barrier_semaphore()

        def signal(dp, tensor):
            pl.semaphore_signal(barrier, inc=1, device_id=(dp, tensor), device_id_type=MESH)

        if everyone:

            @pl.loop(1, self.dp_size)
            def _(shift):
                signal(lax.rem(self.dp + shift, self.dp_size), self.tensor)

            for shift in range(1, 4):
                signal(self.dp, lax.rem(self.tensor + shift, 4))
            pl.semaphore_wait(barrier, self.dp_size + 2)
        else:

            @pl.loop(1, self.outer_size)
            def _(shift):
                signal(self.ahead(shift), self.tensor)

            signal(self.other, self.tensor)
            signal(self.dp, self.across)
            signal(self.dp, self.twin)
            pl.semaphore_wait(barrier, self.outer_size + 2)


class Gather:
    def __init__(self, place, ref, micro, sems, index, source=None):
        own = ref.at[micro, tile(place.tensor)]
        source = own if source is None else source
        theirs = ref.at[micro, tile(place.across)]
        self.to_across = place.copy(source, own, sems, index, tensor=place.across)
        self.to_twin = place.copy(source, own, sems, index + 1, tensor=place.twin)
        self.on_to_twin = place.copy(theirs, theirs, sems, index + 2, tensor=place.twin)

    def start(self):
        self.to_across.start()
        self.to_twin.start()

    def relay(self):
        self.to_across.wait_recv()
        self.on_to_twin.start()

    def finish(self):
        self.to_twin.wait_recv()
        self.on_to_twin.wait_recv()

    def drain(self):
        self.to_across.wait_send()
        self.to_twin.wait_send()
        self.on_to_twin.wait_send()


class Scatter:
    def __init__(self, place, staged, from_twin, from_across, sems, index):
        self.staged = staged
        self.from_twin = from_twin
        self.from_across = from_across
        self.twins = [
            place.copy(staged.at[half], from_twin.at[half], sems, index + half, tensor=place.twin)
            for half in range(2)
        ]
        self.crossing = place.copy(
            staged.at[2], from_across, sems, index + 2, tensor=place.across
        )

    def give(self, step, values):
        if step == 0 or step == 2:
            half = step // 2
            self.staged[half] = values.astype(BF16)
            self.twins[half].start()
        elif step == 1:
            self.twins[0].wait_recv()
            self.staged[2] = (values + self.from_twin[0].astype(F32)).astype(BF16)
            self.crossing.start()

    def result(self, values):
        self.twins[1].wait_recv()
        self.crossing.wait_recv()
        return values + self.from_twin[1].astype(F32) + self.from_across[...].astype(F32)

    def drain(self):
        self.twins[0].wait_send()
        self.twins[1].wait_send()
        self.crossing.wait_send()


class Weights:
    def __init__(self, place, shard, full, outer_sems, inner_sems, piece):
        self.place = place
        self.shard = shard
        self.full = full
        self.outer_sems = outer_sems
        self.inner_sems = inner_sems
        self.piece = piece
        self.rows = shard.shape[0]

    def at(self, index):
        return self.full.at[pl.ds(pl.multiple_of(index * self.rows, self.rows), self.rows), :]

    def outer_copy(self, shift):
        place = self.place
        return place.copy(
            self.shard,
            self.at(place.dp),
            self.outer_sems,
            (self.piece, shift),
            dp=place.ahead(shift),
        )

    def inner_copy(self, shift):
        place = self.place
        rows = self.at(place.behind(shift))
        return place.copy(rows, rows, self.inner_sems, (self.piece, shift), dp=place.other)

    def own_copy(self):
        place = self.place
        return place.copy(
            self.shard, self.at(place.dp), self.inner_sems, (self.piece, 0), dp=place.other
        )

    def send_outer(self):
        @pl.loop(1, self.place.outer_size)
        def _(shift):
            self.outer_copy(shift).start()

    def send_inner(self):
        self.own_copy().start()

    def relay(self, first, last):
        @pl.loop(first, last)
        def _(shift):
            self.outer_copy(shift).wait_recv()
            self.inner_copy(shift).start()

    def finish(self):
        @pl.loop(0, self.place.outer_size)
        def _(shift):
            self.inner_copy(shift).wait_recv()

    def drain(self):
        self.own_copy().wait_send()

        @pl.loop(1, self.place.outer_size)
        def _(shift):
            self.outer_copy(shift).wait_send()
            self.inner_copy(shift).wait_send()


def forward_kernel(
    dp_size,
    tokens,
    cotangent,
    attn_shard,
    gate_shard,
    up_shard,
    down_shard,
    attn_gain,
    ffn_gain,
    tables,
    query_marks,
    key_marks,
    mixer,
    out_attn_full,
    out_gate_full,
    out_up_full,
    out_down_full,
    out_normed,
    out_ffn,
    out_cot,
    out_gate_slope,
    out_up_slope,
    out_hidden,
    out_grad_down,
    out_query,
    out_key,
    out_value,
    out_attended,
    out_proj,
    out_middle,
    normed,
    ffn_all,
    cot_all,
    attn_full,
    gate_full,
    up_full,
    slopes,
    hidden,
    grad_down,
    query,
    key,
    value,
    attended,
    proj,
    middle,
    staged,
    from_twin,
    from_across,
    outer_send,
    outer_recv,
    inner_send,
    inner_recv,
    group_send,
    group_recv,
    local_sems,
    slope_sems,
):
    place = Place(dp_size)
    micro_count = tokens.shape[0]
    outer_size = place.outer_size
    group_sems = (group_send, group_recv)
    outer_sems = (outer_send, outer_recv)
    inner_sems = (inner_send, inner_recv)
    own = tile(place.tensor)
    place.greet(False)

    attn_w = Weights(place, attn_shard, attn_full, outer_sems, inner_sems, 0)
    gate_w = Weights(place, gate_shard, gate_full, outer_sems, inner_sems, 1)
    up_w = Weights(place, up_shard, up_full, outer_sems, inner_sems, 2)
    down_w = Weights(place, down_shard, out_down_full, outer_sems, inner_sems, 3)
    normed_g = [Gather(place, normed, m, group_sems, 3 * m) for m in range(micro_count)]
    cot_g = [
        Gather(place, cot_all, m, group_sems, 6 + 3 * m, cotangent.at[m])
        for m in range(micro_count)
    ]
    ffn_g = [Gather(place, ffn_all, m, group_sems, 12 + 3 * m) for m in range(micro_count)]
    branch_s = [
        Scatter(
            place, staged.at[m], from_twin.at[m], from_across.at[m], group_sems, 18 + 3 * m
        )
        for m in range(micro_count)
    ]
    saves = []

    def save(src, dst):
        copy = pltpu.make_async_copy(src, dst, local_sems.at[len(saves)])
        copy.start()
        saves.append(copy)
        return copy

    attn_w.send_outer()
    attn_w.send_inner()
    for m in range(micro_count):
        normed[m, own] = norm_rows(tokens[m].astype(F32), attn_gain[...]).astype(BF16)
        normed_g[m].start()
    gate_w.send_outer()
    up_w.send_outer()
    down_w.send_outer()
    cot_g[0].start()
    attn_w.at(place.dp)[...] = attn_shard[...]
    gate_w.at(place.dp)[...] = gate_shard[...]
    up_w.at(place.dp)[...] = up_shard[...]
    save(down_shard, down_w.at(place.dp))
    for m in range(micro_count):
        cot_all[m, own] = cotangent[m]
    normed_g[0].relay()
    attn_w.relay(1, outer_size)
    gate_w.send_inner()
    up_w.send_inner()
    down_w.send_inner()
    normed_g[0].finish()
    attn_w.finish()
    save(attn_full, out_attn_full)

    lane = lax.broadcasted_iota(jnp.int32, (TILE, 128), 1)
    front = lane < 64
    later = lax.broadcasted_iota(jnp.int32, (TILE, TILE), 1) > lax.broadcasted_iota(
        jnp.int32, (TILE, TILE), 0
    )
    causal = jnp.where(later, APART, 0.0)
    block_count = normed.shape[1] // TILE
    pending = []

    def project(m):
        @pl.loop(0, block_count)
        def _(block):
            rows = tile(block)
            product = nn(normed[m, rows], attn_full[:, 0:512])
            proj[m, rows] = product[:, :384]
            heads = product[:, :256]
            inverse = lax.rsqrt(head_mean(heads * heads, mixer[...]) + NORM_EPS)
            for group in range(2):
                lanes = slice(128 * group, 128 * group + 128)
                part = heads[:, lanes]
                turned = part * tables[0, rows] + swap_halves(part) * tables[1, rows]
                query[m, group, rows, 0:128] = (turned * inverse[:, lanes]).astype(BF16)
                query[m, group, rows, 128:256] = query_marks[m, rows]
            part = product[:, 256:384]
            inverse = lax.rsqrt(head_mean(part * part, mixer[0:128, 0:128]) + NORM_EPS)
            turned = (part * tables[2, rows] + swap_halves(part) * tables[3, rows]) * inverse
            moved = pltpu.roll(turned, 64, 1)
            val = product[:, 384:512]
            val_moved = pltpu.roll(val, 64, 1)
            for group in range(2):
                first, second = (turned, moved) if group == 0 else (moved, turned)
                key[m, group, 0, rows, 0:128] = jnp.where(front, first, 0.0).astype(BF16)
                key[m, group, 1, rows, 0:128] = jnp.where(front, 0.0, second).astype(BF16)
                first, second = (val, val_moved) if group == 0 else (val_moved, val)
                value[m, group, 0, rows, 0:128] = jnp.where(front, first, 0.0).astype(BF16)
                value[m, group, 1, rows, 0:128] = jnp.where(front, 0.0, second).astype(BF16)
                for head in range(2):
                    key[m, group, head, rows, 128:256] = key_marks[head, m, rows]
                value[m, group, 0, rows, 128:256] = jnp.where(front, 1.0, 0.0).astype(BF16)
                value[m, group, 1, rows, 128:256] = jnp.where(front, 0.0, 1.0).astype(BF16)

    def attend(m):
        @pl.loop(0, 2)
        def _(group):
            for block in range(block_count):
                rows = slice(block * TILE, (block + 1) * TILE)
                query_block = query[m, group, rows]
                total = jnp.zeros((TILE, 256), F32)
                for head in range(2):
                    if block > 0:
                        before = slice(0, block * TILE)
                        scores = nt(query_block, key[m, group, head, before])
                        weights = jnp.exp2(scores).astype(BF16)
                        total = total + nn(weights, value[m, group, head, before])
                    scores = nt(query_block, key[m, group, head, rows]) + causal
                    weights = jnp.exp2(scores).astype(BF16)
                    total = total + nn(weights, value[m, group, head, rows])
                sums = total[:, 128:256]
                attended[m, group, rows] = (total[:, 0:128] / sums).astype(BF16)
                shift = -jnp.log2(sums)
                high = shift.astype(BF16)
                middle_part = (shift - high.astype(F32)).astype(BF16)
                last = (shift - high.astype(F32) - middle_part.astype(F32)).astype(BF16)
                place_in = lax.rem(lane, 64)
                marks = jnp.where(
                    place_in == 0,
                    high.astype(F32),
                    jnp.where(
                        place_in == 1,
                        middle_part.astype(F32),
                        jnp.where(
                            place_in == 2,
                            last.astype(F32),
                            query_block[:, 128:256].astype(F32),
                        ),
                    ),
                )
                query[m, group, rows, 128:256] = marks.astype(BF16)

    def branch_block(m, step):
        rows = tile(place.block(step))
        heads = jnp.concatenate([attended[m, 0, rows], attended[m, 1, rows]], axis=1)
        return nt(heads, attn_full[:, 512:768])

    def branch(m):
        for step in range(3):
            branch_s[m].give(step, branch_block(m, step))

    def enter_ffn(m):
        total = branch_s[m].result(branch_block(m, 3))
        middle[m] = tokens[m].astype(F32) + total
        save(middle.at[m], out_middle.at[m])
        ffn_all[m, own] = norm_rows(middle[m], ffn_gain[...]).astype(BF16)
        ffn_g[m].start()

    project(0)
    normed_g[1].relay()
    attend(0)
    branch(0)
    cot_g[1].start()
    cot_g[0].relay()
    normed_g[1].finish()
    project(1)
    gate_w.relay(1, outer_size // 2)
    attend(1)
    branch(1)
    for m in range(micro_count):
        save(query.at[m], out_query.at[m])
        save(key.at[m], out_key.at[m])
        save(value.at[m], out_value.at[m])
        save(attended.at[m], out_attended.at[m])
        save(proj.at[m], out_proj.at[m])
        save(normed.at[m], out_normed.at[m])
    enter_ffn(0)
    gate_w.relay(outer_size // 2, outer_size)
    enter_ffn(1)
    cot_g[1].relay()
    up_w.relay(1, outer_size // 2)
    ffn_g[0].relay()
    up_w.relay(outer_size // 2, outer_size)
    gate_w.finish()
    save(gate_full, out_gate_full)
    ffn_g[1].relay()
    for m in range(micro_count):
        cot_g[m].finish()
        save(cot_all.at[m], out_cot.at[m])
    ffn_g[0].finish()
    save(ffn_all.at[0], out_ffn.at[0])
    up_w.finish()
    save(up_full, out_up_full)

    def slope_copies(m, block, slot):
        rows = tile(block)
        return [
            pltpu.make_async_copy(slopes.at[slot, 0], out_gate_slope.at[m, rows], slope_sems.at[slot, 0]),
            pltpu.make_async_copy(slopes.at[slot, 1], out_up_slope.at[m, rows], slope_sems.at[slot, 1]),
        ]

    def ffn_tile(m, block):
        rows = tile(block)
        slot = lax.rem(block, 2)

        @pl.when(block >= 2)
        def _():
            for copy in slope_copies(m, block - 2, slot):
                copy.wait()

        gate = nn(ffn_all[m, rows], gate_full[...])
        up = nn(ffn_all[m, rows], up_full[...])
        sig = 1.0 / (1.0 + jnp.exp(-gate))
        act = gate * sig
        hidden[m, rows] = (act * up).astype(BF16)
        slopes[slot, 0] = (up * (sig + act * (1.0 - sig))).astype(BF16)
        slopes[slot, 1] = act.astype(BF16)
        for copy in slope_copies(m, block, slot):
            copy.start()

    def ffn(m):
        @pl.loop(0, block_count)
        def _(block):
            ffn_tile(m, block)

        for block in (block_count - 2, block_count - 1):
            for copy in slope_copies(m, block, block % 2):
                copy.wait()

    ffn(0)
    save(hidden.at[0], out_hidden.at[0])
    down_w.relay(1, outer_size // 2)
    ffn_g[1].finish()
    save(ffn_all.at[1], out_ffn.at[1])
    ffn(1)
    save(hidden.at[1], out_hidden.at[1])

    @pl.loop(0, block_count)
    def _(block):
        columns = tile(block)
        grad_down[columns] = (
            tn(cot_all[0, :, columns], hidden[0]) + tn(cot_all[1, :, columns], hidden[1])
        ).astype(BF16)

    save(grad_down, out_grad_down)
    down_w.relay(outer_size // 2, outer_size)
    down_w.finish()
    for piece in (attn_w, gate_w, up_w, down_w):
        piece.drain()
    for m in range(micro_count):
        normed_g[m].drain()
        cot_g[m].drain()
        ffn_g[m].drain()
        branch_s[m].drain()
    for copy in saves:
        copy.wait()


def forward(dp_size, tokens, cotangent, shards, attn_gain, ffn_gain, tables, query_marks, key_marks, mixer):
    micro, rows, width = tokens.shape
    length = tables.shape[1]
    hidden_width = shards[1].shape[1]
    attn_width = shards[0].shape[1]
    outer_size = dp_size // 2
    whole = pl.BlockSpec(memory_space=pltpu.VMEM)
    anywhere = pl.BlockSpec(memory_space=pl.ANY)
    shape = jax.ShapeDtypeStruct
    out_shape = [
        shape((width, attn_width), BF16),
        shape((width, hidden_width), BF16),
        shape((width, hidden_width), BF16),
        shape((width, hidden_width), BF16),
        shape((micro, length, width), BF16),
        shape((micro, length, width), BF16),
        shape((micro, length, width), BF16),
        shape((micro, length, hidden_width), BF16),
        shape((micro, length, hidden_width), BF16),
        shape((micro, length, hidden_width), BF16),
        shape((width, hidden_width), BF16),
        shape((micro, 2, length, 256), BF16),
        shape((micro, 2, 2, length, 256), BF16),
        shape((micro, 2, 2, length, 256), BF16),
        shape((micro, 2, length, 128), BF16),
        shape((micro, length, 384), F32),
        shape((micro, rows, width), F32),
    ]
    scratch = [
        pltpu.VMEM((micro, length, width), BF16),
        pltpu.VMEM((micro, length, width), BF16),
        pltpu.VMEM((micro, length, width), BF16),
        pltpu.VMEM((width, attn_width), BF16),
        pltpu.VMEM((width, hidden_width), BF16),
        pltpu.VMEM((width, hidden_width), BF16),
        pltpu.VMEM((2, 2, TILE, hidden_width), BF16),
        pltpu.VMEM((micro, length, hidden_width), BF16),
        pltpu.VMEM((width, hidden_width), BF16),
        pltpu.VMEM((micro, 2, length, 256), BF16),
        pltpu.VMEM((micro, 2, 2, length, 256), BF16),
        pltpu.VMEM((micro, 2, 2, length, 256), BF16),
        pltpu.VMEM((micro, 2, length, 128), BF16),
        pltpu.VMEM((micro, length, 384), F32),
        pltpu.VMEM((micro, rows, width), F32),
        pltpu.VMEM((micro, 3, rows, width), BF16),
        pltpu.VMEM((micro, 2, rows, width), BF16),
        pltpu.VMEM((micro, rows, width), BF16),
        pltpu.SemaphoreType.DMA((4, outer_size)),
        pltpu.SemaphoreType.DMA((4, outer_size)),
        pltpu.SemaphoreType.DMA((4, outer_size)),
        pltpu.SemaphoreType.DMA((4, outer_size)),
        pltpu.SemaphoreType.DMA((24,)),
        pltpu.SemaphoreType.DMA((24,)),
        pltpu.SemaphoreType.DMA((32,)),
        pltpu.SemaphoreType.DMA((2, 2)),
    ]
    return pl.pallas_call(
        functools.partial(forward_kernel, dp_size),
        out_shape=out_shape,
        in_specs=[whole, whole, whole, whole, whole, anywhere] + [whole] * 6,
        out_specs=[anywhere] * len(out_shape),
        scratch_shapes=scratch,
        compiler_params=pltpu.CompilerParams(
            collective_id=0, has_side_effects=True, vmem_limit_bytes=VMEM_LIMIT
        ),
        name="forward_pass",
    )(tokens, cotangent, *shards, attn_gain, ffn_gain, tables, query_marks, key_marks, mixer)


class Shares:
    def __init__(self, place, partial, kept, from_inner, from_outer, total, outer_sems, inner_sems, piece):
        self.place = place
        self.partial = partial
        self.kept = kept
        self.from_inner = from_inner
        self.from_outer = from_outer
        self.total = total
        self.outer_sems = outer_sems
        self.inner_sems = inner_sems
        self.piece = piece
        self.rows = total.shape[0]

    def at(self, index):
        return self.partial.at[pl.ds(pl.multiple_of(index * self.rows, self.rows), self.rows), :]

    def mine(self, shift):
        if self.kept is not None:
            return self.kept.at[shift]
        return self.at(self.place.ahead(shift))

    def inner_copy(self, shift):
        place = self.place
        return place.copy(
            self.at(place.ahead(shift, 1 - place.inner)),
            self.from_inner.at[shift],
            self.inner_sems,
            (self.piece, shift),
            dp=place.other,
        )

    def outer_copy(self, shift):
        place = self.place
        return place.copy(
            self.mine(shift),
            self.from_outer.at[shift - 1],
            self.outer_sems,
            (self.piece, shift),
            dp=place.ahead(shift),
        )

    def give(self):
        @pl.loop(1, self.place.outer_size)
        def _(shift):
            self.inner_copy(shift).start()

        self.inner_copy(0).start()

    def turn(self, first, last):
        @pl.loop(first, last)
        def _(shift):
            self.inner_copy(shift).wait_recv()
            mine = self.mine(shift)
            mine[...] = (mine[...].astype(F32) + self.from_inner[shift].astype(F32)).astype(BF16)
            self.outer_copy(shift).start()

    def keep(self):
        self.inner_copy(0).wait_recv()
        self.total[...] = self.mine(0)[...].astype(F32) + self.from_inner[0].astype(F32)

    def finish(self):
        @pl.loop(1, self.place.outer_size)
        def _(shift):
            self.outer_copy(shift).wait_recv()
            self.total[...] += self.from_outer[shift - 1].astype(F32)

    def drain(self):
        self.inner_copy(0).wait_send()

        @pl.loop(1, self.place.outer_size)
        def _(shift):
            self.inner_copy(shift).wait_send()
            self.outer_copy(shift).wait_send()


def backward_kernel(
    dp_size,
    cotangent,
    attn_gain,
    ffn_gain,
    mixer,
    tokens,
    tables,
    attn_full,
    gate_full,
    up_full,
    down_full,
    normed,
    ffn_all,
    cot_all,
    gate_slope,
    up_slope,
    hidden,
    grad_down,
    query,
    key,
    value,
    attended,
    proj,
    middle_in,
    mixed,
    grad_tokens,
    gain_sums,
    attn_total,
    gate_total,
    up_total,
    down_total,
    mid_all,
    gate_part,
    up_part,
    down_kept,
    attn_inner,
    gate_inner,
    up_inner,
    down_inner,
    attn_outer,
    gate_outer,
    up_outer,
    down_outer,
    staged,
    part_twin,
    part_across,
    out_twin,
    out_across,
    middle,
    gain_parts,
    gain_group,
    gain_dp,
    outer_send,
    outer_recv,
    inner_send,
    inner_recv,
    group_send,
    group_recv,
    gain_send,
    gain_recv,
    local_sems,
    tile_sems,
):
    place = Place(dp_size)
    micro_count = cotangent.shape[0]
    length = mid_all.shape[1]
    width = mid_all.shape[2]
    hidden_width = gate_full.shape[1]
    attn_width = attn_full.shape[1]
    block_count = length // TILE
    outer_size = place.outer_size
    group_sems = (group_send, group_recv)
    outer_sems = (outer_send, outer_recv)
    inner_sems = (inner_send, inner_recv)
    own = tile(place.tensor)
    place.greet(True)
    counter = []

    def load(src, dst):
        copy = pltpu.make_async_copy(src, dst, local_sems.at[len(counter)])
        counter.append(copy)
        copy.start()
        return copy

    down_s = Shares(place, grad_down, down_kept, down_inner, down_outer, down_total, outer_sems, inner_sems, 3)
    gate_s = Shares(place, gate_part, None, gate_inner, gate_outer, gate_total, outer_sems, inner_sems, 1)
    up_s = Shares(place, up_part, None, up_inner, up_outer, up_total, outer_sems, inner_sems, 2)
    mid_g = [Gather(place, mid_all, m, group_sems, 3 * m) for m in range(micro_count)]

    def twin_copy(kind, m, half):
        from_twin = (part_twin, out_twin, part_twin)[kind]
        return place.copy(
            staged.at[m, half],
            from_twin.at[m, half],
            group_sems,
            6 + 6 * kind + 3 * m + half,
            tensor=place.twin,
        )

    def across_copy(kind, m):
        from_across = (part_across, out_across, part_across)[kind]
        return place.copy(
            staged.at[m, 2], from_across.at[m], group_sems, 6 + 6 * kind + 3 * m + 2, tensor=place.across
        )

    def block_of(step):
        side = jnp.where(step < 2, 1 - place.side, place.side)
        core = jnp.where(lax.rem(step, 2) == 0, 1 - place.core, place.core)
        return side * 2 + core

    def hand_out(kind, m, step, values):
        from_twin = (part_twin, out_twin, part_twin)[kind]
        half = step // 2

        @pl.when(lax.rem(step, 2) == 0)
        def _():
            staged[m, half] = values.astype(BF16)
            twin_copy(kind, m, half).start()

        @pl.when(step == 1)
        def _():
            twin_copy(kind, m, 0).wait_recv()
            staged[m, 2] = (values + from_twin[m, 0].astype(F32)).astype(BF16)
            across_copy(kind, m).start()

        @pl.when(step == 3)
        def _():
            staged[m, 3] = values.astype(BF16)

    def collect(kind, m):
        from_twin = (part_twin, out_twin, part_twin)[kind]
        from_across = (part_across, out_across, part_across)[kind]
        twin_copy(kind, m, 1).wait_recv()
        across_copy(kind, m).wait_recv()
        return staged[m, 3].astype(F32) + from_twin[m, 1].astype(F32) + from_across[m].astype(F32)

    def drain(kind, m):
        twin_copy(kind, m, 0).wait_send()
        twin_copy(kind, m, 1).wait_send()
        across_copy(kind, m).wait_send()

    gain_parts[...] = jnp.zeros_like(gain_parts)

    def leave_ffn(m):
        upstream = collect(0, m)
        back, term = norm_rows_back(middle[m], ffn_gain[...], upstream)
        grad = cotangent[m].astype(F32) + back
        grad_tokens[m] = grad
        mid_all[m, own] = grad.astype(BF16)
        mid_g[m].start()
        gain_parts[1:2, :] += term

    down_s.give()
    middle_load = load(middle_in, middle)

    @pl.loop(0, outer_size)
    def _(shift):
        pltpu.make_async_copy(
            down_s.at(place.ahead(shift)), down_kept.at[shift], tile_sems.at[4, 0]
        ).start()
        pltpu.make_async_copy(
            down_s.at(place.ahead(shift)), down_kept.at[shift], tile_sems.at[4, 0]
        ).wait()

    def ffn_phase(gate_w, up_w, down_w, gate_grad, up_grad, rows_buf, hidden_buf, ffn_cols):
        loads = [load(down_full, down_w)]

        def rows_copy(index, slot):
            m = index // block_count
            rows = tile(block_of(lax.rem(index, block_count)))
            return pltpu.make_async_copy(cot_all.at[m, rows], rows_buf.at[slot], tile_sems.at[0, slot])

        def hidden_copy(index, slot):
            m = index // block_count
            rows = tile(block_of(lax.rem(index, block_count)))
            return pltpu.make_async_copy(hidden.at[m, rows], hidden_buf.at[slot], tile_sems.at[1, slot])

        rows_copy(0, 0).start()
        loads += [load(gate_slope.at[0], gate_grad.at[0]), load(up_slope.at[0], up_grad.at[0])]
        loads += [load(gate_full, gate_w), load(up_full, up_w)]
        loads += [load(gate_slope.at[1], gate_grad.at[1]), load(up_slope.at[1], up_grad.at[1])]
        for copy in loads:
            copy.wait()
        middle_load.wait()
        tile_count = micro_count * block_count

        @pl.loop(0, tile_count)
        def _(index):
            m = index // block_count
            step = lax.rem(index, block_count)
            rows = tile(block_of(step))
            slot = lax.rem(index, 2)

            @pl.when(index + 1 < tile_count)
            def _():
                rows_copy(index + 1, 1 - slot).start()

            rows_copy(index, slot).wait()
            hidden_grad = nn(rows_buf[slot], down_w[...])
            gate_low = (hidden_grad * gate_grad[m, rows].astype(F32)).astype(BF16)
            up_low = (hidden_grad * up_grad[m, rows].astype(F32)).astype(BF16)
            gate_grad[m, rows] = gate_low
            up_grad[m, rows] = up_low
            hand_out(0, m, step, nt(gate_low, gate_w[...]) + nt(up_low, up_w[...]))

            @pl.when(index == block_count + 2)
            def _():
                leave_ffn(0)

            @pl.when((index >= block_count) & (index < block_count + outer_size - 1))
            def _():
                down_s.turn(index - block_count + 1, index - block_count + 2)

        if outer_size - 1 > block_count:
            down_s.turn(block_count + 1, outer_size)

        def cols_copy(index, slot):
            block = lax.rem(index, block_count)
            return pltpu.make_async_copy(
                ffn_all.at[:, :, tile(block)], ffn_cols.at[slot], tile_sems.at[2, slot]
            )

        cols_copy(0, 0).start()
        down_s.keep()
        for piece, grads, shares in ((gate_part, gate_grad, gate_s), (up_part, up_grad, up_s)):

            @pl.loop(0, block_count)
            def _(block):
                slot = lax.rem(block, 2)
                cols_copy(block, slot).wait()
                cols_copy(block + 1, 1 - slot).start()
                piece[tile(block)] = (
                    tn(ffn_cols[slot, 0], grads[0]) + tn(ffn_cols[slot, 1], grads[1])
                ).astype(BF16)

            shares.give()
        cols_copy(0, 0).wait()
        mid_g[0].relay()
        hidden_copy(0, 0).start()
        leave_ffn(1)
        down_s.finish()

        @pl.loop(0, tile_count)
        def _(index):
            m = index // block_count
            step = lax.rem(index, block_count)
            slot = lax.rem(index, 2)

            @pl.when(index + 1 < tile_count)
            def _():
                hidden_copy(index + 1, 1 - slot).start()

            hidden_copy(index, slot).wait()

            @pl.when(step == 0)
            def _():
                drain(0, m)

            hand_out(1, m, step, nt(hidden_buf[slot], down_w[...]))

        gate_s.turn(1, outer_size)

    pl.run_scoped(
        ffn_phase,
        pltpu.VMEM((width, hidden_width), BF16),
        pltpu.VMEM((width, hidden_width), BF16),
        pltpu.VMEM((width, hidden_width), BF16),
        pltpu.VMEM((micro_count, length, hidden_width), BF16),
        pltpu.VMEM((micro_count, length, hidden_width), BF16),
        pltpu.VMEM((2, TILE, width), BF16),
        pltpu.VMEM((2, TILE, hidden_width), BF16),
        pltpu.VMEM((2, micro_count, length, TILE), BF16),
    )

    def attn_phase(
        attn_w, toks, tabs, norm_cols, att, qry, ky, val, prj, grad_att, grad_q, grad_k, grad_v, grad_qkv, attn_part
    ):
        attn_s = Shares(place, attn_part, None, attn_inner, attn_outer, attn_total, outer_sems, inner_sems, 0)
        lane = lax.broadcasted_iota(jnp.int32, (TILE, 128), 1)
        front = lane < 64
        place_in = lax.rem(lane, 64)
        later = lax.broadcasted_iota(jnp.int32, (TILE, TILE), 0) > lax.broadcasted_iota(
            jnp.int32, (TILE, TILE), 1
        )
        causal = jnp.where(later, APART, 0.0)
        small = mixer[0:128, 0:128]
        loads = [load(attn_full, attn_w)]

        def micro_loads(m):
            return [
                load(attended.at[m], att.at[m]),
                load(value.at[m], val),
                load(key.at[m], ky),
                load(query.at[m], qry),
                load(proj.at[m], prj),
            ]

        ready = [micro_loads(0)]
        loads.append(load(tables, tabs))
        others = [load(tokens, toks)]

        def attend_back(m):
            for copy in ready[m]:
                copy.wait()

            @pl.loop(0, block_count)
            def _(block):
                rows = tile(block)
                low = nn(mid_all[m, rows], attn_w[:, 512:768]).astype(BF16)
                for group in range(2):
                    part = low[:, 128 * group : 128 * group + 128]
                    both = part.astype(F32) * att[m, group, rows].astype(F32)
                    shift = head_mean(both, small) * -64.0
                    high = shift.astype(BF16)
                    rest = shift - high.astype(F32)
                    mid = rest.astype(BF16)
                    last = (rest - mid.astype(F32)).astype(BF16)
                    marks = jnp.where(
                        place_in == 0,
                        high.astype(F32),
                        jnp.where(
                            place_in == 1,
                            mid.astype(F32),
                            jnp.where(place_in == 2, last.astype(F32), 0.0),
                        ),
                    )
                    grad_att[group, rows, 0:128] = part
                    grad_att[group, rows, 128:256] = marks.astype(BF16)

            @pl.loop(0, 2)
            def _(group):
                for block in range(block_count):
                    rows = slice(block * TILE, (block + 1) * TILE)
                    spans = [(rows, True)]
                    if block + 1 < block_count:
                        spans.append((slice((block + 1) * TILE, length), False))
                    sums_k = []
                    sums_v = []
                    for head in range(2):
                        key_block = ky[group, head, rows]
                        value_block = val[group, head, rows]
                        sum_k = None
                        sum_v = None
                        for span, masked in spans:
                            query_span = qry[group, span]
                            grad_span = grad_att[group, span]
                            scores = nt(key_block, query_span)
                            if masked:
                                scores = scores + causal
                            probs = jnp.exp2(scores)
                            score_grad = (probs * nt(value_block, grad_span)).astype(BF16)
                            probs_low = probs.astype(BF16)
                            part_v = nn(probs_low, grad_span[:, 0:128])
                            part_k = nn(score_grad, query_span[:, 0:128])
                            sum_v = part_v if sum_v is None else sum_v + part_v
                            sum_k = part_k if sum_k is None else sum_k + part_k
                            part_q = tn(score_grad, key_block[:, 0:128])
                            if block == 0 and head == 0:
                                grad_q[group, span] = part_q
                            else:
                                grad_q[group, span] += part_q
                        sums_k.append(sum_k)
                        sums_v.append(sum_v)
                    both_k = jnp.where(front, sums_k[0], sums_k[1])
                    both_v = jnp.where(front, sums_v[0], sums_v[1])
                    grad_k[group, rows] = both_k + pltpu.roll(both_k, 64, 1)
                    grad_v[group, rows] = both_v + pltpu.roll(both_v, 64, 1)

            def normalize_back(grads, values, cosine, sine):
                scaled = grads * LN2
                weighted = scaled * cosine + swap_halves(scaled * sine)
                inverse = lax.rsqrt(head_mean(values * values, small) + NORM_EPS)
                unit = values * inverse
                both = weighted * unit
                back = inverse * (weighted - unit * head_mean(both, small))
                return back.astype(BF16), jnp.sum(both, axis=0, keepdims=True)

            @pl.loop(0, block_count)
            def _(block):
                rows = tile(block)
                cosine, sine = tabs[0, rows], tabs[1, rows]
                for group in range(2):
                    lanes = slice(128 * group, 128 * group + 128)
                    back, term = normalize_back(grad_q[group, rows], prj[rows, lanes], cosine, sine)
                    grad_qkv[m, rows, lanes] = back
                    gain_parts[2:3, 0:128] += term
                back, term = normalize_back(
                    jnp.where(front, grad_k[0, rows], grad_k[1, rows]),
                    prj[rows, 256:384],
                    tabs[2, rows],
                    tabs[3, rows],
                )
                grad_qkv[m, rows, 256:384] = back
                gain_parts[2:3, 128:256] += term
                grad_qkv[m, rows, 384:512] = jnp.where(
                    front, grad_v[0, rows], grad_v[1, rows]
                ).astype(BF16)

            leave_out(m)
            drain(1, m)

            @pl.loop(0, block_count)
            def _(step):
                rows = tile(block_of(step))
                hand_out(2, m, step, nt(grad_qkv[m, rows], attn_w[:, 0:512]))

        def leave_out(m):
            mixed[m] = (middle[m] + collect(1, m)).astype(BF16)

        def leave_attn(m):
            upstream = collect(2, m)
            back, term = norm_rows_back(toks[m].astype(F32), attn_gain[...], upstream)
            grad_tokens[m] += back
            gain_parts[0:1, :] += term

        mid_g[0].finish()
        for copy in loads:
            copy.wait()
        attend_back(0)
        ready.append(micro_loads(1))
        mid_g[1].relay()
        gate_s.keep()
        up_s.turn(1, outer_size)
        gate_s.finish()
        mid_g[1].finish()
        attend_back(1)
        for copy in others:
            copy.wait()

        def cols_copy(block, slot):
            return pltpu.make_async_copy(
                normed.at[:, :, tile(lax.rem(block, block_count))], norm_cols.at[slot], tile_sems.at[3, slot]
            )

        cols_copy(0, 0).start()

        @pl.loop(0, block_count)
        def _(block):
            columns = tile(block)
            slot = lax.rem(block, 2)
            cols_copy(block, slot).wait()
            cols_copy(block + 1, 1 - slot).start()
            attn_part[columns, 0:512] = (
                tn(norm_cols[slot, 0], grad_qkv[0]) + tn(norm_cols[slot, 1], grad_qkv[1])
            ).astype(BF16)
            total = jnp.zeros((TILE, 256), F32)
            for m in range(micro_count):
                heads = jnp.concatenate([att[m, 0], att[m, 1]], axis=1)
                total = total + tn(mid_all[m, :, columns], heads)
            attn_part[columns, 512:768] = total.astype(BF16)

        cols_copy(0, 0).wait()
        attn_s.give()
        up_s.keep()
        leave_attn(0)
        up_s.finish()
        attn_s.turn(1, outer_size)
        leave_attn(1)

        def group_gain(shift):
            return place.copy(
                gain_parts,
                gain_group.at[shift - 1],
                (gain_send, gain_recv),
                shift - 1,
                tensor=lax.rem(place.tensor + shift, 4),
            )

        for shift in range(1, 4):
            group_gain(shift).start()
        attn_s.keep()
        for shift in range(1, 4):
            group_gain(shift).wait_recv()
        gain_dp[0] = gain_parts[...] + gain_group[0] + gain_group[1] + gain_group[2]

        def dp_gain(shift):
            return place.copy(
                gain_dp.at[0],
                gain_dp.at[shift],
                (gain_send, gain_recv),
                2 + shift,
                dp=lax.rem(place.dp + shift, dp_size),
            )

        @pl.loop(1, dp_size)
        def _(shift):
            dp_gain(shift).start()

        attn_s.finish()
        gain_sums[...] = gain_dp[0]

        @pl.loop(1, dp_size)
        def _(shift):
            dp_gain(shift).wait_recv()
            gain_sums[...] += gain_dp[shift]

        for shift in range(1, 4):
            group_gain(shift).wait_send()

        @pl.loop(1, dp_size)
        def _(shift):
            dp_gain(shift).wait_send()

        attn_s.drain()

    pl.run_scoped(
        attn_phase,
        pltpu.VMEM((width, attn_width), BF16),
        pltpu.VMEM(tokens.shape, BF16),
        pltpu.VMEM(tables.shape, F32),
        pltpu.VMEM((2, micro_count, length, TILE), BF16),
        pltpu.VMEM((micro_count, 2, length, 128), BF16),
        pltpu.VMEM((2, length, 256), BF16),
        pltpu.VMEM((2, 2, length, 256), BF16),
        pltpu.VMEM((2, 2, length, 256), BF16),
        pltpu.VMEM((length, 384), F32),
        pltpu.VMEM((2, length, 256), BF16),
        pltpu.VMEM((2, length, 128), F32),
        pltpu.VMEM((2, length, 128), F32),
        pltpu.VMEM((2, length, 128), F32),
        pltpu.VMEM((micro_count, length, 512), BF16),
        pltpu.VMEM((width, attn_width), BF16),
    )
    for shares in (down_s, gate_s, up_s):
        shares.drain()
    for m in range(micro_count):
        mid_g[m].drain()
        drain(2, m)


def backward(dp_size, cotangent, attn_gain, ffn_gain, mixer, tokens, tables, saved):
    micro, rows, width = tokens.shape
    length = tables.shape[1]
    attn_width = saved[0].shape[1]
    hidden_width = saved[1].shape[1]
    outer_size = dp_size // 2
    share = width // dp_size
    whole = pl.BlockSpec(memory_space=pltpu.VMEM)
    anywhere = pl.BlockSpec(memory_space=pl.ANY)
    shape = jax.ShapeDtypeStruct
    widths = (attn_width, hidden_width, hidden_width, hidden_width)
    out_shape = [
        shape((micro, rows, width), BF16),
        shape((micro, rows, width), F32),
        shape((8, width), F32),
    ] + [shape((share, w), F32) for w in widths]
    scratch = (
        [
            pltpu.VMEM((micro, length, width), BF16),
            pltpu.VMEM((width, hidden_width), BF16),
            pltpu.VMEM((width, hidden_width), BF16),
            pltpu.VMEM((outer_size, share, hidden_width), BF16),
        ]
        + [pltpu.VMEM((outer_size, share, w), BF16) for w in widths]
        + [pltpu.VMEM((outer_size - 1, share, w), BF16) for w in widths]
        + [
            pltpu.VMEM((micro, 4, rows, width), BF16),
            pltpu.VMEM((micro, 2, rows, width), BF16),
            pltpu.VMEM((micro, rows, width), BF16),
            pltpu.VMEM((micro, 2, rows, width), BF16),
            pltpu.VMEM((micro, rows, width), BF16),
            pltpu.VMEM((micro, rows, width), F32),
            pltpu.VMEM((8, width), F32),
            pltpu.VMEM((3, 8, width), F32),
            pltpu.VMEM((dp_size, 8, width), F32),
        ]
        + [pltpu.SemaphoreType.DMA((4, outer_size))] * 4
        + [pltpu.SemaphoreType.DMA((24,))] * 2
        + [pltpu.SemaphoreType.DMA((dp_size + 2,))] * 2
        + [pltpu.SemaphoreType.DMA((32,)), pltpu.SemaphoreType.DMA((5, 2))]
    )
    return pl.pallas_call(
        functools.partial(backward_kernel, dp_size),
        out_shape=out_shape,
        in_specs=[whole] * 4 + [anywhere] * (2 + len(saved)),
        out_specs=[whole] * len(out_shape),
        scratch_shapes=scratch,
        compiler_params=pltpu.CompilerParams(
            collective_id=1, has_side_effects=True, vmem_limit_bytes=VMEM_LIMIT
        ),
        name="backward_pass",
    )(cotangent, attn_gain, ffn_gain, mixer, tokens, tables, *saved)


def rope_tables(length, gain, scale):
    freq_index = jnp.arange(DH // 2, dtype=F32)
    inverse_freq = ROPE_BASE ** (-2.0 * freq_index / DH)
    angles = jnp.arange(length, dtype=F32)[:, None] * inverse_freq[None, :]
    cosine, sine = jnp.cos(angles) * scale, jnp.sin(angles) * scale
    front, back = gain[: DH // 2], gain[DH // 2 :]
    straight = jnp.concatenate([cosine * front, cosine * back], axis=1)
    crossed = jnp.concatenate([-sine * back, sine * front], axis=1)
    return jnp.stack([jnp.tile(straight, (1, 2)), jnp.tile(crossed, (1, 2))])


def segment_marks(segments):
    lane = jnp.arange(128)
    ids = segments[..., None] == (lane - 8)
    used = (lane >= 8) & (lane < 11)
    query_marks = jnp.where(ids, 1.0, 0.0).astype(BF16)
    base = jnp.where(used & ~ids, APART, 0.0)
    first = jnp.where(lane < 3, 1.0, base)
    second = jnp.where((lane >= 64) & (lane < 67), 1.0, base)
    return query_marks, jnp.stack([first, second]).astype(BF16)


def shards(
    dp_size,
    tokens,
    segment_ids,
    attn_gain,
    query_gain,
    key_gain,
    w_query,
    w_key,
    w_value,
    w_out,
    ffn_gain,
    w_gate,
    w_up,
    w_down,
    cotangent,
):
    length = segment_ids.shape[2]
    query_end = w_query.shape[1]
    key_end = query_end + w_key.shape[1]
    value_end = key_end + w_value.shape[1]
    tables = jnp.concatenate(
        [
            rope_tables(length, query_gain, DH**-0.5 / LN2),
            rope_tables(length, key_gain, 1.0),
        ]
    )
    query_marks, key_marks = segment_marks(segment_ids[:, 0])
    head = jnp.arange(256) // DH
    mixer = jnp.where(head[:, None] == head[None, :], 1.0 / DH, 0.0).astype(BF16)
    pieces = (
        jnp.concatenate([w_query, w_key, w_value, w_out.T], axis=1),
        w_gate,
        w_up,
        w_down.T,
    )
    own_tokens, own_cot = tokens[:, 0], cotangent[:, 0]
    attn_row, ffn_row = attn_gain[None], ffn_gain[None]
    saved = forward(
        dp_size, own_tokens, own_cot, pieces, attn_row, ffn_row, tables, query_marks, key_marks, mixer
    )
    mixed, grad_tokens, gains, attn_sum, gate_sum, up_sum, down_sum = backward(
        dp_size, own_cot, attn_row, ffn_row, mixer, own_tokens, tables, saved
    )
    query_term = gains[2, :128].reshape(2, DH).sum(0) / query_gain
    key_term = gains[2, 128:256].reshape(2, DH).sum(0) / key_gain
    return (
        mixed[:, None],
        grad_tokens[:, None],
        gains[0],
        query_term,
        key_term,
        attn_sum[:, :query_end],
        attn_sum[:, query_end:key_end],
        attn_sum[:, key_end:value_end],
        attn_sum[:, value_end:].T,
        gains[1],
        gate_sum,
        up_sum,
        down_sum.T,
    )


def solution(mesh):
    sequence = P(None, "dp", "tensor", None)
    rows = P("dp", "tensor")
    columns = P("tensor", "dp")
    return jax.shard_map(
        functools.partial(shards, mesh.shape["dp"]),
        mesh=mesh,
        in_specs=(sequence, P(None, "dp", None), P(), P(), P(), rows, rows, rows, columns, P(), rows, rows, columns, sequence),
        out_specs=(sequence, sequence, P(), P(), P(), rows, rows, rows, columns, P(), rows, rows, columns),
        check_vma=False,
    )
```

```python
import functools
import math

import jax
import jax.numpy as jnp
import numpy as np
from jax import lax
from jax.experimental import pallas as pl
from jax.experimental.pallas import tpu as pltpu
from jax.sharding import PartitionSpec as P

MESH = pl.DeviceIdType.MESH
VMEM_LIMIT = 67000000
NORM_EPS = 1e-05
ROPE_BASE = 1000000.0
DH = 64
TILE = 256
LN2 = math.log(2.0)
APART = -32768.0
BF16 = jnp.bfloat16
F32 = jnp.float32


def nn(left, right):
    return lax.dot_general(left, right, (((1,), (0,)), ((), ())), preferred_element_type=F32)


def nt(left, right):
    return lax.dot_general(left, right, (((1,), (1,)), ((), ())), preferred_element_type=F32)


def tn(left, right):
    return lax.dot_general(left, right, (((0,), (0,)), ((), ())), preferred_element_type=F32)


def tile(index, size=TILE):
    return pl.ds(pl.multiple_of(index * size, size), size)


def rem(value, divisor):
    return value % divisor if isinstance(value, int) else lax.rem(value, divisor)


def low_parts(values):
    high = values.astype(BF16)
    return high, (values - high.astype(F32)).astype(BF16)


def head_mean(values, mixer):
    high, rest = low_parts(values)
    return nn(high, mixer) + nn(rest, mixer)


def swap_halves(values):
    lane = lax.broadcasted_iota(jnp.int32, values.shape, 1)
    ahead = pltpu.roll(values, 96, 1)
    behind = pltpu.roll(values, 32, 1)
    return jnp.where(lax.rem(lane, 64) < 32, ahead, behind)


def norm_rows(values, gain):
    inverse = lax.rsqrt(jnp.mean(values * values, axis=-1, keepdims=True) + NORM_EPS)
    return values * inverse * gain


def norm_rows_back(values, gain, upstream):
    inverse = lax.rsqrt(jnp.mean(values * values, axis=-1, keepdims=True) + NORM_EPS)
    scaled = values * inverse
    weighted = upstream * gain
    back = inverse * (weighted - scaled * jnp.mean(weighted * scaled, axis=-1, keepdims=True))
    return back, jnp.sum(upstream * scaled, axis=0, keepdims=True)


class Place:
    def __init__(self, dp_size):
        self.dp_size = dp_size
        self.dp = lax.axis_index("dp")
        self.tensor = lax.axis_index("tensor")
        self.outer_size = dp_size // 2
        self.outer = self.dp // 2
        self.inner = lax.rem(self.dp, 2)
        self.other = self.outer * 2 + 1 - self.inner
        self.side = self.tensor // 2
        self.core = lax.rem(self.tensor, 2)
        self.across = (1 - self.side) * 2 + self.core
        self.twin = self.side * 2 + 1 - self.core

    def ahead(self, shift, inner=None):
        inner = self.inner if inner is None else inner
        return lax.rem(self.outer + shift, self.outer_size) * 2 + inner

    def behind(self, shift):
        return lax.rem(self.outer - shift + self.outer_size, self.outer_size) * 2 + self.inner

    def block(self, step):
        side = 1 - self.side if step < 2 else self.side
        core = 1 - self.core if step % 2 == 0 else self.core
        return side * 2 + core

    def copy(self, src, dst, sems, index, dp=None, tensor=None):
        return pltpu.make_async_remote_copy(
            src_ref=src,
            dst_ref=dst,
            send_sem=sems[0].at[index],
            recv_sem=sems[1].at[index],
            device_id=(
                self.dp if dp is None else dp,
                self.tensor if tensor is None else tensor,
            ),
            device_id_type=MESH,
        )

    def greet(self, everyone):
        barrier = pltpu.get_barrier_semaphore()

        def signal(dp, tensor):
            pl.semaphore_signal(barrier, inc=1, device_id=(dp, tensor), device_id_type=MESH)

        if everyone:

            @pl.loop(1, self.dp_size)
            def _(shift):
                signal(lax.rem(self.dp + shift, self.dp_size), self.tensor)

            for shift in range(1, 4):
                signal(self.dp, lax.rem(self.tensor + shift, 4))
            pl.semaphore_wait(barrier, self.dp_size + 2)
        else:

            @pl.loop(1, self.outer_size)
            def _(shift):
                signal(self.ahead(shift), self.tensor)

            signal(self.other, self.tensor)
            signal(self.dp, self.across)
            signal(self.dp, self.twin)
            pl.semaphore_wait(barrier, self.outer_size + 2)


def pack_gains(packed, terms):
    part = 0
    for row, width in enumerate((terms.shape[1], terms.shape[1], 256)):
        for start in range(0, width, 128):
            packed[part // 3 : part // 3 + 1, 128 * (part % 3) : 128 * (part % 3) + 128] = terms[
                row : row + 1, start : start + 128
            ]
            part += 1


class Gather:
    def __init__(self, place, ref, micro, sems, index, source=None):
        own = ref.at[micro, tile(place.tensor)]
        source = own if source is None else source
        theirs = ref.at[micro, tile(place.across)]
        self.to_across = place.copy(source, own, sems, index, tensor=place.across)
        self.to_twin = place.copy(source, own, sems, index + 1, tensor=place.twin)
        self.on_to_twin = place.copy(theirs, theirs, sems, index + 2, tensor=place.twin)

    def start(self):
        self.to_across.start()
        self.to_twin.start()

    def relay(self):
        self.to_across.wait_recv()
        self.on_to_twin.start()

    def finish(self):
        self.to_twin.wait_recv()
        self.on_to_twin.wait_recv()

    def drain(self):
        self.to_across.wait_send()
        self.to_twin.wait_send()
        self.on_to_twin.wait_send()


class Scatter:
    def __init__(self, place, staged, from_twin, from_across, sems, index):
        self.place = place
        self.staged = staged
        self.from_twin = from_twin
        self.from_across = from_across
        self.sems = sems
        self.index = index

    def twin(self, half):
        return self.place.copy(
            self.staged.at[half],
            self.from_twin.at[half],
            self.sems,
            self.index + half,
            tensor=self.place.twin,
        )

    def crossing(self):
        return self.place.copy(
            self.staged.at[2],
            self.from_across,
            self.sems,
            self.index + 2,
            tensor=self.place.across,
        )

    def give(self, step, values):
        if step == 0 or step == 2:
            half = step // 2
            self.staged[half] = values.astype(BF16)
            self.twin(half).start()
        elif step == 1:
            self.twin(0).wait_recv()
            self.staged[2] = (values + self.from_twin[0].astype(F32)).astype(BF16)
            self.crossing().start()

    def result(self, values):
        self.twin(1).wait_recv()
        self.crossing().wait_recv()
        return values + self.from_twin[1].astype(F32) + self.from_across[...].astype(F32)

    def drain(self):
        self.twin(0).wait_send()
        self.twin(1).wait_send()
        self.crossing().wait_send()


def fill_mixer(mixer):
    row = lax.broadcasted_iota(jnp.int32, mixer.shape, 0) // DH
    column = lax.broadcasted_iota(jnp.int32, mixer.shape, 1) // DH
    mixer[...] = jnp.where(row == column, 1.0 / DH, 0.0).astype(BF16)


class Weights:
    def __init__(self, place, shard, full, outer_sems, inner_sems, piece):
        self.place = place
        self.shard = shard
        self.full = full
        self.outer_sems = outer_sems
        self.inner_sems = inner_sems
        self.piece = piece
        self.rows = shard.shape[0]

    def at(self, index):
        return self.full.at[pl.ds(pl.multiple_of(index * self.rows, self.rows), self.rows), :]

    def outer_copy(self, shift):
        place = self.place
        return place.copy(
            self.shard,
            self.at(place.dp),
            self.outer_sems,
            (self.piece, shift),
            dp=place.ahead(shift),
        )

    def inner_copy(self, shift):
        place = self.place
        rows = self.at(place.behind(shift))
        return place.copy(rows, rows, self.inner_sems, (self.piece, shift), dp=place.other)

    def own_copy(self):
        place = self.place
        return place.copy(
            self.shard, self.at(place.dp), self.inner_sems, (self.piece, 0), dp=place.other
        )

    def send_outer(self):
        @pl.loop(1, self.place.outer_size)
        def _(shift):
            self.outer_copy(shift).start()

    def send_inner(self):
        self.own_copy().start()

    def relay(self, first, last):
        @pl.loop(first, last)
        def _(shift):
            self.outer_copy(shift).wait_recv()
            self.inner_copy(shift).start()

    def finish(self):
        @pl.loop(0, self.place.outer_size)
        def _(shift):
            self.inner_copy(shift).wait_recv()

    def drain(self):
        self.own_copy().wait_send()

        @pl.loop(1, self.place.outer_size)
        def _(shift):
            self.outer_copy(shift).wait_send()
            self.inner_copy(shift).wait_send()


def rotation_angles(length):
    frequency = ROPE_BASE ** (-2.0 * (np.arange(128) % (DH // 2)) / DH)
    steps = np.arange(8) * TILE if length <= 8 * TILE else np.arange(0, length, TILE)
    positions = np.concatenate([np.arange(TILE), steps])
    turns = positions[:, None] * frequency[None, :]
    return jnp.asarray(np.stack([np.cos(turns), np.sin(turns)]).astype(np.float32))


def forward_kernel(
    dp_size,
    turned,
    tokens,
    cotangent,
    segments,
    w_query,
    w_key,
    w_value,
    w_out,
    gate_shard,
    up_shard,
    w_down,
    attn_gain,
    ffn_gain,
    query_gain,
    key_gain,
    angles,
    out_qkv_full,
    out_back_full,
    out_gate_full,
    out_up_full,
    out_down_full,
    out_normed,
    out_ffn,
    out_cot,
    out_gate_slope,
    out_up_slope,
    out_hidden,
    out_grad_down,
    out_query,
    out_key,
    out_value,
    out_attended,
    out_proj,
    out_middle,
    out_tables,
    qkv_shard,
    back_shard,
    down_shard,
    tables,
    query_marks,
    key_marks,
    mixer,
    normed,
    ffn_all,
    cot_all,
    qkv_full,
    back_full,
    gate_full,
    up_full,
    slopes,
    hidden,
    grad_down,
    query,
    key,
    value,
    attended,
    proj,
    middle,
    staged,
    from_twin,
    from_across,
    outer_send,
    outer_recv,
    inner_send,
    inner_recv,
    group_send,
    group_recv,
    local_sems,
    slope_sems,
):
    place = Place(dp_size)
    micro_count = tokens.shape[0]
    block_count = normed.shape[1] // TILE
    outer_size = place.outer_size
    group_sems = (group_send, group_recv)
    outer_sems = (outer_send, outer_recv)
    inner_sems = (inner_send, inner_recv)
    own = tile(place.tensor)
    first_cut = 1 + (outer_size - 1) // 3
    second_cut = 1 + 2 * (outer_size - 1) // 3
    qkv_w = Weights(place, qkv_shard, qkv_full, outer_sems, inner_sems, 0)
    back_w = Weights(place, back_shard, back_full, outer_sems, inner_sems, 1)
    gate_w = Weights(place, gate_shard, gate_full, outer_sems, inner_sems, 2)
    up_w = Weights(place, up_shard, up_full, outer_sems, inner_sems, 3)
    down_w = Weights(place, down_shard, out_down_full, outer_sems, inner_sems, 4)
    normed_g = [Gather(place, normed, m, group_sems, 3 * m) for m in range(micro_count)]
    cot_g = [
        Gather(place, cot_all, m, group_sems, 6 + 3 * m, cotangent.at[m])
        for m in range(micro_count)
    ]
    ffn_g = [Gather(place, ffn_all, m, group_sems, 12 + 3 * m) for m in range(micro_count)]

    def branch_s(m):
        return Scatter(
            place, staged.at[m], from_twin.at[m], from_across.at[m], group_sems, 18 + 3 * m
        )

    saves = []

    def save(src, dst):
        copy = pltpu.make_async_copy(src, dst, local_sems.at[len(saves)])
        copy.start()
        saves.append(copy)
        return copy

    lane = lax.broadcasted_iota(jnp.int32, (TILE, 128), 1)
    front = lane < 64
    place_in = rem(lane, 64)

    value_end = w_query.shape[1] + w_key.shape[1]
    qkv_shard[:, : w_query.shape[1]] = w_query[...]
    qkv_shard[:, w_query.shape[1] : value_end] = w_key[...]
    qkv_shard[:, value_end:] = w_value[...]
    for m in range(micro_count):
        normed[m, own] = norm_rows(tokens[m].astype(F32), attn_gain[...]).astype(BF16)
    if turned:
        back_shard[...] = w_out[...]
        down_shard[...] = w_down[...]
    else:
        back_shard[...] = w_out[...].T
        down_shard[...] = w_down[...].T
    place.greet(False)
    qkv_w.send_outer()
    qkv_w.send_inner()
    normed_g[0].start()
    normed_g[1].start()
    cot_g[0].start()

    def prepare():
        fill_mixer(mixer)
        sign = jnp.where(place_in < 32, -1.0, 1.0)
        for kind, (gain_ref, scale) in enumerate(((query_gain, DH**-0.5 / LN2), (key_gain, 1.0))):
            gain = jnp.broadcast_to(
                jnp.concatenate([gain_ref[...], gain_ref[...]], axis=1) * scale, (TILE, 128)
            )
            crossed = swap_halves(gain) * sign
            for block in range(block_count):
                rows = slice(block * TILE, (block + 1) * TILE)
                cos_step = angles[0, TILE + block : TILE + block + 1]
                sin_step = angles[1, TILE + block : TILE + block + 1]
                cosine = angles[0, 0:TILE] * cos_step - angles[1, 0:TILE] * sin_step
                sine = angles[1, 0:TILE] * cos_step + angles[0, 0:TILE] * sin_step
                tables[2 * kind, rows] = cosine * gain
                tables[2 * kind + 1, rows] = sine * crossed
        row = lax.broadcasted_iota(jnp.int32, (16, 128), 0)
        mark_lane = lax.broadcasted_iota(jnp.int32, (16, 128), 1)
        spread = jnp.where(mark_lane == row + 8, 1.0, 0.0).astype(BF16)
        used = (lane >= 8) & (lane < 11)
        for m in range(micro_count):
            for block in range(block_count):
                rows = slice(block * TILE, (block + 1) * TILE)
                ids = jnp.broadcast_to(segments[m : m + 1, rows], (16, TILE))
                match = lax.broadcasted_iota(jnp.int32, (16, TILE), 0) == ids
                marks = tn(jnp.where(match, 1.0, 0.0).astype(BF16), spread)
                query_marks[m, rows] = marks.astype(BF16)
                apart = jnp.where(used, APART * (1.0 - marks), 0.0)
                for head in range(2):
                    chosen = (lane >= 64 * head) & (lane < 64 * head + 3)
                    key_marks[head, m, rows] = jnp.where(chosen, 1.0, apart).astype(BF16)
        qkv_w.at(place.dp)[...] = qkv_shard[...]
        back_w.at(place.dp)[...] = back_shard[...]
        gate_w.at(place.dp)[...] = gate_shard[...]
        up_w.at(place.dp)[...] = up_shard[...]
        for m in range(micro_count):
            cot_all[m, own] = cotangent[m]

    prepare()
    save(down_shard, down_w.at(place.dp))
    save(tables, out_tables)
    qkv_w.relay(1, second_cut)
    back_w.send_outer()
    qkv_w.relay(second_cut, outer_size)
    back_w.send_inner()
    gate_w.send_outer()
    gate_w.send_inner()
    up_w.send_outer()
    down_w.send_outer()

    later = lax.broadcasted_iota(jnp.int32, (TILE, TILE), 1) > lax.broadcasted_iota(
        jnp.int32, (TILE, TILE), 0
    )
    causal = jnp.where(later, APART, 0.0)

    def project(m):
        @pl.loop(0, block_count)
        def _(block):
            rows = tile(block)
            product = nn(normed[m, rows], qkv_full[...])
            proj[m, rows] = product[:, :384]
            heads = product[:, :256]
            inverse = lax.rsqrt(head_mean(heads * heads, mixer[...]) + NORM_EPS)
            for group in range(2):
                lanes = slice(128 * group, 128 * group + 128)
                part = heads[:, lanes]
                turned = part * tables[0, rows] + swap_halves(part) * tables[1, rows]
                query[m, group, rows, 0:128] = (turned * inverse[:, lanes]).astype(BF16)
                query[m, group, rows, 128:256] = query_marks[m, rows]
            part = product[:, 256:384]
            inverse = lax.rsqrt(head_mean(part * part, mixer[0:128, 0:128]) + NORM_EPS)
            turned = (part * tables[2, rows] + swap_halves(part) * tables[3, rows]) * inverse
            moved = pltpu.roll(turned, 64, 1)
            val = product[:, 384:512]
            val_moved = pltpu.roll(val, 64, 1)
            for group in range(2):
                first, second = (turned, moved) if group == 0 else (moved, turned)
                key[m, group, 0, rows, 0:128] = jnp.where(front, first, 0.0).astype(BF16)
                key[m, group, 1, rows, 0:128] = jnp.where(front, 0.0, second).astype(BF16)
                first, second = (val, val_moved) if group == 0 else (val_moved, val)
                value[m, group, 0, rows, 0:128] = jnp.where(front, first, 0.0).astype(BF16)
                value[m, group, 1, rows, 0:128] = jnp.where(front, 0.0, second).astype(BF16)
                for head in range(2):
                    key[m, group, head, rows, 128:256] = key_marks[head, m, rows]
                value[m, group, 0, rows, 128:256] = jnp.where(front, 1.0, 0.0).astype(BF16)
                value[m, group, 1, rows, 128:256] = jnp.where(front, 0.0, 1.0).astype(BF16)

    def attend(m):
        @pl.loop(0, 2)
        def _(group):
            for block in range(block_count):
                rows = slice(block * TILE, (block + 1) * TILE)
                query_block = query[m, group, rows]
                total = jnp.zeros((TILE, 256), F32)
                for head in range(2):
                    if block > 0:
                        before = slice(0, block * TILE)
                        scores = nt(query_block, key[m, group, head, before])
                        weights = jnp.exp2(scores).astype(BF16)
                        total = total + nn(weights, value[m, group, head, before])
                    scores = nt(query_block, key[m, group, head, rows]) + causal
                    weights = jnp.exp2(scores).astype(BF16)
                    total = total + nn(weights, value[m, group, head, rows])
                sums = total[:, 128:256]
                attended[m, group, rows] = (total[:, 0:128] / sums).astype(BF16)
                shift = -jnp.log2(sums)
                high = shift.astype(BF16)
                middle_part = (shift - high.astype(F32)).astype(BF16)
                last = (shift - high.astype(F32) - middle_part.astype(F32)).astype(BF16)
                marks = jnp.where(
                    place_in == 0,
                    high.astype(F32),
                    jnp.where(
                        place_in == 1,
                        middle_part.astype(F32),
                        jnp.where(
                            place_in == 2,
                            last.astype(F32),
                            query_block[:, 128:256].astype(F32),
                        ),
                    ),
                )
                query[m, group, rows, 128:256] = marks.astype(BF16)

    def branch_block(m, step):
        rows = tile(place.block(step))
        heads = jnp.concatenate([attended[m, 0, rows], attended[m, 1, rows]], axis=1)
        return nt(heads, back_full[...])

    def branch(m):
        for step in range(3):
            branch_s(m).give(step, branch_block(m, step))

    def enter_ffn(m):
        total = branch_s(m).result(branch_block(m, 3))
        middle[m] = tokens[m].astype(F32) + total
        save(middle.at[m], out_middle.at[m])
        ffn_all[m, own] = norm_rows(middle[m], ffn_gain[...]).astype(BF16)
        ffn_g[m].start()

    @pl.loop(0, micro_count)
    def _(m):
        @pl.when(m == 0)
        def _():
            normed_g[0].relay()
            normed_g[0].finish()
            qkv_w.finish()

        @pl.when(m == 1)
        def _():
            normed_g[1].finish()

        project(m)

        @pl.when(m == 0)
        def _():
            back_w.relay(1, outer_size)
            up_w.send_inner()

        @pl.when(m == 1)
        def _():
            gate_w.relay(1, first_cut)

        attend(m)

        @pl.when(m == 0)
        def _():
            normed_g[1].relay()
            back_w.finish()

        @pl.when(m == 1)
        def _():
            down_w.send_inner()

        branch(m)

    save(qkv_full, out_qkv_full)
    save(back_full, out_back_full)
    for m in range(micro_count):
        save(query.at[m], out_query.at[m])
        save(key.at[m], out_key.at[m])
        save(value.at[m], out_value.at[m])
        save(attended.at[m], out_attended.at[m])
        save(proj.at[m], out_proj.at[m])
        save(normed.at[m], out_normed.at[m])
    gate_w.relay(first_cut, second_cut)
    cot_g[0].relay()
    gate_w.relay(second_cut, outer_size)
    enter_ffn(0)
    up_w.relay(1, first_cut)
    enter_ffn(1)
    cot_g[1].start()
    up_w.relay(first_cut, second_cut)
    cot_g[0].finish()
    save(cot_all.at[0], out_cot.at[0])
    gate_w.finish()
    save(gate_full, out_gate_full)
    up_w.relay(second_cut, outer_size)
    ffn_g[0].relay()
    ffn_g[0].finish()
    save(ffn_all.at[0], out_ffn.at[0])
    up_w.finish()
    save(up_full, out_up_full)

    def slope_copies(index):
        m = index // block_count
        rows = tile(rem(index, block_count))
        slot = rem(index, 2)
        return [
            pltpu.make_async_copy(
                slopes.at[slot, kind], out.at[m, rows], slope_sems.at[slot, kind]
            )
            for kind, out in enumerate((out_gate_slope, out_up_slope))
        ]

    tile_count = micro_count * block_count

    @pl.loop(0, tile_count)
    def _(index):
        m = index // block_count
        rows = tile(rem(index, block_count))
        slot = rem(index, 2)

        @pl.when(index >= 2)
        def _():
            for copy in slope_copies(index - 2):
                copy.wait()

        @pl.when(index == 2)
        def _():
            down_w.relay(1, first_cut)

        @pl.when(index == block_count)
        def _():
            ffn_g[1].relay()
            ffn_g[1].finish()

        @pl.when(index == block_count + 2)
        def _():
            down_w.relay(first_cut, second_cut)

        gate = nn(ffn_all[m, rows], gate_full[...])
        up = nn(ffn_all[m, rows], up_full[...])
        sig = 1.0 / (1.0 + jnp.exp(-gate))
        act = gate * sig
        hidden[m, rows] = (act * up).astype(BF16)
        slopes[slot, 0] = (up * (sig + act * (1.0 - sig))).astype(BF16)
        slopes[slot, 1] = act.astype(BF16)
        for copy in slope_copies(index):
            copy.start()

    save(ffn_all.at[1], out_ffn.at[1])
    save(hidden, out_hidden)
    for index in (tile_count - 2, tile_count - 1):
        for copy in slope_copies(index):
            copy.wait()
    cot_g[1].relay()
    down_w.relay(second_cut, outer_size)
    cot_g[1].finish()
    save(cot_all.at[1], out_cot.at[1])

    @pl.loop(0, block_count)
    def _(block):
        columns = tile(block)
        grad_down[columns] = (
            tn(cot_all[0, :, columns], hidden[0]) + tn(cot_all[1, :, columns], hidden[1])
        ).astype(BF16)

    save(grad_down, out_grad_down)
    down_w.finish()
    for piece in (qkv_w, back_w, gate_w, up_w, down_w):
        piece.drain()
    for m in range(micro_count):
        normed_g[m].drain()
        cot_g[m].drain()
        ffn_g[m].drain()
        branch_s(m).drain()
    for copy in saves:
        copy.wait()


def forward(dp_size, tokens, cotangent, segments, weights, gains):
    w_query, w_key, w_value, w_out, w_gate, w_up, w_down = weights
    micro, rows, width = tokens.shape
    length = segments.shape[1]
    share, hidden_width = w_gate.shape
    qkv_width = w_query.shape[1] + w_key.shape[1] + w_value.shape[1]
    back_width = w_out.shape[0]
    turned = share % 128 != 0
    if turned:
        w_out, w_down = w_out.T, w_down.T
    outer_size = dp_size // 2
    whole = pl.BlockSpec(memory_space=pltpu.VMEM)
    anywhere = pl.BlockSpec(memory_space=pl.ANY)
    shape = jax.ShapeDtypeStruct
    out_shape = [
        shape((width, qkv_width), BF16),
        shape((width, back_width), BF16),
        shape((width, hidden_width), BF16),
        shape((width, hidden_width), BF16),
        shape((width, hidden_width), BF16),
        shape((micro, length, width), BF16),
        shape((micro, length, width), BF16),
        shape((micro, length, width), BF16),
        shape((micro, length, hidden_width), BF16),
        shape((micro, length, hidden_width), BF16),
        shape((micro, length, hidden_width), BF16),
        shape((width, hidden_width), BF16),
        shape((micro, 2, length, 256), BF16),
        shape((micro, 2, 2, length, 256), BF16),
        shape((micro, 2, 2, length, 256), BF16),
        shape((micro, 2, length, 128), BF16),
        shape((micro, length, 384), F32),
        shape((micro, rows, width), F32),
        shape((4, length, 128), F32),
    ]
    scratch = [
        pltpu.VMEM((share, qkv_width), BF16),
        pltpu.VMEM((share, back_width), BF16),
        pltpu.VMEM((share, hidden_width), BF16),
        pltpu.VMEM((4, length, 128), F32),
        pltpu.VMEM((micro, length, 128), BF16),
        pltpu.VMEM((2, micro, length, 128), BF16),
        pltpu.VMEM((256, 256), BF16),
        pltpu.VMEM((micro, length, width), BF16),
        pltpu.VMEM((micro, length, width), BF16),
        pltpu.VMEM((micro, length, width), BF16),
        pltpu.VMEM((width, qkv_width), BF16),
        pltpu.VMEM((width, back_width), BF16),
        pltpu.VMEM((width, hidden_width), BF16),
        pltpu.VMEM((width, hidden_width), BF16),
        pltpu.VMEM((2, 2, TILE, hidden_width), BF16),
        pltpu.VMEM((micro, length, hidden_width), BF16),
        pltpu.VMEM((width, hidden_width), BF16),
        pltpu.VMEM((micro, 2, length, 256), BF16),
        pltpu.VMEM((micro, 2, 2, length, 256), BF16),
        pltpu.VMEM((micro, 2, 2, length, 256), BF16),
        pltpu.VMEM((micro, 2, length, 128), BF16),
        pltpu.VMEM((micro, length, 384), F32),
        pltpu.VMEM((micro, rows, width), F32),
        pltpu.VMEM((micro, 3, rows, width), BF16),
        pltpu.VMEM((micro, 2, rows, width), BF16),
        pltpu.VMEM((micro, rows, width), BF16),
        pltpu.SemaphoreType.DMA((5, outer_size)),
        pltpu.SemaphoreType.DMA((5, outer_size)),
        pltpu.SemaphoreType.DMA((5, outer_size)),
        pltpu.SemaphoreType.DMA((5, outer_size)),
        pltpu.SemaphoreType.DMA((24,)),
        pltpu.SemaphoreType.DMA((24,)),
        pltpu.SemaphoreType.DMA((32,)),
        pltpu.SemaphoreType.DMA((2, 2)),
    ]
    operands = (
        tokens,
        cotangent,
        segments,
        w_query,
        w_key,
        w_value,
        w_out,
        w_gate,
        w_up,
        w_down,
        *gains,
        rotation_angles(length),
    )
    return pl.pallas_call(
        functools.partial(forward_kernel, dp_size, turned),
        out_shape=out_shape,
        in_specs=[whole] * len(operands),
        out_specs=[anywhere] * len(out_shape),
        scratch_shapes=scratch,
        compiler_params=pltpu.CompilerParams(
            collective_id=0, has_side_effects=True, vmem_limit_bytes=VMEM_LIMIT
        ),
        name="forward_pass",
    )(*operands)


class Shares:
    def __init__(self, place, partial, kept, from_inner, from_outer, outer_sems, inner_sems, piece):
        self.place = place
        self.partial = partial
        self.kept = kept
        self.from_inner = from_inner
        self.from_outer = from_outer
        self.outer_sems = outer_sems
        self.inner_sems = inner_sems
        self.piece = piece
        self.rows = from_inner.shape[1]

    def at(self, index):
        return self.partial.at[pl.ds(pl.multiple_of(index * self.rows, self.rows), self.rows), :]

    def mine(self, shift):
        if self.kept is not None:
            return self.kept.at[shift]
        return self.at(self.place.ahead(shift))

    def inner_copy(self, shift):
        place = self.place
        return place.copy(
            self.at(place.ahead(shift, 1 - place.inner)),
            self.from_inner.at[shift],
            self.inner_sems,
            (self.piece, shift),
            dp=place.other,
        )

    def outer_copy(self, shift):
        place = self.place
        return place.copy(
            self.mine(shift),
            self.from_outer.at[shift - 1],
            self.outer_sems,
            (self.piece, shift),
            dp=place.ahead(shift),
        )

    def give(self):
        @pl.loop(1, self.place.outer_size)
        def _(shift):
            self.inner_copy(shift).start()

        self.inner_copy(0).start()

    def turn(self, first, last):
        @pl.loop(first, last)
        def _(shift):
            self.inner_copy(shift).wait_recv()
            mine = self.mine(shift)
            mine[...] = (mine[...].astype(F32) + self.from_inner[shift].astype(F32)).astype(BF16)
            self.outer_copy(shift).start()

    def keep(self, total):
        self.inner_copy(0).wait_recv()
        total[...] = self.mine(0)[...].astype(F32) + self.from_inner[0].astype(F32)

    def finish(self, total):
        @pl.loop(1, self.place.outer_size)
        def _(shift):
            self.outer_copy(shift).wait_recv()
            total[...] += self.from_outer[shift - 1].astype(F32)

    def drain(self):
        self.inner_copy(0).wait_send()

        @pl.loop(1, self.place.outer_size)
        def _(shift):
            self.inner_copy(shift).wait_send()
            self.outer_copy(shift).wait_send()


def backward_kernel(
    dp_size,
    cotangent,
    attn_gain,
    ffn_gain,
    tokens,
    qkv_full,
    back_full,
    gate_full,
    up_full,
    down_full,
    normed,
    ffn_all,
    cot_all,
    gate_slope,
    up_slope,
    hidden,
    grad_down,
    query,
    key,
    value,
    attended,
    proj,
    middle_in,
    tables,
    out_mixed,
    out_tokens,
    gain_sums,
    out_qkv,
    out_back,
    out_gate,
    out_up,
    out_down,
    mixed,
    mid_all,
    mixer,
    ffn_w,
    down_w,
    qkv_w,
    att,
    qry,
    ky,
    val,
    prj,
    down_kept,
    qkv_inner,
    back_inner,
    ffn_inner,
    down_inner,
    qkv_outer,
    back_outer,
    ffn_outer,
    down_outer,
    staged,
    part_twin,
    part_across,
    out_twin,
    out_across,
    middle,
    gain_parts,
    gain_packed,
    gain_group,
    gain_dp,
    outer_send,
    outer_recv,
    inner_send,
    inner_recv,
    group_send,
    group_recv,
    gain_send,
    gain_recv,
    local_sems,
    tile_sems,
):
    place = Place(dp_size)
    micro_count = mixed.shape[0]
    length = mid_all.shape[1]
    width = mid_all.shape[2]
    hidden_width = down_w.shape[1]
    block_count = length // TILE
    tile_count = micro_count * block_count
    outer_size = place.outer_size
    group_sems = (group_send, group_recv)
    outer_sems = (outer_send, outer_recv)
    inner_sems = (inner_send, inner_recv)
    own = tile(place.tensor)
    first_cut = 1 + (outer_size - 1) // 3
    second_cut = 1 + 2 * (outer_size - 1) // 3
    outers = outer_size // 4
    own_outer_block = place.outer // outers
    counter = []

    def load(src, dst):
        copy = pltpu.make_async_copy(src, dst, local_sems.at[len(counter) + (8 if len(counter) >= 8 else 0)])
        counter.append(copy)
        copy.start()
        return copy

    down_s = Shares(place, grad_down, down_kept, down_inner, down_outer, outer_sems, inner_sems, 4)

    def ffn_shares(kind):
        return Shares(
            place,
            ffn_w.at[kind],
            None,
            ffn_inner.at[kind],
            ffn_outer.at[kind],
            outer_sems,
            inner_sems,
            2 + kind,
        )

    gate_s, up_s = ffn_shares(0), ffn_shares(1)
    mid_g = [Gather(place, mid_all, m, group_sems, 3 * m) for m in range(micro_count)]

    def turn_block(step):
        return rem(step + 1 + own_outer_block, 4)

    def give_block(share, block):
        @pl.loop(0, outers)
        def _(index):
            shift = rem(block * outers + index - place.outer + outer_size, outer_size)
            share.inner_copy(shift).start()

    def twin_copy(kind, m, half):
        from_twin = (part_twin, out_twin, part_twin)[kind]
        return place.copy(
            staged.at[m, half],
            from_twin.at[m, half],
            group_sems,
            6 + 6 * kind + 3 * m + half,
            tensor=place.twin,
        )

    def across_copy(kind, m):
        from_across = (part_across, out_across, part_across)[kind]
        return place.copy(
            staged.at[m, 2],
            from_across.at[m],
            group_sems,
            6 + 6 * kind + 3 * m + 2,
            tensor=place.across,
        )

    def block_of(step):
        side = jnp.where(step < 2, 1 - place.side, place.side)
        core = jnp.where(rem(step, 2) == 0, 1 - place.core, place.core)
        return side * 2 + core

    def hand_out(kind, m, step, values):
        from_twin = (part_twin, out_twin, part_twin)[kind]
        half = step // 2

        @pl.when(rem(step, 2) == 0)
        def _():
            staged[m, half] = values.astype(BF16)
            twin_copy(kind, m, half).start()

        @pl.when(step == 1)
        def _():
            twin_copy(kind, m, 0).wait_recv()
            staged[m, 2] = (values + from_twin[m, 0].astype(F32)).astype(BF16)
            across_copy(kind, m).start()

        @pl.when(step == 3)
        def _():
            staged[m, 3] = values.astype(BF16)

    def collect(kind, m):
        from_twin = (part_twin, out_twin, part_twin)[kind]
        from_across = (part_across, out_across, part_across)[kind]
        twin_copy(kind, m, 1).wait_recv()
        across_copy(kind, m).wait_recv()
        return staged[m, 3].astype(F32) + from_twin[m, 1].astype(F32) + from_across[m].astype(F32)

    def drain(kind, m):
        twin_copy(kind, m, 0).wait_send()
        twin_copy(kind, m, 1).wait_send()
        across_copy(kind, m).wait_send()

    def leave_ffn(m):
        upstream = collect(0, m)
        back, term = norm_rows_back(middle[m], ffn_gain[...], upstream)
        mid_all[m, own] = (mixed[m].astype(F32) + back).astype(BF16)
        mid_g[m].start()
        gain_parts[1:2, :] += term

    def leave_out(m):
        mixed[m] = (middle[m] + collect(1, m)).astype(BF16)

    def attn_copies():
        pairs = (
            (back_full, qkv_w.at[:, 512:768]),
            (attended, att),
            (value.at[0], val),
            (key.at[0], ky),
            (query.at[0], qry),
            (proj.at[0], prj),
            (qkv_full, qkv_w.at[:, 0:512]),
        )
        return [
            pltpu.make_async_copy(src, dst, local_sems.at[30 + index])
            for index, (src, dst) in enumerate(pairs)
        ]

    def ffn_phase(grads, rows_buf, hidden_buf, ffn_cols):
        def rows_copy(index):
            m = index // block_count
            rows = tile(block_of(rem(index, block_count)))
            slot = rem(index, 2)
            return pltpu.make_async_copy(cot_all.at[m, rows], rows_buf.at[slot], tile_sems.at[0, slot])

        def hidden_copy(index):
            m = index // block_count
            rows = tile(block_of(rem(index, block_count)))
            slot = rem(index, 2)
            return pltpu.make_async_copy(hidden.at[m, rows], hidden_buf.at[slot], tile_sems.at[1, slot])

        def cols_copy(index):
            slot = rem(index, 2)
            return pltpu.make_async_copy(
                ffn_all.at[:, :, tile(turn_block(rem(index, block_count)))],
                ffn_cols.at[slot],
                tile_sems.at[2, slot],
            )

        loads = [load(down_full, down_w)]
        rows_copy(0).start()
        loads += [load(gate_slope.at[0], grads.at[0, 0]), load(up_slope.at[0], grads.at[1, 0])]
        loads += [load(gate_full, ffn_w.at[0]), load(up_full, ffn_w.at[1]), load(middle_in, middle)]
        loads.append(load(cotangent, mixed))

        def second_copies():
            return [
                pltpu.make_async_copy(slope.at[1], grads.at[kind, 1], local_sems.at[38 + kind])
                for kind, slope in enumerate((gate_slope, up_slope))
            ]

        def kept_copy(shift):
            return pltpu.make_async_copy(
                down_s.at(place.ahead(shift)), down_kept.at[shift], local_sems.at[40 + shift]
            )

        for copy in second_copies():
            copy.start()

        @pl.loop(0, outer_size)
        def _(shift):
            kept_copy(shift).start()

        fill_mixer(mixer)
        gain_parts[...] = jnp.zeros_like(gain_parts)
        gain_packed[...] = jnp.zeros_like(gain_packed)
        place.greet(True)
        down_s.give()
        for copy in loads:
            copy.wait()

        @pl.loop(0, tile_count)
        def _(index):
            m = index // block_count
            step = rem(index, block_count)
            rows = tile(block_of(step))
            slot = rem(index, 2)

            @pl.when(index + 1 < tile_count)
            def _():
                rows_copy(index + 1).start()

            @pl.when(index == 2)
            def _():
                @pl.loop(0, outer_size)
                def _(shift):
                    kept_copy(shift).wait()

                down_s.turn(1, first_cut)

            @pl.when(index == block_count)
            def _():
                for copy in second_copies():
                    copy.wait()

            @pl.when(index == block_count + 1)
            def _():
                down_s.turn(first_cut, second_cut)

            @pl.when(index == block_count + 3)
            def _():
                down_s.turn(second_cut, outer_size)
                leave_ffn(0)

            rows_copy(index).wait()
            hidden_grad = nn(rows_buf[slot], down_w[...])
            gate_low = (hidden_grad * grads[0, m, rows].astype(F32)).astype(BF16)
            up_low = (hidden_grad * grads[1, m, rows].astype(F32)).astype(BF16)
            grads[0, m, rows] = gate_low
            grads[1, m, rows] = up_low
            hand_out(0, m, step, nt(gate_low, ffn_w[0]) + nt(up_low, ffn_w[1]))

        for copy in attn_copies():
            copy.start()
        cols_copy(0).start()

        @pl.loop(0, 2 * block_count)
        def _(index):
            kind = index // block_count
            block = turn_block(rem(index, block_count))
            slot = rem(index, 2)
            cols_copy(index).wait()

            @pl.when(index + 1 < 2 * block_count)
            def _():
                cols_copy(index + 1).start()

            ffn_w[kind, tile(block)] = (
                tn(ffn_cols[slot, 0], grads[kind, 0]) + tn(ffn_cols[slot, 1], grads[kind, 1])
            ).astype(BF16)
            give_block(ffn_shares(kind), block)

            @pl.when(index == block_count + 2)
            def _():
                leave_ffn(1)

        hidden_copy(0).start()

        @pl.loop(0, tile_count)
        def _(index):
            m = index // block_count
            step = rem(index, block_count)
            slot = rem(index, 2)

            @pl.when(index + 1 < tile_count)
            def _():
                hidden_copy(index + 1).start()

            hidden_copy(index).wait()

            @pl.when(step == 0)
            def _():
                drain(0, m)

            hand_out(1, m, step, nt(hidden_buf[slot], down_w[...]))

    pl.run_scoped(
        ffn_phase,
        pltpu.VMEM((2, micro_count, length, hidden_width), BF16),
        pltpu.VMEM((2, TILE, width), BF16),
        pltpu.VMEM((2, TILE, hidden_width), BF16),
        pltpu.VMEM((2, micro_count, length, TILE), BF16),
    )

    def attn_phase(
        toks,
        tabs,
        grad_att,
        grad_q,
        grad_k,
        grad_v,
        grad_qkv,
        qkv_total,
        back_total,
        gate_total,
        up_total,
        down_total,
    ):
        qkv_part = down_w.at[:, 0:512]
        back_part = down_w.at[:, 512:768]
        qkv_s = Shares(place, qkv_part, None, qkv_inner, qkv_outer, outer_sems, inner_sems, 0)
        back_s = Shares(place, back_part, None, back_inner, back_outer, outer_sems, inner_sems, 1)
        lane = lax.broadcasted_iota(jnp.int32, (TILE, 128), 1)
        front = lane < 64
        place_in = rem(lane, 64)
        later = lax.broadcasted_iota(jnp.int32, (TILE, TILE), 0) > lax.broadcasted_iota(
            jnp.int32, (TILE, TILE), 1
        )
        causal = jnp.where(later, APART, 0.0)
        small = mixer[0:128, 0:128]
        table_load = load(tables, tabs)
        token_load = load(tokens, toks)

        def score_ready(m):
            @pl.loop(0, block_count)
            def _(block):
                rows = tile(block)
                low = nn(mid_all[m, rows], qkv_w[:, 512:768]).astype(BF16)
                for group in range(2):
                    part = low[:, 128 * group : 128 * group + 128]
                    both = part.astype(F32) * att[m, group, rows].astype(F32)
                    shift = head_mean(both, small) * -64.0
                    high = shift.astype(BF16)
                    rest = shift - high.astype(F32)
                    mid = rest.astype(BF16)
                    last = (rest - mid.astype(F32)).astype(BF16)
                    marks = jnp.where(
                        place_in == 0,
                        high.astype(F32),
                        jnp.where(
                            place_in == 1,
                            mid.astype(F32),
                            jnp.where(place_in == 2, last.astype(F32), 0.0),
                        ),
                    )
                    grad_att[group, rows, 0:128] = part
                    grad_att[group, rows, 128:256] = marks.astype(BF16)

        def attend_back(m, between):
            @pl.loop(0, 2)
            def _(group):
                for block in range(block_count):
                    rows = slice(block * TILE, (block + 1) * TILE)
                    spans = [(rows, True)]
                    if block + 1 < block_count:
                        spans.append((slice((block + 1) * TILE, length), False))
                    sums_k = []
                    sums_v = []
                    for head in range(2):
                        key_block = ky[group, head, rows]
                        value_block = val[group, head, rows]
                        sum_k = None
                        sum_v = None
                        for span, masked in spans:
                            query_span = qry[group, span]
                            grad_span = grad_att[group, span]
                            scores = nt(key_block, query_span)
                            if masked:
                                scores = scores + causal
                            probs = jnp.exp2(scores)
                            score_grad = (probs * nt(value_block, grad_span)).astype(BF16)
                            probs_low = probs.astype(BF16)
                            part_v = nn(probs_low, grad_span[:, 0:128])
                            part_k = nn(score_grad, query_span[:, 0:128])
                            sum_v = part_v if sum_v is None else sum_v + part_v
                            sum_k = part_k if sum_k is None else sum_k + part_k
                            part_q = tn(score_grad, key_block[:, 0:128])
                            if block == 0 and head == 0:
                                grad_q[group, span] = part_q
                            else:
                                grad_q[group, span] += part_q
                        sums_k.append(sum_k)
                        sums_v.append(sum_v)
                    both_k = jnp.where(front, sums_k[0], sums_k[1])
                    both_v = jnp.where(front, sums_v[0], sums_v[1])
                    grad_k[group, rows] = both_k + pltpu.roll(both_k, 64, 1)
                    grad_v[group, rows] = both_v + pltpu.roll(both_v, 64, 1)

                @pl.when(group == 0)
                def _():
                    between()

        def normalize_back(grads, values, cosine, sine):
            scaled = grads * LN2
            weighted = scaled * cosine + swap_halves(scaled * sine)
            inverse = lax.rsqrt(head_mean(values * values, small) + NORM_EPS)
            unit = values * inverse
            both = weighted * unit
            back = inverse * (weighted - unit * head_mean(both, small))
            return back.astype(BF16), jnp.sum(both, axis=0, keepdims=True)

        def leave_heads(m):
            @pl.loop(0, block_count)
            def _(block):
                rows = tile(block)
                cosine, sine = tabs[0, rows], tabs[1, rows]
                for group in range(2):
                    lanes = slice(128 * group, 128 * group + 128)
                    back, term = normalize_back(grad_q[group, rows], prj[rows, lanes], cosine, sine)
                    grad_qkv[m, rows, lanes] = back
                    gain_parts[2:3, 0:128] += term
                back, term = normalize_back(
                    jnp.where(front, grad_k[0, rows], grad_k[1, rows]),
                    prj[rows, 256:384],
                    tabs[2, rows],
                    tabs[3, rows],
                )
                grad_qkv[m, rows, 256:384] = back
                gain_parts[2:3, 128:256] += term
                grad_qkv[m, rows, 384:512] = jnp.where(
                    front, grad_v[0, rows], grad_v[1, rows]
                ).astype(BF16)

        def enter_norm(m):
            drain(1, m)

            @pl.loop(0, block_count)
            def _(step):
                rows = tile(block_of(step))
                hand_out(2, m, step, nt(grad_qkv[m, rows], qkv_w[:, 0:512]))

        def leave_attn(m):
            upstream = collect(2, m)
            back, term = norm_rows_back(toks[m].astype(F32), attn_gain[...], upstream)
            middle[m] = mid_all[m, own].astype(F32) + back
            gain_parts[0:1, :] += term

        def norm_copy(index):
            slot = rem(index, 2)
            return pltpu.make_async_copy(
                normed.at[:, :, tile(turn_block(index))], val.at[slot], tile_sems.at[3, slot]
            )

        reloads = ((value, val), (key, ky), (query, qry), (proj, prj))

        def reload_copy(index):
            src, dst = reloads[index]
            return pltpu.make_async_copy(src.at[1], dst, local_sems.at[10 + index])

        def mixed_save(m):
            return pltpu.make_async_copy(mixed.at[m], out_mixed.at[m], local_sems.at[14 + m])

        def enter_back():
            @pl.loop(0, block_count)
            def _(step):
                block = turn_block(step)
                columns = tile(block)
                total = jnp.zeros((TILE, 256), F32)
                for m in range(micro_count):
                    heads = jnp.concatenate([att[m, 0], att[m, 1]], axis=1)
                    total = total + tn(mid_all[m, :, columns], heads)
                back_part[columns] = total.astype(BF16)
                give_block(back_s, block)

        table_load.wait()
        token_load.wait()

        @pl.loop(0, micro_count)
        def _(m):
            @pl.when(m == 0)
            def _():
                down_s.keep(down_total)
                gate_s.turn(1, first_cut)
                mid_g[0].relay()
                for copy in attn_copies():
                    copy.wait()
                mid_g[0].finish()

            @pl.when(m == 1)
            def _():
                mid_g[1].finish()
                for index in range(4):
                    reload_copy(index).wait()

            score_ready(m)

            @pl.when(m == 0)
            def _():
                gate_s.turn(first_cut, second_cut)

            @pl.when(m == 1)
            def _():
                enter_back()
                up_s.turn(first_cut, second_cut)

            def between():
                @pl.when(m == 0)
                def _():
                    gate_s.turn(second_cut, outer_size)
                    mid_g[1].relay()

                @pl.when(m == 1)
                def _():
                    up_s.turn(second_cut, outer_size)

            attend_back(m, between)

            @pl.when(m == 0)
            def _():
                for index in range(3):
                    reload_copy(index).start()
                gate_s.keep(gate_total)

            @pl.when(m == 1)
            def _():
                norm_copy(0).start()

            leave_heads(m)

            @pl.when(m == 0)
            def _():
                reload_copy(3).start()
                up_s.turn(1, first_cut)

            @pl.when(m == 1)
            def _():
                up_s.keep(up_total)

            leave_out(m)
            mixed_save(m).start()
            enter_norm(m)

        saves = [mixed_save(m) for m in range(micro_count)]
        down_s.finish(down_total)
        saves.append(load(down_total, out_down))
        gate_s.finish(gate_total)
        saves.append(load(gate_total, out_gate))
        back_s.turn(1, outer_size)

        @pl.loop(0, block_count)
        def _(step):
            block = turn_block(step)
            columns = tile(block)
            slot = rem(step, 2)
            norm_copy(step).wait()

            @pl.when(step + 1 < block_count)
            def _():
                norm_copy(step + 1).start()

            qkv_part[columns] = (
                tn(val[slot, 0], grad_qkv[0]) + tn(val[slot, 1], grad_qkv[1])
            ).astype(BF16)
            give_block(qkv_s, block)

        back_s.keep(back_total)
        leave_attn(0)
        saves.append(load(middle.at[0], out_tokens.at[0]))
        qkv_s.turn(1, outer_size)
        up_s.finish(up_total)
        saves.append(load(up_total, out_up))
        leave_attn(1)
        saves.append(load(middle.at[1], out_tokens.at[1]))

        def group_gain(shift):
            return place.copy(
                gain_packed,
                gain_group.at[shift - 1],
                (gain_send, gain_recv),
                shift - 1,
                tensor=rem(place.tensor + shift, 4),
            )

        pack_gains(gain_packed, gain_parts)
        for shift in range(1, 4):
            group_gain(shift).start()
        qkv_s.keep(qkv_total)
        back_s.finish(back_total)
        saves.append(load(back_total, out_back))
        for shift in range(1, 4):
            group_gain(shift).wait_recv()
        gain_dp[0] = gain_packed[...] + gain_group[0] + gain_group[1] + gain_group[2]

        def dp_gain(shift):
            return place.copy(
                gain_dp.at[0],
                gain_dp.at[shift],
                (gain_send, gain_recv),
                2 + shift,
                dp=rem(place.dp + shift, dp_size),
            )

        @pl.loop(1, dp_size)
        def _(shift):
            dp_gain(shift).start()

        qkv_s.finish(qkv_total)
        saves.append(load(qkv_total, out_qkv))
        gain_sums[...] = gain_dp[0]

        @pl.loop(1, dp_size)
        def _(shift):
            dp_gain(shift).wait_recv()
            gain_sums[...] += gain_dp[shift]

        for shift in range(1, 4):
            group_gain(shift).wait_send()

        @pl.loop(1, dp_size)
        def _(shift):
            dp_gain(shift).wait_send()

        qkv_s.drain()
        back_s.drain()
        for copy in saves:
            copy.wait()

    pl.run_scoped(
        attn_phase,
        pltpu.VMEM(tokens.shape, BF16),
        pltpu.VMEM(tables.shape, F32),
        pltpu.VMEM((2, length, 256), BF16),
        pltpu.VMEM((2, length, 128), F32),
        pltpu.VMEM((2, length, 128), F32),
        pltpu.VMEM((2, length, 128), F32),
        pltpu.VMEM((micro_count, length, 512), BF16),
        *[
            pltpu.VMEM((width // dp_size, w), F32)
            for w in (512, 256, hidden_width, hidden_width, hidden_width)
        ],
    )
    for share in (down_s, gate_s, up_s):
        share.drain()
    for m in range(micro_count):
        mid_g[m].drain()
        drain(2, m)


def backward(dp_size, cotangent, attn_gain, ffn_gain, tokens, saved):
    micro, rows, width = tokens.shape
    length = saved[5].shape[1]
    hidden_width = saved[2].shape[1]
    outer_size = dp_size // 2
    share = width // dp_size
    whole = pl.BlockSpec(memory_space=pltpu.VMEM)
    anywhere = pl.BlockSpec(memory_space=pl.ANY)
    shape = jax.ShapeDtypeStruct
    widths = (512, 256, hidden_width, hidden_width, hidden_width)
    out_shape = [
        shape((micro, rows, width), BF16),
        shape((micro, rows, width), F32),
        shape((8, 384), F32),
    ] + [shape((share, w), F32) for w in widths]
    scratch = (
        [pltpu.VMEM((micro, rows, width), BF16)]
        + [
            pltpu.VMEM((micro, length, width), BF16),
            pltpu.VMEM((256, 256), BF16),
            pltpu.VMEM((2, width, hidden_width), BF16),
            pltpu.VMEM((width, hidden_width), BF16),
            pltpu.VMEM((width, 768), BF16),
            pltpu.VMEM((micro, 2, length, 128), BF16),
            pltpu.VMEM((2, length, 256), BF16),
            pltpu.VMEM((2, 2, length, 256), BF16),
            pltpu.VMEM((2, 2, length, 256), BF16),
            pltpu.VMEM((length, 384), F32),
            pltpu.VMEM((outer_size, share, hidden_width), BF16),
            pltpu.VMEM((outer_size, share, 512), BF16),
            pltpu.VMEM((outer_size, share, 256), BF16),
            pltpu.VMEM((2, outer_size, share, hidden_width), BF16),
            pltpu.VMEM((outer_size, share, hidden_width), BF16),
            pltpu.VMEM((outer_size - 1, share, 512), BF16),
            pltpu.VMEM((outer_size - 1, share, 256), BF16),
            pltpu.VMEM((2, outer_size - 1, share, hidden_width), BF16),
            pltpu.VMEM((outer_size - 1, share, hidden_width), BF16),
            pltpu.VMEM((micro, 4, rows, width), BF16),
            pltpu.VMEM((micro, 2, rows, width), BF16),
            pltpu.VMEM((micro, rows, width), BF16),
            pltpu.VMEM((micro, 2, rows, width), BF16),
            pltpu.VMEM((micro, rows, width), BF16),
            pltpu.VMEM((micro, rows, width), F32),
            pltpu.VMEM((8, width), F32),
            pltpu.VMEM((8, 384), F32),
            pltpu.VMEM((3, 8, 384), F32),
            pltpu.VMEM((dp_size, 8, 384), F32),
        ]
        + [pltpu.SemaphoreType.DMA((5, outer_size))] * 4
        + [pltpu.SemaphoreType.DMA((24,))] * 2
        + [pltpu.SemaphoreType.DMA((dp_size + 2,))] * 2
        + [pltpu.SemaphoreType.DMA((40 + outer_size,)), pltpu.SemaphoreType.DMA((4, 2))]
    )
    return pl.pallas_call(
        functools.partial(backward_kernel, dp_size),
        out_shape=out_shape,
        in_specs=[anywhere, whole, whole] + [anywhere] * (1 + len(saved)),
        out_specs=[anywhere, anywhere, whole] + [anywhere] * 5,
        scratch_shapes=scratch,
        compiler_params=pltpu.CompilerParams(
            collective_id=1, has_side_effects=True, vmem_limit_bytes=VMEM_LIMIT
        ),
        name="backward_pass",
    )(cotangent, attn_gain, ffn_gain, tokens, *saved)


def deliver_kernel(
    turned,
    in_mixed,
    in_tokens,
    gains,
    in_qkv,
    in_back,
    in_gate,
    in_up,
    in_down,
    mixed,
    grad_tokens,
    attn_gain,
    ffn_gain,
    head_gains,
    grad_query,
    grad_key,
    grad_value,
    grad_out,
    grad_gate,
    grad_up,
    grad_down,
    buf_mixed,
    buf_tokens,
    buf_gate,
    buf_up,
    buf_qkv,
    buf_back,
    buf_down,
    sems,
):
    flows = [
        (in_qkv, buf_qkv, None),
        (in_back, buf_back, None),
        (in_down, buf_down, None),
        (in_mixed, buf_mixed, mixed),
        (in_tokens.at[0], buf_tokens.at[0], grad_tokens.at[0]),
        (in_tokens.at[1], buf_tokens.at[1], grad_tokens.at[1]),
        (in_gate, buf_gate, grad_gate),
        (in_up, buf_up, grad_up),
    ]
    arrivals = [
        pltpu.make_async_copy(src, buf, sems.at[0, index]) for index, (src, buf, _) in enumerate(flows)
    ]
    departures = []
    for copy in arrivals:
        copy.start()
    part = 0
    for out in (attn_gain, ffn_gain, head_gains):
        for start in range(0, out.shape[1], 128):
            out[:, start : start + 128] = gains[
                part // 3 : part // 3 + 1, 128 * (part % 3) : 128 * (part % 3) + 128
            ]
            part += 1
    for index, (_, buf, dst) in enumerate(flows):
        arrivals[index].wait()
        if dst is not None:
            copy = pltpu.make_async_copy(buf, dst, sems.at[1, index])
            copy.start()
            departures.append(copy)
        if index == 2:
            grad_query[...] = buf_qkv[:, 0:256]
            grad_key[...] = buf_qkv[:, 256:384]
            grad_value[...] = buf_qkv[:, 384:512]
            grad_out[...] = buf_back[...] if turned else buf_back[...].T
            grad_down[...] = buf_down[...] if turned else buf_down[...].T
    for copy in departures:
        copy.wait()


def deliver(results):
    mixed, grad_tokens, gains, qkv, back, gate, up, down = results
    turned = qkv.shape[0] % 128 != 0
    whole = pl.BlockSpec(memory_space=pltpu.VMEM)
    anywhere = pl.BlockSpec(memory_space=pl.ANY)
    shape = jax.ShapeDtypeStruct
    share, width = qkv.shape[0], mixed.shape[2]

    def facing(array):
        return array.shape if turned else array.shape[::-1]

    out_shape = [
        shape(mixed.shape, BF16),
        shape(grad_tokens.shape, F32),
        shape((1, width), F32),
        shape((1, width), F32),
        shape((1, 256), F32),
        shape((share, 256), F32),
        shape((share, 128), F32),
        shape((share, 128), F32),
        shape(facing(back), F32),
        shape(gate.shape, F32),
        shape(up.shape, F32),
        shape(facing(down), F32),
    ]
    out = pl.pallas_call(
        functools.partial(deliver_kernel, turned),
        out_shape=out_shape,
        in_specs=[anywhere, anywhere, whole] + [anywhere] * 5,
        out_specs=[anywhere, anywhere] + [whole] * 7 + [anywhere, anywhere, whole],
        scratch_shapes=[
            pltpu.VMEM(mixed.shape, BF16),
            pltpu.VMEM(grad_tokens.shape, F32),
            pltpu.VMEM(gate.shape, F32),
            pltpu.VMEM(up.shape, F32),
            pltpu.VMEM(qkv.shape, F32),
            pltpu.VMEM(back.shape, F32),
            pltpu.VMEM(down.shape, F32),
            pltpu.SemaphoreType.DMA((2, 8)),
        ],
        compiler_params=pltpu.CompilerParams(vmem_limit_bytes=32000 * 1024),
        name="deliver_pass",
    )(*results)
    out = list(out)
    if turned:
        out[8], out[11] = out[8].T, out[11].T
    return out


def shards(
    dp_size,
    tokens,
    segment_ids,
    attn_gain,
    query_gain,
    key_gain,
    w_query,
    w_key,
    w_value,
    w_out,
    ffn_gain,
    w_gate,
    w_up,
    w_down,
    cotangent,
):
    own_tokens, own_cot = tokens[:, 0], cotangent[:, 0]
    attn_row, ffn_row = attn_gain[None], ffn_gain[None]
    saved = forward(
        dp_size,
        own_tokens,
        own_cot,
        segment_ids[:, 0],
        (w_query, w_key, w_value, w_out, w_gate, w_up, w_down),
        (attn_row, ffn_row, query_gain[None], key_gain[None]),
    )
    results = backward(dp_size, own_cot, attn_row, ffn_row, own_tokens, saved)
    (
        mixed,
        grad_tokens,
        attn_term,
        ffn_term,
        head_terms,
        grad_query,
        grad_key,
        grad_value,
        grad_out,
        grad_gate,
        grad_up,
        grad_down,
    ) = deliver(results)
    query_term = head_terms[0, :128].reshape(2, DH).sum(0) / query_gain
    key_term = head_terms[0, 128:256].reshape(2, DH).sum(0) / key_gain
    return (
        mixed[:, None],
        grad_tokens[:, None],
        attn_term[0],
        query_term,
        key_term,
        grad_query,
        grad_key,
        grad_value,
        grad_out,
        ffn_term[0],
        grad_gate,
        grad_up,
        grad_down,
    )


def solution(mesh):
    sequence = P(None, "dp", "tensor", None)
    rows = P("dp", "tensor")
    columns = P("tensor", "dp")
    return jax.shard_map(
        functools.partial(shards, mesh.shape["dp"]),
        mesh=mesh,
        in_specs=(sequence, P(None, "dp", None), P(), P(), P(), rows, rows, rows, columns, P(), rows, rows, columns, sequence),
        out_specs=(sequence, sequence, P(), P(), P(), rows, rows, rows, columns, P(), rows, rows, columns),
        check_vma=False,
    )
```

```python
import functools
import math

import jax
import jax.numpy as jnp
import numpy as np
from jax import lax
from jax.experimental import pallas as pl
from jax.experimental.pallas import tpu as pltpu
from jax.sharding import PartitionSpec as P

MESH = pl.DeviceIdType.MESH
VMEM_LIMIT = 67000000
NORM_EPS = 1e-05
ROPE_BASE = 1000000.0
DH = 64
TILE = 256
LN2 = math.log(2.0)
APART = -32768.0
BF16 = jnp.bfloat16
F32 = jnp.float32


def nn(left, right):
    return lax.dot_general(left, right, (((1,), (0,)), ((), ())), preferred_element_type=F32)


def nt(left, right):
    return lax.dot_general(left, right, (((1,), (1,)), ((), ())), preferred_element_type=F32)


def tn(left, right):
    return lax.dot_general(left, right, (((0,), (0,)), ((), ())), preferred_element_type=F32)


def tile(index, size=TILE):
    return pl.ds(pl.multiple_of(index * size, size), size)


def rem(value, divisor):
    return value % divisor if isinstance(value, int) else lax.rem(value, divisor)


def low_parts(values):
    high = values.astype(BF16)
    return high, (values - high.astype(F32)).astype(BF16)


def head_mean(values, mixer):
    high, rest = low_parts(values)
    return nn(high, mixer) + nn(rest, mixer)


def swap_halves(values):
    lane = lax.broadcasted_iota(jnp.int32, values.shape, 1)
    ahead = pltpu.roll(values, 96, 1)
    behind = pltpu.roll(values, 32, 1)
    return jnp.where(lax.rem(lane, 64) < 32, ahead, behind)


def norm_rows(values, gain):
    inverse = lax.rsqrt(jnp.mean(values * values, axis=-1, keepdims=True) + NORM_EPS)
    return values * inverse * gain


def norm_rows_back(values, gain, upstream):
    inverse = lax.rsqrt(jnp.mean(values * values, axis=-1, keepdims=True) + NORM_EPS)
    scaled = values * inverse
    weighted = upstream * gain
    back = inverse * (weighted - scaled * jnp.mean(weighted * scaled, axis=-1, keepdims=True))
    return back, jnp.sum(upstream * scaled, axis=0, keepdims=True)


class Place:
    def __init__(self, dp_size):
        self.dp_size = dp_size
        self.dp = lax.axis_index("dp")
        self.tensor = lax.axis_index("tensor")
        self.outer_size = dp_size // 2
        self.outer = self.dp // 2
        self.inner = lax.rem(self.dp, 2)
        self.other = self.outer * 2 + 1 - self.inner
        self.side = self.tensor // 2
        self.core = lax.rem(self.tensor, 2)
        self.across = (1 - self.side) * 2 + self.core
        self.twin = self.side * 2 + 1 - self.core

    def ahead(self, shift, inner=None):
        inner = self.inner if inner is None else inner
        return lax.rem(self.outer + shift, self.outer_size) * 2 + inner

    def behind(self, shift):
        return lax.rem(self.outer - shift + self.outer_size, self.outer_size) * 2 + self.inner

    def block(self, step):
        side = 1 - self.side if step < 2 else self.side
        core = 1 - self.core if step % 2 == 0 else self.core
        return side * 2 + core

    def copy(self, src, dst, sems, index, dp=None, tensor=None):
        return pltpu.make_async_remote_copy(
            src_ref=src,
            dst_ref=dst,
            send_sem=sems[0].at[index],
            recv_sem=sems[1].at[index],
            device_id=(
                self.dp if dp is None else dp,
                self.tensor if tensor is None else tensor,
            ),
            device_id_type=MESH,
        )

    def greet(self, everyone):
        barrier = pltpu.get_barrier_semaphore()

        def signal(dp, tensor):
            pl.semaphore_signal(barrier, inc=1, device_id=(dp, tensor), device_id_type=MESH)

        if everyone:

            @pl.loop(1, self.dp_size)
            def _(shift):
                signal(lax.rem(self.dp + shift, self.dp_size), self.tensor)

            for shift in range(1, 4):
                signal(self.dp, lax.rem(self.tensor + shift, 4))
            pl.semaphore_wait(barrier, self.dp_size + 2)
        else:

            @pl.loop(1, self.outer_size)
            def _(shift):
                signal(self.ahead(shift), self.tensor)

            signal(self.other, self.tensor)
            signal(self.dp, self.across)
            signal(self.dp, self.twin)
            pl.semaphore_wait(barrier, self.outer_size + 2)


def pack_gains(packed, terms):
    part = 0
    for row, width in enumerate((terms.shape[1], terms.shape[1], 256)):
        for start in range(0, width, 128):
            packed[part // 3 : part // 3 + 1, 128 * (part % 3) : 128 * (part % 3) + 128] = terms[
                row : row + 1, start : start + 128
            ]
            part += 1


class Gather:
    def __init__(self, place, ref, micro, sems, index, source=None):
        own = ref.at[micro, tile(place.tensor)]
        source = own if source is None else source
        theirs = ref.at[micro, tile(place.across)]
        self.to_across = place.copy(source, own, sems, index, tensor=place.across)
        self.to_twin = place.copy(source, own, sems, index + 1, tensor=place.twin)
        self.on_to_twin = place.copy(theirs, theirs, sems, index + 2, tensor=place.twin)

    def start(self):
        self.to_across.start()
        self.to_twin.start()

    def relay(self):
        self.to_across.wait_recv()
        self.on_to_twin.start()

    def finish(self):
        self.to_twin.wait_recv()
        self.on_to_twin.wait_recv()

    def drain(self):
        self.to_across.wait_send()
        self.to_twin.wait_send()
        self.on_to_twin.wait_send()


class Scatter:
    def __init__(self, place, staged, from_twin, from_across, sems, index):
        self.place = place
        self.staged = staged
        self.from_twin = from_twin
        self.from_across = from_across
        self.sems = sems
        self.index = index

    def twin(self, half):
        return self.place.copy(
            self.staged.at[half],
            self.from_twin.at[half],
            self.sems,
            self.index + half,
            tensor=self.place.twin,
        )

    def crossing(self):
        return self.place.copy(
            self.staged.at[2],
            self.from_across,
            self.sems,
            self.index + 2,
            tensor=self.place.across,
        )

    def give(self, step, values):
        if step == 0 or step == 2:
            half = step // 2
            self.staged[half] = values.astype(BF16)
            self.twin(half).start()
        elif step == 1:
            self.staged[2] = values.astype(BF16)

    def cross(self):
        self.twin(0).wait_recv()
        self.staged[2] = (self.staged[2].astype(F32) + self.from_twin[0].astype(F32)).astype(BF16)
        self.crossing().start()

    def result(self, values):
        self.twin(1).wait_recv()
        self.crossing().wait_recv()
        return values + self.from_twin[1].astype(F32) + self.from_across[...].astype(F32)

    def drain(self):
        self.twin(0).wait_send()
        self.twin(1).wait_send()
        self.crossing().wait_send()


def fill_mixer(mixer):
    row = lax.broadcasted_iota(jnp.int32, mixer.shape, 0) // DH
    column = lax.broadcasted_iota(jnp.int32, mixer.shape, 1) // DH
    mixer[...] = jnp.where(row == column, 1.0 / DH, 0.0).astype(BF16)


class Weights:
    def __init__(self, place, shard, full, outer_sems, inner_sems, piece):
        self.place = place
        self.shard = shard
        self.full = full
        self.outer_sems = outer_sems
        self.inner_sems = inner_sems
        self.piece = piece
        self.rows = shard.shape[0]

    def at(self, index):
        return self.full.at[pl.ds(pl.multiple_of(index * self.rows, self.rows), self.rows), :]

    def outer_copy(self, shift):
        place = self.place
        return place.copy(
            self.shard,
            self.at(place.dp),
            self.outer_sems,
            (self.piece, shift),
            dp=place.ahead(shift),
        )

    def inner_copy(self, shift):
        place = self.place
        rows = self.at(place.behind(shift))
        return place.copy(rows, rows, self.inner_sems, (self.piece, shift), dp=place.other)

    def own_copy(self):
        place = self.place
        return place.copy(
            self.shard, self.at(place.dp), self.inner_sems, (self.piece, 0), dp=place.other
        )

    def send_outer(self, first, last):
        @pl.loop(first, last)
        def _(shift):
            self.outer_copy(shift).start()

    def send_inner(self):
        self.own_copy().start()

    def relay(self, first, last):
        @pl.loop(first, last)
        def _(shift):
            self.outer_copy(shift).wait_recv()
            self.inner_copy(shift).start()

    def finish(self):
        @pl.loop(0, self.place.outer_size)
        def _(shift):
            self.inner_copy(shift).wait_recv()

    def drain(self):
        self.own_copy().wait_send()

        @pl.loop(1, self.place.outer_size)
        def _(shift):
            self.outer_copy(shift).wait_send()
            self.inner_copy(shift).wait_send()


def rotation_angles(length):
    frequency = ROPE_BASE ** (-2.0 * (np.arange(128) % (DH // 2)) / DH)
    steps = np.arange(8) * TILE if length <= 8 * TILE else np.arange(0, length, TILE)
    positions = np.concatenate([np.arange(TILE), steps])
    turns = positions[:, None] * frequency[None, :]
    return jnp.asarray(np.stack([np.cos(turns), np.sin(turns)]).astype(np.float32))


def forward_kernel(
    dp_size,
    turned,
    tokens,
    cotangent,
    segments,
    w_query,
    w_key,
    w_value,
    w_out,
    gate_shard,
    up_shard,
    w_down,
    attn_gain,
    ffn_gain,
    query_gain,
    key_gain,
    angles,
    out_qkv_full,
    out_back_full,
    out_gate_full,
    out_up_full,
    out_down_full,
    out_normed,
    out_ffn,
    out_cot,
    out_gate_slope,
    out_up_slope,
    out_hidden,
    out_grad_down,
    out_query,
    out_key,
    out_value,
    out_attended,
    out_proj,
    out_middle,
    out_tables,
    qkv_shard,
    back_shard,
    down_shard,
    tables,
    query_marks,
    key_marks,
    mixer,
    normed,
    ffn_all,
    cot_all,
    qkv_full,
    back_full,
    gate_full,
    up_full,
    slopes,
    hidden,
    grad_down,
    query,
    key,
    value,
    attended,
    proj,
    middle,
    staged,
    from_twin,
    from_across,
    outer_send,
    outer_recv,
    inner_send,
    inner_recv,
    group_send,
    group_recv,
    local_sems,
    slope_sems,
):
    place = Place(dp_size)
    micro_count = tokens.shape[0]
    block_count = normed.shape[1] // TILE
    outer_size = place.outer_size
    group_sems = (group_send, group_recv)
    outer_sems = (outer_send, outer_recv)
    inner_sems = (inner_send, inner_recv)
    own = tile(place.tensor)
    first_cut = 1 + (outer_size - 1) // 3
    second_cut = 1 + 2 * (outer_size - 1) // 3
    qkv_w = Weights(place, qkv_shard, qkv_full, outer_sems, inner_sems, 0)
    back_w = Weights(place, back_shard, back_full, outer_sems, inner_sems, 1)
    gate_w = Weights(place, gate_shard, gate_full, outer_sems, inner_sems, 2)
    up_w = Weights(place, up_shard, up_full, outer_sems, inner_sems, 3)
    down_w = Weights(place, down_shard, out_down_full, outer_sems, inner_sems, 4)
    normed_g = [Gather(place, normed, m, group_sems, 3 * m) for m in range(micro_count)]
    cot_g = [
        Gather(place, cot_all, m, group_sems, 6 + 3 * m, cotangent.at[m])
        for m in range(micro_count)
    ]
    ffn_g = [Gather(place, ffn_all, m, group_sems, 12 + 3 * m) for m in range(micro_count)]

    def branch_s(m):
        return Scatter(
            place, staged.at[m], from_twin.at[m], from_across.at[m], group_sems, 18 + 3 * m
        )

    saves = []

    def save(src, dst):
        copy = pltpu.make_async_copy(src, dst, local_sems.at[len(saves)])
        copy.start()
        saves.append(copy)
        return copy

    def save_columns(src, dst, m):
        for block in range(dst.shape[0]):
            save(src.at[m, :, TILE * block : TILE * block + TILE], dst.at[block, m])

    lane = lax.broadcasted_iota(jnp.int32, (TILE, 128), 1)
    front = lane < 64
    place_in = rem(lane, 64)

    value_end = w_query.shape[1] + w_key.shape[1]
    qkv_shard[:, : w_query.shape[1]] = w_query[...]
    qkv_shard[:, w_query.shape[1] : value_end] = w_key[...]
    qkv_shard[:, value_end:] = w_value[...]
    for m in range(micro_count):
        normed[m, own] = norm_rows(tokens[m].astype(F32), attn_gain[...]).astype(BF16)
    if turned:
        back_shard[...] = w_out[...]
        down_shard[...] = w_down[...]
    else:
        back_shard[...] = w_out[...].T
        down_shard[...] = w_down[...].T
    place.greet(False)
    cuts = (1, first_cut, second_cut, outer_size)
    order = (qkv_w, back_w, gate_w, up_w, down_w)

    def issue(item):
        piece, part = order[item // 3], item % 3
        piece.send_outer(cuts[part], cuts[part + 1])
        if part == 0:
            piece.send_inner()

    def take(item):
        part = item % 3
        order[item // 3].relay(cuts[part], cuts[part + 1])
        for following in {0: (2,), 1: (3, 4), 2: (5, 6), 3: (7,), 4: (), 5: (8,)}.get(item, (item + 3,)):
            if following < 3 * len(order):
                issue(following)

    issue(0)
    issue(1)
    normed_g[0].start()

    def prepare():
        fill_mixer(mixer)
        sign = jnp.where(place_in < 32, -1.0, 1.0)
        for kind, (gain_ref, scale) in enumerate(((query_gain, DH**-0.5 / LN2), (key_gain, 1.0))):
            gain = jnp.broadcast_to(
                jnp.concatenate([gain_ref[...], gain_ref[...]], axis=1) * scale, (TILE, 128)
            )
            crossed = swap_halves(gain) * sign
            for block in range(block_count):
                rows = slice(block * TILE, (block + 1) * TILE)
                cos_step = angles[0, TILE + block : TILE + block + 1]
                sin_step = angles[1, TILE + block : TILE + block + 1]
                cosine = angles[0, 0:TILE] * cos_step - angles[1, 0:TILE] * sin_step
                sine = angles[1, 0:TILE] * cos_step + angles[0, 0:TILE] * sin_step
                tables[2 * kind, rows] = cosine * gain
                tables[2 * kind + 1, rows] = sine * crossed
        row = lax.broadcasted_iota(jnp.int32, (16, 128), 0)
        mark_lane = lax.broadcasted_iota(jnp.int32, (16, 128), 1)
        spread = jnp.where(mark_lane == row + 8, 1.0, 0.0).astype(BF16)
        used = (lane >= 8) & (lane < 11)
        for m in range(micro_count):
            for block in range(block_count):
                rows = slice(block * TILE, (block + 1) * TILE)
                ids = jnp.broadcast_to(segments[m, :, rows], (16, TILE))
                match = lax.broadcasted_iota(jnp.int32, (16, TILE), 0) == ids
                marks = tn(jnp.where(match, 1.0, 0.0).astype(BF16), spread)
                query_marks[m, rows] = marks.astype(BF16)
                apart = jnp.where(used, APART * (1.0 - marks), 0.0)
                for head in range(2):
                    chosen = (lane >= 64 * head) & (lane < 64 * head + 3)
                    key_marks[head, m, rows] = jnp.where(chosen, 1.0, apart).astype(BF16)
        qkv_w.at(place.dp)[...] = qkv_shard[...]
        back_w.at(place.dp)[...] = back_shard[...]
        gate_w.at(place.dp)[...] = gate_shard[...]
        up_w.at(place.dp)[...] = up_shard[...]
        for m in range(micro_count):
            cot_all[m, own] = cotangent[m]

    prepare()
    save(down_shard, down_w.at(place.dp))
    save(tables, out_tables)
    take(0)
    take(1)
    take(2)
    normed_g[1].start()

    later = lax.broadcasted_iota(jnp.int32, (TILE, TILE), 1) > lax.broadcasted_iota(
        jnp.int32, (TILE, TILE), 0
    )
    causal = jnp.where(later, APART, 0.0)

    def project(m):
        @pl.loop(0, block_count)
        def _(block):
            rows = tile(block)
            product = nn(normed[m, rows], qkv_full[...])
            proj[m, rows] = product[:, :384]
            heads = product[:, :256]
            inverse = lax.rsqrt(head_mean(heads * heads, mixer[...]) + NORM_EPS)
            for group in range(2):
                lanes = slice(128 * group, 128 * group + 128)
                part = heads[:, lanes]
                turned = part * tables[0, rows] + swap_halves(part) * tables[1, rows]
                query[m, group, rows, 0:128] = (turned * inverse[:, lanes]).astype(BF16)
                query[m, group, rows, 128:256] = query_marks[m, rows]
            part = product[:, 256:384]
            inverse = lax.rsqrt(head_mean(part * part, mixer[0:128, 0:128]) + NORM_EPS)
            turned = (part * tables[2, rows] + swap_halves(part) * tables[3, rows]) * inverse
            moved = pltpu.roll(turned, 64, 1)
            val = product[:, 384:512]
            val_moved = pltpu.roll(val, 64, 1)
            for group in range(2):
                first, second = (turned, moved) if group == 0 else (moved, turned)
                key[m, group, 0, rows, 0:128] = jnp.where(front, first, 0.0).astype(BF16)
                key[m, group, 1, rows, 0:128] = jnp.where(front, 0.0, second).astype(BF16)
                first, second = (val, val_moved) if group == 0 else (val_moved, val)
                value[m, group, 0, rows, 0:128] = jnp.where(front, first, 0.0).astype(BF16)
                value[m, group, 1, rows, 0:128] = jnp.where(front, 0.0, second).astype(BF16)
                for head in range(2):
                    key[m, group, head, rows, 128:256] = key_marks[head, m, rows]
                value[m, group, 0, rows, 128:256] = jnp.where(front, 1.0, 0.0).astype(BF16)
                value[m, group, 1, rows, 128:256] = jnp.where(front, 0.0, 1.0).astype(BF16)

    def attend(m):
        @pl.loop(0, 2)
        def _(group):
            for block in range(block_count):
                rows = slice(block * TILE, (block + 1) * TILE)
                query_block = query[m, group, rows]
                total = jnp.zeros((TILE, 256), F32)
                for head in range(2):
                    if block > 0:
                        before = slice(0, block * TILE)
                        scores = nt(query_block, key[m, group, head, before])
                        weights = jnp.exp2(scores).astype(BF16)
                        total = total + nn(weights, value[m, group, head, before])
                    scores = nt(query_block, key[m, group, head, rows]) + causal
                    weights = jnp.exp2(scores).astype(BF16)
                    total = total + nn(weights, value[m, group, head, rows])
                sums = total[:, 128:256]
                attended[m, group, rows] = (total[:, 0:128] / sums).astype(BF16)
                shift = -jnp.log2(sums)
                high = shift.astype(BF16)
                middle_part = (shift - high.astype(F32)).astype(BF16)
                last = (shift - high.astype(F32) - middle_part.astype(F32)).astype(BF16)
                marks = jnp.where(
                    place_in == 0,
                    high.astype(F32),
                    jnp.where(
                        place_in == 1,
                        middle_part.astype(F32),
                        jnp.where(
                            place_in == 2,
                            last.astype(F32),
                            query_block[:, 128:256].astype(F32),
                        ),
                    ),
                )
                query[m, group, rows, 128:256] = marks.astype(BF16)

    def branch_block(m, step):
        rows = tile(place.block(step))
        heads = jnp.concatenate([attended[m, 0, rows], attended[m, 1, rows]], axis=1)
        return nt(heads, back_full[...])

    def branch(m):
        for step in range(3):
            branch_s(m).give(step, branch_block(m, step))

    def enter_ffn(m):
        total = branch_s(m).result(branch_block(m, 3))
        middle[m] = tokens[m].astype(F32) + total
        save(middle.at[m], out_middle.at[m])
        ffn_all[m, own] = norm_rows(middle[m], ffn_gain[...]).astype(BF16)
        ffn_g[m].start()

    @pl.loop(0, micro_count)
    def _(m):
        @pl.when(m == 0)
        def _():
            normed_g[0].relay()
            take(3)
            normed_g[0].finish()
            qkv_w.finish()

        @pl.when(m == 1)
        def _():
            normed_g[1].finish()

        project(m)

        @pl.when(m == 0)
        def _():
            take(4)
            take(5)
            cot_g[0].start()

        attend(m)

        @pl.when(m == 0)
        def _():
            normed_g[1].relay()
            back_w.finish()

        branch(m)

        @pl.when(m == 0)
        def _():
            take(6)

        branch_s(m).cross()

    save(qkv_full, out_qkv_full)
    save(back_full, out_back_full)
    for m in range(micro_count):
        save(query.at[m], out_query.at[m])
        save(key.at[m], out_key.at[m])
        save(value.at[m], out_value.at[m])
        save(attended.at[m], out_attended.at[m])
        save(proj.at[m], out_proj.at[m])
        save_columns(normed, out_normed, m)
    take(7)
    cot_g[0].relay()
    take(8)
    enter_ffn(0)
    take(9)
    enter_ffn(1)
    cot_g[0].finish()
    save(cot_all.at[0], out_cot.at[0])
    gate_w.finish()
    save(gate_full, out_gate_full)
    take(10)
    ffn_g[0].relay()
    cot_g[1].start()
    take(11)
    ffn_g[0].finish()
    save_columns(ffn_all, out_ffn, 0)
    up_w.finish()
    save(up_full, out_up_full)

    def slope_copies(index):
        m = index // block_count
        rows = tile(rem(index, block_count))
        slot = rem(index, 2)
        return [
            pltpu.make_async_copy(
                slopes.at[slot, kind], out.at[m, rows], slope_sems.at[slot, kind]
            )
            for kind, out in enumerate((out_gate_slope, out_up_slope))
        ]

    tile_count = micro_count * block_count

    @pl.loop(0, tile_count)
    def _(index):
        m = index // block_count
        rows = tile(rem(index, block_count))
        slot = rem(index, 2)

        @pl.when(index >= 2)
        def _():
            for copy in slope_copies(index - 2):
                copy.wait()

        @pl.when(index == 1)
        def _():
            take(12)

        @pl.when(index == block_count)
        def _():
            ffn_g[1].relay()
            ffn_g[1].finish()

        @pl.when(index == block_count + 3)
        def _():
            take(13)

        gate = nn(ffn_all[m, rows], gate_full[...])
        up = nn(ffn_all[m, rows], up_full[...])
        sig = 1.0 / (1.0 + jnp.exp(-gate))
        act = gate * sig
        hidden[m, rows] = (act * up).astype(BF16)
        slopes[slot, 0] = (up * (sig + act * (1.0 - sig))).astype(BF16)
        slopes[slot, 1] = act.astype(BF16)
        for copy in slope_copies(index):
            copy.start()

    save_columns(ffn_all, out_ffn, 1)
    save(hidden, out_hidden)
    for index in (tile_count - 2, tile_count - 1):
        for copy in slope_copies(index):
            copy.wait()
    cot_g[1].relay()
    take(14)
    cot_g[1].finish()
    save(cot_all.at[1], out_cot.at[1])

    @pl.loop(0, block_count)
    def _(block):
        columns = tile(block)
        grad_down[columns] = (
            tn(cot_all[0, :, columns], hidden[0]) + tn(cot_all[1, :, columns], hidden[1])
        ).astype(BF16)

    save(grad_down, out_grad_down)
    down_w.finish()
    for piece in (qkv_w, back_w, gate_w, up_w, down_w):
        piece.drain()
    for m in range(micro_count):
        normed_g[m].drain()
        cot_g[m].drain()
        ffn_g[m].drain()
        branch_s(m).drain()
    for copy in saves:
        copy.wait()


def forward(dp_size, tokens, cotangent, segments, weights, gains):
    w_query, w_key, w_value, w_out, w_gate, w_up, w_down = weights
    micro, rows, width = tokens.shape
    length = segments.shape[2]
    share, hidden_width = w_gate.shape
    qkv_width = w_query.shape[1] + w_key.shape[1] + w_value.shape[1]
    back_width = w_out.shape[0]
    turned = share % 128 != 0
    if turned:
        w_out, w_down = w_out.T, w_down.T
    outer_size = dp_size // 2
    whole = pl.BlockSpec(memory_space=pltpu.VMEM)
    anywhere = pl.BlockSpec(memory_space=pl.ANY)
    shape = jax.ShapeDtypeStruct
    out_shape = [
        shape((width, qkv_width), BF16),
        shape((width, back_width), BF16),
        shape((width, hidden_width), BF16),
        shape((width, hidden_width), BF16),
        shape((width, hidden_width), BF16),
        shape((width // TILE, micro, length, TILE), BF16),
        shape((width // TILE, micro, length, TILE), BF16),
        shape((micro, length, width), BF16),
        shape((micro, length, hidden_width), BF16),
        shape((micro, length, hidden_width), BF16),
        shape((micro, length, hidden_width), BF16),
        shape((width, hidden_width), BF16),
        shape((micro, 2, length, 256), BF16),
        shape((micro, 2, 2, length, 256), BF16),
        shape((micro, 2, 2, length, 256), BF16),
        shape((micro, 2, length, 128), BF16),
        shape((micro, length, 384), F32),
        shape((micro, rows, width), F32),
        shape((4, length, 128), F32),
    ]
    scratch = [
        pltpu.VMEM((share, qkv_width), BF16),
        pltpu.VMEM((share, back_width), BF16),
        pltpu.VMEM((share, hidden_width), BF16),
        pltpu.VMEM((4, length, 128), F32),
        pltpu.VMEM((micro, length, 128), BF16),
        pltpu.VMEM((2, micro, length, 128), BF16),
        pltpu.VMEM((256, 256), BF16),
        pltpu.VMEM((micro, length, width), BF16),
        pltpu.VMEM((micro, length, width), BF16),
        pltpu.VMEM((micro, length, width), BF16),
        pltpu.VMEM((width, qkv_width), BF16),
        pltpu.VMEM((width, back_width), BF16),
        pltpu.VMEM((width, hidden_width), BF16),
        pltpu.VMEM((width, hidden_width), BF16),
        pltpu.VMEM((2, 2, TILE, hidden_width), BF16),
        pltpu.VMEM((micro, length, hidden_width), BF16),
        pltpu.VMEM((width, hidden_width), BF16),
        pltpu.VMEM((micro, 2, length, 256), BF16),
        pltpu.VMEM((micro, 2, 2, length, 256), BF16),
        pltpu.VMEM((micro, 2, 2, length, 256), BF16),
        pltpu.VMEM((micro, 2, length, 128), BF16),
        pltpu.VMEM((micro, length, 384), F32),
        pltpu.VMEM((micro, rows, width), F32),
        pltpu.VMEM((micro, 3, rows, width), BF16),
        pltpu.VMEM((micro, 2, rows, width), BF16),
        pltpu.VMEM((micro, rows, width), BF16),
        pltpu.SemaphoreType.DMA((5, outer_size)),
        pltpu.SemaphoreType.DMA((5, outer_size)),
        pltpu.SemaphoreType.DMA((5, outer_size)),
        pltpu.SemaphoreType.DMA((5, outer_size)),
        pltpu.SemaphoreType.DMA((24,)),
        pltpu.SemaphoreType.DMA((24,)),
        pltpu.SemaphoreType.DMA((48,)),
        pltpu.SemaphoreType.DMA((2, 2)),
    ]
    operands = (
        tokens,
        cotangent,
        segments,
        w_query,
        w_key,
        w_value,
        w_out,
        w_gate,
        w_up,
        w_down,
        *gains,
        rotation_angles(length),
    )
    return pl.pallas_call(
        functools.partial(forward_kernel, dp_size, turned),
        out_shape=out_shape,
        in_specs=[whole] * len(operands),
        out_specs=[anywhere] * len(out_shape),
        scratch_shapes=scratch,
        compiler_params=pltpu.CompilerParams(
            collective_id=0, has_side_effects=True, vmem_limit_bytes=VMEM_LIMIT
        ),
        name="forward_pass",
    )(*operands)


class Shares:
    def __init__(self, place, partial, kept, from_inner, from_outer, outer_sems, inner_sems, piece):
        self.place = place
        self.partial = partial
        self.kept = kept
        self.from_inner = from_inner
        self.from_outer = from_outer
        self.outer_sems = outer_sems
        self.inner_sems = inner_sems
        self.piece = piece
        self.rows = from_inner.shape[1]

    def at(self, index):
        return self.partial.at[pl.ds(pl.multiple_of(index * self.rows, self.rows), self.rows), :]

    def mine(self, shift):
        if self.kept is not None:
            return self.kept.at[shift]
        return self.at(self.place.ahead(shift))

    def inner_copy(self, shift):
        place = self.place
        return place.copy(
            self.at(place.ahead(shift, 1 - place.inner)),
            self.from_inner.at[shift],
            self.inner_sems,
            (self.piece, shift),
            dp=place.other,
        )

    def outer_copy(self, shift):
        place = self.place
        return place.copy(
            self.mine(shift),
            self.from_outer.at[shift - 1],
            self.outer_sems,
            (self.piece, shift),
            dp=place.ahead(shift),
        )

    def give(self, first, last):
        @pl.loop(first, last)
        def _(shift):
            self.inner_copy(shift).start()

    def turn(self, first, last):
        @pl.loop(first, last)
        def _(shift):
            self.inner_copy(shift).wait_recv()
            mine = self.mine(shift)
            mine[...] = (mine[...].astype(F32) + self.from_inner[shift].astype(F32)).astype(BF16)
            self.outer_copy(shift).start()

    def keep(self, total):
        self.inner_copy(0).wait_recv()
        total[...] = self.mine(0)[...].astype(F32) + self.from_inner[0].astype(F32)

    def finish(self, total):
        @pl.loop(1, self.place.outer_size)
        def _(shift):
            self.outer_copy(shift).wait_recv()
            total[...] += self.from_outer[shift - 1].astype(F32)

    def drain(self):
        self.inner_copy(0).wait_send()

        @pl.loop(1, self.place.outer_size)
        def _(shift):
            self.inner_copy(shift).wait_send()
            self.outer_copy(shift).wait_send()


def backward_kernel(
    dp_size,
    cotangent,
    attn_gain,
    ffn_gain,
    tokens,
    qkv_full,
    back_full,
    gate_full,
    up_full,
    down_full,
    normed,
    ffn_all,
    cot_all,
    gate_slope,
    up_slope,
    hidden,
    grad_down,
    query,
    key,
    value,
    attended,
    proj,
    middle_in,
    tables,
    out_mixed,
    out_tokens,
    gain_sums,
    out_qkv,
    out_back,
    out_gate,
    out_up,
    out_down,
    mixed,
    mid_all,
    mixer,
    ffn_w,
    down_w,
    qkv_w,
    att,
    qry,
    ky,
    val,
    prj,
    down_kept,
    qkv_inner,
    back_inner,
    ffn_inner,
    down_inner,
    qkv_outer,
    back_outer,
    ffn_outer,
    down_outer,
    staged,
    part_twin,
    part_across,
    out_twin,
    out_across,
    middle,
    gain_parts,
    gain_packed,
    gain_group,
    gain_dp,
    outer_send,
    outer_recv,
    inner_send,
    inner_recv,
    group_send,
    group_recv,
    gain_send,
    gain_recv,
    local_sems,
    tile_sems,
):
    place = Place(dp_size)
    micro_count = mixed.shape[0]
    length = mid_all.shape[1]
    width = mid_all.shape[2]
    hidden_width = down_w.shape[1]
    block_count = length // TILE
    tile_count = micro_count * block_count
    outer_size = place.outer_size
    group_sems = (group_send, group_recv)
    outer_sems = (outer_send, outer_recv)
    inner_sems = (inner_send, inner_recv)
    own = tile(place.tensor)
    first_cut = 1 + (outer_size - 1) // 3
    second_cut = 1 + 2 * (outer_size - 1) // 3
    outers = outer_size // 4
    own_outer_block = place.outer // outers
    counter = []

    def load(src, dst):
        copy = pltpu.make_async_copy(src, dst, local_sems.at[len(counter) + (8 if len(counter) >= 8 else 0)])
        counter.append(copy)
        copy.start()
        return copy

    down_s = Shares(place, grad_down, down_kept, down_inner, down_outer, outer_sems, inner_sems, 4)

    def ffn_shares(kind):
        return Shares(
            place,
            ffn_w.at[kind],
            None,
            ffn_inner.at[kind],
            ffn_outer.at[kind],
            outer_sems,
            inner_sems,
            2 + kind,
        )

    gate_s, up_s = ffn_shares(0), ffn_shares(1)
    mid_g = [Gather(place, mid_all, m, group_sems, 3 * m) for m in range(micro_count)]

    def turn_block(step):
        return rem(step + 1 + own_outer_block, 4)

    cuts = (1, first_cut, second_cut, outer_size)

    def issue(share, part):
        share.give(*((0, 1) if part == 3 else (cuts[part], cuts[part + 1])))

    def take(share, part):
        share.turn(cuts[part], cuts[part + 1])

    def twin_copy(kind, m, half):
        from_twin = (part_twin, out_twin, part_twin)[kind]
        return place.copy(
            staged.at[m, half],
            from_twin.at[m, half],
            group_sems,
            6 + 6 * kind + 3 * m + half,
            tensor=place.twin,
        )

    def across_copy(kind, m):
        from_across = (part_across, out_across, part_across)[kind]
        return place.copy(
            staged.at[m, 2],
            from_across.at[m],
            group_sems,
            6 + 6 * kind + 3 * m + 2,
            tensor=place.across,
        )

    def block_of(step):
        side = jnp.where(step < 2, 1 - place.side, place.side)
        core = jnp.where(rem(step, 2) == 0, 1 - place.core, place.core)
        return side * 2 + core

    def hand_out(m, step, values):
        staged[m, rem(step, 2) * 2 + step // 2] = values.astype(BF16)

    def send_twin(kind, m, step):
        @pl.when(rem(step, 2) == 0)
        def _():
            twin_copy(kind, m, step // 2).start()

    def cross(kind, m):
        from_twin = (part_twin, out_twin, part_twin)[kind]
        twin_copy(kind, m, 0).wait_recv()
        staged[m, 2] = (staged[m, 2].astype(F32) + from_twin[m, 0].astype(F32)).astype(BF16)
        across_copy(kind, m).start()

    def collect(kind, m):
        from_twin = (part_twin, out_twin, part_twin)[kind]
        from_across = (part_across, out_across, part_across)[kind]
        twin_copy(kind, m, 1).wait_recv()
        across_copy(kind, m).wait_recv()
        return staged[m, 3].astype(F32) + from_twin[m, 1].astype(F32) + from_across[m].astype(F32)

    def drain(kind, m):
        twin_copy(kind, m, 0).wait_send()
        twin_copy(kind, m, 1).wait_send()
        across_copy(kind, m).wait_send()

    def leave_ffn(m):
        upstream = collect(0, m)
        back, term = norm_rows_back(middle[m], ffn_gain[...], upstream)
        mid_all[m, own] = (mixed[m].astype(F32) + back).astype(BF16)
        mid_g[m].start()
        gain_parts[1:2, :] += term

    def leave_out(m):
        mixed[m] = (middle[m] + collect(1, m)).astype(BF16)

    def attn_copies():
        pairs = (
            (back_full, qkv_w.at[:, 512:768]),
            (attended, att),
            (value.at[0], val),
            (key.at[0], ky),
            (query.at[0], qry),
            (proj.at[0], prj),
            (qkv_full, qkv_w.at[:, 0:512]),
        )
        return [
            pltpu.make_async_copy(src, dst, local_sems.at[30 + index])
            for index, (src, dst) in enumerate(pairs)
        ]

    def rows_of(index):
        return index // block_count, tile(block_of(rem(index, block_count)))

    def ffn_phase(grads, rows_buf, ffn_cols):
        def rows_copy(index):
            m, rows = rows_of(index)
            slot = rem(index, 2)
            return pltpu.make_async_copy(cot_all.at[m, rows], rows_buf.at[slot], tile_sems.at[0, slot])

        def cols_copy(index):
            slot = rem(index, 2)
            return pltpu.make_async_copy(
                ffn_all.at[turn_block(rem(index, block_count))], ffn_cols.at[slot], tile_sems.at[2, slot]
            )

        loads = [load(down_full, down_w)]
        rows_copy(0).start()
        loads += [load(gate_slope.at[0], grads.at[0, 0]), load(up_slope.at[0], grads.at[1, 0])]
        loads += [load(gate_full, ffn_w.at[0]), load(up_full, ffn_w.at[1])]
        others = [
            load(gate_slope.at[1], grads.at[0, 1]),
            load(up_slope.at[1], grads.at[1, 1]),
            load(middle_in, middle),
            load(cotangent, mixed),
        ]

        def kept_copy(shift):
            return pltpu.make_async_copy(
                down_s.at(place.ahead(shift)), down_kept.at[shift], local_sems.at[40 + shift]
            )

        @pl.loop(0, outer_size)
        def _(shift):
            kept_copy(shift).start()

        fill_mixer(mixer)
        gain_parts[...] = jnp.zeros_like(gain_parts)
        gain_packed[...] = jnp.zeros_like(gain_packed)
        place.greet(True)
        issue(down_s, 0)
        issue(down_s, 1)
        for copy in loads:
            copy.wait()

        @pl.loop(0, tile_count)
        def _(index):
            m, rows = rows_of(index)
            step = rem(index, block_count)
            slot = rem(index, 2)

            @pl.when(index + 1 < tile_count)
            def _():
                rows_copy(index + 1).start()

            @pl.when(index == block_count)
            def _():
                pltpu.make_async_copy(gate_slope.at[1], grads.at[0, 1], local_sems.at[5]).wait()
                pltpu.make_async_copy(up_slope.at[1], grads.at[1, 1], local_sems.at[6]).wait()

            @pl.when(index == 2)
            def _():
                @pl.loop(0, outer_size)
                def _(shift):
                    kept_copy(shift).wait()

                take(down_s, 0)
                issue(down_s, 2)

            @pl.when(index == block_count + 1)
            def _():
                take(down_s, 1)
                issue(down_s, 3)

            rows_copy(index).wait()
            hidden_grad = nn(rows_buf[slot], down_w[...])
            gate_low = (hidden_grad * grads[0, m, rows].astype(F32)).astype(BF16)
            up_low = (hidden_grad * grads[1, m, rows].astype(F32)).astype(BF16)
            grads[0, m, rows] = gate_low
            grads[1, m, rows] = up_low
            hand_out(m, step, nt(gate_low, ffn_w[0]) + nt(up_low, ffn_w[1]))

            send_twin(0, m, step)

            @pl.when(index == 2)
            def _():
                cross(0, 0)

        for copy in attn_copies():
            copy.start()
        cols_copy(0).start()
        for copy in others[2:]:
            copy.wait()
        leave_ffn(0)
        cross(0, 1)

        @pl.loop(0, 2 * block_count)
        def _(index):
            kind = index // block_count
            block = turn_block(rem(index, block_count))
            slot = rem(index, 2)
            cols_copy(index).wait()

            @pl.when(index + 1 < 2 * block_count)
            def _():
                cols_copy(index + 1).start()

            ffn_w[kind, tile(block)] = (
                tn(ffn_cols[slot, 0], grads[kind, 0]) + tn(ffn_cols[slot, 1], grads[kind, 1])
            ).astype(BF16)

            @pl.when(index == 1)
            def _():
                take(down_s, 2)
                if outers == 1:
                    issue(gate_s, 0)

            @pl.when(index == block_count - 1)
            def _():
                if outers > 1:
                    issue(gate_s, 0)
                issue(gate_s, 1)

            @pl.when(index == block_count + 3)
            def _():
                take(gate_s, 0)
                issue(gate_s, 2)

    pl.run_scoped(
        ffn_phase,
        pltpu.VMEM((2, micro_count, length, hidden_width), BF16),
        pltpu.VMEM((2, TILE, width), BF16),
        pltpu.VMEM((2, micro_count, length, TILE), BF16),
    )

    def attn_phase(
        toks,
        tabs,
        hidden_buf,
        grad_att,
        grad_q,
        grad_k,
        grad_v,
        grad_qkv,
        qkv_total,
        back_total,
        gate_total,
        up_total,
        down_total,
    ):
        qkv_part = down_w.at[:, 0:512]
        back_part = down_w.at[:, 512:768]
        qkv_s = Shares(place, qkv_part, None, qkv_inner, qkv_outer, outer_sems, inner_sems, 0)
        back_s = Shares(place, back_part, None, back_inner, back_outer, outer_sems, inner_sems, 1)
        lane = lax.broadcasted_iota(jnp.int32, (TILE, 128), 1)
        front = lane < 64
        place_in = rem(lane, 64)
        later = lax.broadcasted_iota(jnp.int32, (TILE, TILE), 0) > lax.broadcasted_iota(
            jnp.int32, (TILE, TILE), 1
        )
        causal = jnp.where(later, APART, 0.0)
        small = mixer[0:128, 0:128]
        table_load = load(tables, tabs)
        token_load = load(tokens, toks)

        def score_ready(m):
            @pl.loop(0, block_count)
            def _(block):
                rows = tile(block)
                low = nn(mid_all[m, rows], qkv_w[:, 512:768]).astype(BF16)
                for group in range(2):
                    part = low[:, 128 * group : 128 * group + 128]
                    both = part.astype(F32) * att[m, group, rows].astype(F32)
                    shift = head_mean(both, small) * -64.0
                    high = shift.astype(BF16)
                    rest = shift - high.astype(F32)
                    mid = rest.astype(BF16)
                    last = (rest - mid.astype(F32)).astype(BF16)
                    marks = jnp.where(
                        place_in == 0,
                        high.astype(F32),
                        jnp.where(
                            place_in == 1,
                            mid.astype(F32),
                            jnp.where(place_in == 2, last.astype(F32), 0.0),
                        ),
                    )
                    grad_att[group, rows, 0:128] = part
                    grad_att[group, rows, 128:256] = marks.astype(BF16)

        def attend_back(m, between):
            @pl.loop(0, 2)
            def _(group):
                for block in range(block_count):
                    rows = slice(block * TILE, (block + 1) * TILE)
                    spans = [(rows, True)]
                    if block + 1 < block_count:
                        spans.append((slice((block + 1) * TILE, length), False))
                    sums_k = []
                    sums_v = []
                    for head in range(2):
                        key_block = ky[group, head, rows]
                        value_block = val[group, head, rows]
                        sum_k = None
                        sum_v = None
                        for span, masked in spans:
                            query_span = qry[group, span]
                            grad_span = grad_att[group, span]
                            scores = nt(key_block, query_span)
                            if masked:
                                scores = scores + causal
                            probs = jnp.exp2(scores)
                            score_grad = (probs * nt(value_block, grad_span)).astype(BF16)
                            probs_low = probs.astype(BF16)
                            part_v = nn(probs_low, grad_span[:, 0:128])
                            part_k = nn(score_grad, query_span[:, 0:128])
                            sum_v = part_v if sum_v is None else sum_v + part_v
                            sum_k = part_k if sum_k is None else sum_k + part_k
                            part_q = tn(score_grad, key_block[:, 0:128])
                            if block == 0 and head == 0:
                                grad_q[group, span] = part_q
                            else:
                                grad_q[group, span] += part_q
                        sums_k.append(sum_k)
                        sums_v.append(sum_v)
                    both_k = jnp.where(front, sums_k[0], sums_k[1])
                    both_v = jnp.where(front, sums_v[0], sums_v[1])
                    grad_k[group, rows] = both_k + pltpu.roll(both_k, 64, 1)
                    grad_v[group, rows] = both_v + pltpu.roll(both_v, 64, 1)

                between(group)

        def normalize_back(grads, values, cosine, sine):
            scaled = grads * LN2
            weighted = scaled * cosine + swap_halves(scaled * sine)
            inverse = lax.rsqrt(head_mean(values * values, small) + NORM_EPS)
            unit = values * inverse
            both = weighted * unit
            back = inverse * (weighted - unit * head_mean(both, small))
            return back.astype(BF16), jnp.sum(both, axis=0, keepdims=True)

        def leave_heads(m):
            @pl.loop(0, block_count)
            def _(block):
                rows = tile(block)
                cosine, sine = tabs[0, rows], tabs[1, rows]
                for group in range(2):
                    lanes = slice(128 * group, 128 * group + 128)
                    back, term = normalize_back(grad_q[group, rows], prj[rows, lanes], cosine, sine)
                    grad_qkv[m, rows, lanes] = back
                    gain_parts[2:3, 0:128] += term
                back, term = normalize_back(
                    jnp.where(front, grad_k[0, rows], grad_k[1, rows]),
                    prj[rows, 256:384],
                    tabs[2, rows],
                    tabs[3, rows],
                )
                grad_qkv[m, rows, 256:384] = back
                gain_parts[2:3, 128:256] += term
                grad_qkv[m, rows, 384:512] = jnp.where(
                    front, grad_v[0, rows], grad_v[1, rows]
                ).astype(BF16)

        def enter_norm(m):
            drain(1, m)

            @pl.loop(0, block_count)
            def _(step):
                rows = tile(block_of(step))
                hand_out(m, step, nt(grad_qkv[m, rows], qkv_w[:, 0:512]))
                send_twin(2, m, step)

            cross(2, m)

        def leave_attn(m):
            upstream = collect(2, m)
            back, term = norm_rows_back(toks[m].astype(F32), attn_gain[...], upstream)
            middle[m] = mid_all[m, own].astype(F32) + back
            gain_parts[0:1, :] += term

        def norm_copies():
            return [
                pltpu.make_async_copy(
                    normed.at[turn_block(step)], norm_cols.at[step % 2], local_sems.at[24 + step]
                )
                for step, norm_cols in enumerate((ky, ky, val, val))
            ]

        reloads = ((value, val), (key, ky), (query, qry), (proj, prj))

        def reload_copy(index):
            src, dst = reloads[index]
            return pltpu.make_async_copy(src.at[1], dst, local_sems.at[10 + index])

        def mixed_save(m):
            return pltpu.make_async_copy(mixed.at[m], out_mixed.at[m], local_sems.at[14 + m])

        def enter_back():
            @pl.loop(0, block_count)
            def _(step):
                block = turn_block(step)
                columns = tile(block)
                total = jnp.zeros((TILE, 256), F32)
                for m in range(micro_count):
                    heads = jnp.concatenate([att[m, 0], att[m, 1]], axis=1)
                    total = total + tn(mid_all[m, :, columns], heads)
                back_part[columns] = total.astype(BF16)

        def hidden_copy(index):
            m, rows = rows_of(index)
            slot = rem(index, block_count)
            return pltpu.make_async_copy(
                hidden.at[m, rows], hidden_buf.at[slot], local_sems.at[24 + slot]
            )

        def enter_out():
            for m in range(micro_count):
                drain(0, m)

            @pl.loop(0, tile_count)
            def _(index):
                m = index // block_count
                step = rem(index, block_count)
                hidden_copy(index).wait()
                hand_out(m, step, nt(hidden_buf[step], down_w[...]))
                send_twin(1, m, step)

                @pl.when(index + block_count < tile_count)
                def _():
                    hidden_copy(index + block_count).start()

                @pl.when(index == block_count)
                def _():
                    take(up_s, 0)
                    issue(up_s, 2)

        for slot in range(block_count):
            hidden_copy(slot).start()
        for copy in attn_copies():
            copy.wait()
        down_s.keep(down_total)
        mid_g[0].relay()
        mid_g[0].finish()

        @pl.loop(0, micro_count)
        def _(m):
            score_ready(m)

            @pl.when(m == 0)
            def _():
                take(gate_s, 1)
                issue(gate_s, 3)

            @pl.when(m == 1)
            def _():
                take(up_s, 1)
                issue(up_s, 3)
                enter_back()

            def between(group):
                @pl.when((m == 0) & (group == 0))
                def _():
                    take(gate_s, 2)
                    issue(up_s, 0)
                    leave_ffn(1)

                @pl.when((m == 0) & (group == 1))
                def _():
                    gate_s.keep(gate_total)
                    issue(up_s, 1)

                @pl.when((m == 1) & (group == 0))
                def _():
                    take(up_s, 2)
                    issue(back_s, 0)
                    issue(back_s, 1)
                    leave_out(0)
                    mixed_save(0).start()
                    enter_norm(0)

                @pl.when((m == 1) & (group == 1))
                def _():
                    up_s.keep(up_total)
                    issue(back_s, 2)
                    issue(back_s, 3)

            attend_back(m, between)

            @pl.when(m == 0)
            def _():
                for index in range(3):
                    reload_copy(index).start()
                table_load.wait()

            @pl.when(m == 1)
            def _():
                for copy in norm_copies():
                    copy.start()

            leave_heads(m)

            @pl.when(m == 0)
            def _():
                reload_copy(3).start()
                enter_out()
                mid_g[1].relay()
                cross(1, 0)
                cross(1, 1)
                mid_g[1].finish()
                for index in range(4):
                    reload_copy(index).wait()

        leave_out(1)
        mixed_save(1).start()
        enter_norm(1)
        token_load.wait()
        saves = [mixed_save(m) for m in range(micro_count)]
        down_s.finish(down_total)
        saves.append(load(down_total, out_down))
        gate_s.finish(gate_total)
        saves.append(load(gate_total, out_gate))

        for half, norm_cols in enumerate((ky, val)):

            @pl.loop(2 * half, 2 * half + 2)
            def _(step):
                slot = step - 2 * half
                pltpu.make_async_copy(
                    normed.at[turn_block(step)], norm_cols.at[slot], local_sems.at[24 + step]
                ).wait()
                qkv_part[tile(turn_block(step))] = (
                    tn(norm_cols[slot, 0], grad_qkv[0]) + tn(norm_cols[slot, 1], grad_qkv[1])
                ).astype(BF16)
                if outers == 1:
                    qkv_s.inner_copy(rem(step + 1, outer_size)).start()

        if outers > 1:
            for part in range(4):
                issue(qkv_s, part)
        for part in range(3):
            take(back_s, part)
        leave_attn(0)
        saves.append(load(middle.at[0], out_tokens.at[0]))
        back_s.keep(back_total)
        for part in range(3):
            take(qkv_s, part)
        leave_attn(1)
        saves.append(load(middle.at[1], out_tokens.at[1]))

        def group_gain(shift):
            return place.copy(
                gain_packed,
                gain_group.at[shift - 1],
                (gain_send, gain_recv),
                shift - 1,
                tensor=rem(place.tensor + shift, 4),
            )

        pack_gains(gain_packed, gain_parts)
        for shift in range(1, 4):
            group_gain(shift).start()
        qkv_s.keep(qkv_total)
        up_s.finish(up_total)
        saves.append(load(up_total, out_up))
        back_s.finish(back_total)
        saves.append(load(back_total, out_back))
        for shift in range(1, 4):
            group_gain(shift).wait_recv()
        gain_dp[0] = gain_packed[...] + gain_group[0] + gain_group[1] + gain_group[2]

        def dp_gain(shift):
            return place.copy(
                gain_dp.at[0],
                gain_dp.at[shift],
                (gain_send, gain_recv),
                2 + shift,
                dp=rem(place.dp + shift, dp_size),
            )

        @pl.loop(1, dp_size)
        def _(shift):
            dp_gain(shift).start()

        qkv_s.finish(qkv_total)
        saves.append(load(qkv_total, out_qkv))
        gain_sums[...] = gain_dp[0]

        @pl.loop(1, dp_size)
        def _(shift):
            dp_gain(shift).wait_recv()
            gain_sums[...] += gain_dp[shift]

        for shift in range(1, 4):
            group_gain(shift).wait_send()

        @pl.loop(1, dp_size)
        def _(shift):
            dp_gain(shift).wait_send()

        qkv_s.drain()
        back_s.drain()
        for copy in saves:
            copy.wait()

    pl.run_scoped(
        attn_phase,
        pltpu.VMEM(tokens.shape, BF16),
        pltpu.VMEM(tables.shape, F32),
        pltpu.VMEM((block_count, TILE, hidden_width), BF16),
        pltpu.VMEM((2, length, 256), BF16),
        pltpu.VMEM((2, length, 128), F32),
        pltpu.VMEM((2, length, 128), F32),
        pltpu.VMEM((2, length, 128), F32),
        pltpu.VMEM((micro_count, length, 512), BF16),
        *[
            pltpu.VMEM((width // dp_size, w), F32)
            for w in (512, 256, hidden_width, hidden_width, hidden_width)
        ],
    )
    for share in (down_s, gate_s, up_s):
        share.drain()
    for m in range(micro_count):
        mid_g[m].drain()
        drain(2, m)


def backward(dp_size, cotangent, attn_gain, ffn_gain, tokens, saved):
    micro, rows, width = tokens.shape
    length = saved[7].shape[1]
    hidden_width = saved[2].shape[1]
    outer_size = dp_size // 2
    share = width // dp_size
    whole = pl.BlockSpec(memory_space=pltpu.VMEM)
    anywhere = pl.BlockSpec(memory_space=pl.ANY)
    shape = jax.ShapeDtypeStruct
    widths = (512, 256, hidden_width, hidden_width, hidden_width)
    out_shape = [
        shape((micro, rows, width), BF16),
        shape((micro, rows, width), F32),
        shape((8, 384), F32),
    ] + [shape((share, w), F32) for w in widths]
    scratch = (
        [pltpu.VMEM((micro, rows, width), BF16)]
        + [
            pltpu.VMEM((micro, length, width), BF16),
            pltpu.VMEM((256, 256), BF16),
            pltpu.VMEM((2, width, hidden_width), BF16),
            pltpu.VMEM((width, hidden_width), BF16),
            pltpu.VMEM((width, 768), BF16),
            pltpu.VMEM((micro, 2, length, 128), BF16),
            pltpu.VMEM((2, length, 256), BF16),
            pltpu.VMEM((2, 2, length, 256), BF16),
            pltpu.VMEM((2, 2, length, 256), BF16),
            pltpu.VMEM((length, 384), F32),
            pltpu.VMEM((outer_size, share, hidden_width), BF16),
            pltpu.VMEM((outer_size, share, 512), BF16),
            pltpu.VMEM((outer_size, share, 256), BF16),
            pltpu.VMEM((2, outer_size, share, hidden_width), BF16),
            pltpu.VMEM((outer_size, share, hidden_width), BF16),
            pltpu.VMEM((outer_size - 1, share, 512), BF16),
            pltpu.VMEM((outer_size - 1, share, 256), BF16),
            pltpu.VMEM((2, outer_size - 1, share, hidden_width), BF16),
            pltpu.VMEM((outer_size - 1, share, hidden_width), BF16),
            pltpu.VMEM((micro, 4, rows, width), BF16),
            pltpu.VMEM((micro, 2, rows, width), BF16),
            pltpu.VMEM((micro, rows, width), BF16),
            pltpu.VMEM((micro, 2, rows, width), BF16),
            pltpu.VMEM((micro, rows, width), BF16),
            pltpu.VMEM((micro, rows, width), F32),
            pltpu.VMEM((8, width), F32),
            pltpu.VMEM((8, 384), F32),
            pltpu.VMEM((3, 8, 384), F32),
            pltpu.VMEM((dp_size, 8, 384), F32),
        ]
        + [pltpu.SemaphoreType.DMA((5, outer_size))] * 4
        + [pltpu.SemaphoreType.DMA((24,))] * 2
        + [pltpu.SemaphoreType.DMA((dp_size + 2,))] * 2
        + [pltpu.SemaphoreType.DMA((40 + outer_size,)), pltpu.SemaphoreType.DMA((4, 2))]
    )
    return pl.pallas_call(
        functools.partial(backward_kernel, dp_size),
        out_shape=out_shape,
        in_specs=[anywhere, whole, whole] + [anywhere] * (1 + len(saved)),
        out_specs=[anywhere, anywhere, whole] + [anywhere] * 5,
        scratch_shapes=scratch,
        compiler_params=pltpu.CompilerParams(
            collective_id=1, has_side_effects=True, vmem_limit_bytes=VMEM_LIMIT
        ),
        name="backward_pass",
    )(cotangent, attn_gain, ffn_gain, tokens, *saved)


def deliver_kernel(
    turned,
    in_mixed,
    in_tokens,
    gains,
    query_gain,
    key_gain,
    in_qkv,
    in_back,
    in_gate,
    in_up,
    in_down,
    mixed,
    grad_tokens,
    attn_gain,
    ffn_gain,
    query_term,
    key_term,
    grad_query,
    grad_key,
    grad_value,
    grad_out,
    grad_gate,
    grad_up,
    grad_down,
    buf_mixed,
    buf_tokens,
    buf_gate,
    buf_up,
    buf_qkv,
    buf_back,
    buf_down,
    sems,
):
    flows = [
        (in_qkv, buf_qkv, None),
        (in_back, buf_back, None),
        (in_down, buf_down, None),
        (in_mixed, buf_mixed, mixed),
        (in_tokens.at[0], buf_tokens.at[0], grad_tokens.at[0]),
        (in_tokens.at[1], buf_tokens.at[1], grad_tokens.at[1]),
        (in_gate, buf_gate, grad_gate),
        (in_up, buf_up, grad_up),
    ]
    arrivals = [
        pltpu.make_async_copy(src, buf, sems.at[0, index]) for index, (src, buf, _) in enumerate(flows)
    ]
    departures = []
    for copy in arrivals:
        copy.start()
    part = 0
    for out in (attn_gain, ffn_gain):
        for start in range(0, out.shape[1], 128):
            out[:, start : start + 128] = gains[
                part // 3 : part // 3 + 1, 128 * (part % 3) : 128 * (part % 3) + 128
            ]
            part += 1
    for out, gain in ((query_term, query_gain), (key_term, key_gain)):
        term = gains[part // 3 : part // 3 + 1, 128 * (part % 3) : 128 * (part % 3) + 128]
        out[...] = term[:, :DH] / gain[...] + term[:, DH:] / gain[...]
        part += 1
    for index, (_, buf, dst) in enumerate(flows):
        arrivals[index].wait()
        if dst is not None:
            copy = pltpu.make_async_copy(buf, dst, sems.at[1, index])
            copy.start()
            departures.append(copy)
        if index == 2:
            grad_query[...] = buf_qkv[:, 0:256]
            grad_key[...] = buf_qkv[:, 256:384]
            grad_value[...] = buf_qkv[:, 384:512]
            grad_out[...] = buf_back[...] if turned else buf_back[...].T
            grad_down[...] = buf_down[...] if turned else buf_down[...].T
    for copy in departures:
        copy.wait()


def deliver(results, query_gain, key_gain):
    mixed, grad_tokens, gains, qkv, back, gate, up, down = results
    turned = qkv.shape[0] % 128 != 0
    whole = pl.BlockSpec(memory_space=pltpu.VMEM)
    anywhere = pl.BlockSpec(memory_space=pl.ANY)
    stored = pl.BlockSpec(memory_space=pltpu.HBM)
    shape = jax.ShapeDtypeStruct
    share, width = qkv.shape[0], mixed.shape[2]

    def facing(array):
        return array.shape if turned else array.shape[::-1]

    out_shape = [
        shape(mixed.shape, BF16),
        shape(grad_tokens.shape, F32),
        shape((1, width), F32),
        shape((1, width), F32),
        shape((1, DH), F32),
        shape((1, DH), F32),
        shape((share, 256), F32),
        shape((share, 128), F32),
        shape((share, 128), F32),
        shape(facing(back), F32),
        shape(gate.shape, F32),
        shape(up.shape, F32),
        shape(facing(down), F32),
    ]
    out = pl.pallas_call(
        functools.partial(deliver_kernel, turned),
        out_shape=out_shape,
        in_specs=[stored, stored] + [whole] * 3 + [stored] * 5,
        out_specs=[anywhere, anywhere] + [whole] * 8 + [anywhere, anywhere, whole],
        scratch_shapes=[
            pltpu.VMEM(mixed.shape, BF16),
            pltpu.VMEM(grad_tokens.shape, F32),
            pltpu.VMEM(gate.shape, F32),
            pltpu.VMEM(up.shape, F32),
            pltpu.VMEM(qkv.shape, F32),
            pltpu.VMEM(back.shape, F32),
            pltpu.VMEM(down.shape, F32),
            pltpu.SemaphoreType.DMA((2, 8)),
        ],
        compiler_params=pltpu.CompilerParams(vmem_limit_bytes=VMEM_LIMIT),
        name="deliver_pass",
    )(mixed, grad_tokens, gains, query_gain, key_gain, qkv, back, gate, up, down)
    out = list(out)
    if turned:
        out[9], out[12] = out[9].T, out[12].T
    return out


def shards(
    dp_size,
    tokens,
    segment_ids,
    attn_gain,
    query_gain,
    key_gain,
    w_query,
    w_key,
    w_value,
    w_out,
    ffn_gain,
    w_gate,
    w_up,
    w_down,
    cotangent,
):
    own_tokens, own_cot = tokens[:, 0], cotangent[:, 0]
    attn_row, ffn_row = attn_gain[None], ffn_gain[None]
    saved = forward(
        dp_size,
        own_tokens,
        own_cot,
        segment_ids,
        (w_query, w_key, w_value, w_out, w_gate, w_up, w_down),
        (attn_row, ffn_row, query_gain[None], key_gain[None]),
    )
    results = backward(dp_size, own_cot, attn_row, ffn_row, own_tokens, saved)
    (
        mixed,
        grad_tokens,
        attn_term,
        ffn_term,
        query_term,
        key_term,
        grad_query,
        grad_key,
        grad_value,
        grad_out,
        grad_gate,
        grad_up,
        grad_down,
    ) = deliver(results, query_gain[None], key_gain[None])
    return (
        mixed[:, None],
        grad_tokens[:, None],
        attn_term[0],
        query_term[0],
        key_term[0],
        grad_query,
        grad_key,
        grad_value,
        grad_out,
        ffn_term[0],
        grad_gate,
        grad_up,
        grad_down,
    )


def solution(mesh):
    sequence = P(None, "dp", "tensor", None)
    rows = P("dp", "tensor")
    columns = P("tensor", "dp")
    return jax.shard_map(
        functools.partial(shards, mesh.shape["dp"]),
        mesh=mesh,
        in_specs=(sequence, P(None, "dp", None), P(), P(), P(), rows, rows, rows, columns, P(), rows, rows, columns, sequence),
        out_specs=(sequence, sequence, P(), P(), P(), rows, rows, rows, columns, P(), rows, rows, columns),
        check_vma=False,
    )
```

```python
import functools
import math

import jax
import jax.numpy as jnp
import numpy as np
from jax import lax
from jax.experimental import pallas as pl
from jax.experimental.pallas import tpu as pltpu
from jax.sharding import PartitionSpec as P

MESH = pl.DeviceIdType.MESH
VMEM_LIMIT = 67000000
NORM_EPS = 1e-05
ROPE_BASE = 1000000.0
DH = 64
TILE = 256
LN2 = math.log(2.0)
APART = -32768.0
BF16 = jnp.bfloat16
F32 = jnp.float32


def nn(left, right):
    return lax.dot_general(left, right, (((1,), (0,)), ((), ())), preferred_element_type=F32)


def nt(left, right):
    return lax.dot_general(left, right, (((1,), (1,)), ((), ())), preferred_element_type=F32)


def tn(left, right):
    return lax.dot_general(left, right, (((0,), (0,)), ((), ())), preferred_element_type=F32)


def tile(index, size=TILE):
    return pl.ds(pl.multiple_of(index * size, size), size)


def rem(value, divisor):
    return value % divisor if isinstance(value, int) else lax.rem(value, divisor)


def low_parts(values):
    high = values.astype(BF16)
    return high, (values - high.astype(F32)).astype(BF16)


def head_mean(values, mixer):
    high, rest = low_parts(values)
    return nn(high, mixer) + nn(rest, mixer)


def swap_halves(values):
    lane = lax.broadcasted_iota(jnp.int32, values.shape, 1)
    ahead = pltpu.roll(values, 96, 1)
    behind = pltpu.roll(values, 32, 1)
    return jnp.where(lax.rem(lane, 64) < 32, ahead, behind)


def norm_rows(values, gain):
    inverse = lax.rsqrt(jnp.mean(values * values, axis=-1, keepdims=True) + NORM_EPS)
    return values * inverse * gain


def norm_rows_back(values, gain, upstream):
    inverse = lax.rsqrt(jnp.mean(values * values, axis=-1, keepdims=True) + NORM_EPS)
    scaled = values * inverse
    weighted = upstream * gain
    back = inverse * (weighted - scaled * jnp.mean(weighted * scaled, axis=-1, keepdims=True))
    return back, jnp.sum(upstream * scaled, axis=0, keepdims=True)


class Place:
    def __init__(self, dp_size):
        self.dp_size = dp_size
        self.dp = lax.axis_index("dp")
        self.tensor = lax.axis_index("tensor")
        self.outer_size = dp_size // 2
        self.outer = self.dp // 2
        self.inner = lax.rem(self.dp, 2)
        self.other = self.outer * 2 + 1 - self.inner
        self.side = self.tensor // 2
        self.core = lax.rem(self.tensor, 2)
        self.across = (1 - self.side) * 2 + self.core
        self.twin = self.side * 2 + 1 - self.core

    def ahead(self, shift, inner=None):
        inner = self.inner if inner is None else inner
        return lax.rem(self.outer + shift, self.outer_size) * 2 + inner

    def behind(self, shift):
        return lax.rem(self.outer - shift + self.outer_size, self.outer_size) * 2 + self.inner

    def block(self, step):
        side = 1 - self.side if step < 2 else self.side
        core = 1 - self.core if step % 2 == 0 else self.core
        return side * 2 + core

    def copy(self, src, dst, sems, index, dp=None, tensor=None):
        return pltpu.make_async_remote_copy(
            src_ref=src,
            dst_ref=dst,
            send_sem=sems[0].at[index],
            recv_sem=sems[1].at[index],
            device_id=(
                self.dp if dp is None else dp,
                self.tensor if tensor is None else tensor,
            ),
            device_id_type=MESH,
        )

    def greet(self, everyone):
        barrier = pltpu.get_barrier_semaphore()

        def signal(dp, tensor):
            pl.semaphore_signal(barrier, inc=1, device_id=(dp, tensor), device_id_type=MESH)

        if everyone:

            @pl.loop(1, self.dp_size)
            def _(shift):
                signal(lax.rem(self.dp + shift, self.dp_size), self.tensor)

            for shift in range(1, 4):
                signal(self.dp, lax.rem(self.tensor + shift, 4))
            pl.semaphore_wait(barrier, self.dp_size + 2)
        else:

            @pl.loop(1, self.outer_size)
            def _(shift):
                signal(self.ahead(shift), self.tensor)

            signal(self.other, self.tensor)
            signal(self.dp, self.across)
            signal(self.dp, self.twin)
            pl.semaphore_wait(barrier, self.outer_size + 2)


def pack_gains(packed, terms):
    part = 0
    for row, width in enumerate((terms.shape[1], terms.shape[1], 256)):
        for start in range(0, width, 128):
            packed[part // 3 : part // 3 + 1, 128 * (part % 3) : 128 * (part % 3) + 128] = terms[
                row : row + 1, start : start + 128
            ]
            part += 1


class Gather:
    def __init__(self, place, ref, micro, sems, index, source=None):
        own = ref.at[micro, tile(place.tensor)]
        source = own if source is None else source
        theirs = ref.at[micro, tile(place.across)]
        self.to_across = place.copy(source, own, sems, index, tensor=place.across)
        self.to_twin = place.copy(source, own, sems, index + 1, tensor=place.twin)
        self.on_to_twin = place.copy(theirs, theirs, sems, index + 2, tensor=place.twin)

    def start(self):
        self.to_across.start()
        self.to_twin.start()

    def relay(self):
        self.to_across.wait_recv()
        self.on_to_twin.start()

    def finish(self):
        self.to_twin.wait_recv()
        self.on_to_twin.wait_recv()

    def drain(self):
        self.to_across.wait_send()
        self.to_twin.wait_send()
        self.on_to_twin.wait_send()


class Scatter:
    def __init__(self, place, staged, from_twin, from_across, sems, index):
        self.place = place
        self.staged = staged
        self.from_twin = from_twin
        self.from_across = from_across
        self.sems = sems
        self.index = index

    def twin(self, half):
        return self.place.copy(
            self.staged.at[half],
            self.from_twin.at[half],
            self.sems,
            self.index + half,
            tensor=self.place.twin,
        )

    def crossing(self):
        return self.place.copy(
            self.staged.at[2],
            self.from_across,
            self.sems,
            self.index + 2,
            tensor=self.place.across,
        )

    def give(self, step, values):
        if step == 0 or step == 2:
            half = step // 2
            self.staged[half] = values.astype(BF16)
            self.twin(half).start()
        elif step == 1:
            self.staged[2] = values.astype(BF16)

    def cross(self):
        self.twin(0).wait_recv()
        self.staged[2] = (self.staged[2].astype(F32) + self.from_twin[0].astype(F32)).astype(BF16)
        self.crossing().start()

    def result(self, values):
        self.twin(1).wait_recv()
        self.crossing().wait_recv()
        return values + self.from_twin[1].astype(F32) + self.from_across[...].astype(F32)

    def drain(self):
        self.twin(0).wait_send()
        self.twin(1).wait_send()
        self.crossing().wait_send()


def fill_mixer(mixer):
    row = lax.broadcasted_iota(jnp.int32, mixer.shape, 0) // DH
    column = lax.broadcasted_iota(jnp.int32, mixer.shape, 1) // DH
    mixer[...] = jnp.where(row == column, 1.0 / DH, 0.0).astype(BF16)


class Weights:
    def __init__(self, place, shard, full, outer_sems, inner_sems, piece):
        self.place = place
        self.shard = shard
        self.full = full
        self.outer_sems = outer_sems
        self.inner_sems = inner_sems
        self.piece = piece
        self.rows = shard.shape[0]

    def at(self, index):
        return self.full.at[pl.ds(pl.multiple_of(index * self.rows, self.rows), self.rows), :]

    def hop(self, way, distance, own=False):
        place = self.place
        step = 1 - 2 * way
        rows = self.at((place.outer - step * (distance - 1)) * 2 + place.inner)
        return place.copy(
            self.shard if own else rows,
            rows,
            self.outer_sems,
            (self.piece, way, distance),
            dp=(place.outer + step) * 2 + place.inner,
        )

    def inner_copy(self, source, own=False):
        place = self.place
        rows = self.at(source * 2 + place.inner)
        return place.copy(
            self.shard if own else rows,
            rows,
            self.inner_sems,
            (self.piece, source),
            dp=place.other,
        )

    def arrival(self, way, distance):
        place = self.place
        rows = self.at(place.dp)
        return place.copy(
            rows, rows, self.outer_sems, (self.piece, way, distance), dp=place.other
        )

    def goes(self, way):
        place = self.place
        return place.outer > 0 if way else place.outer + 1 < place.outer_size

    def begin(self):
        for way in range(2):

            @pl.when(self.goes(way))
            def _():
                self.hop(way, 1, own=True).start()

        self.inner_copy(self.place.outer, own=True).start()

    def relay(self, first, last):
        place = self.place

        @pl.loop(first, last)
        def _(distance):
            for way in range(2):
                source = place.outer + distance if way else place.outer - distance

                @pl.when((source >= 0) & (source < place.outer_size))
                def _():
                    self.arrival(way, distance).wait_recv()

                    @pl.when(self.goes(way))
                    def _():
                        self.hop(way, distance + 1).start()

                    self.inner_copy(source).start()

    def finish(self):
        @pl.loop(0, self.place.outer_size)
        def _(source):
            self.inner_copy(source).wait_recv()

    def drain(self):
        place = self.place

        @pl.loop(0, place.outer_size)
        def _(source):
            self.inner_copy(source).wait_send()
            for way in range(2):
                distance = source - place.outer + 1 if way else place.outer - source + 1

                @pl.when(self.goes(way) & (distance >= 1))
                def _():
                    self.hop(way, distance).wait_send()


def rotation_angles(length):
    frequency = ROPE_BASE ** (-2.0 * (np.arange(128) % (DH // 2)) / DH)
    steps = np.arange(8) * TILE if length <= 8 * TILE else np.arange(0, length, TILE)
    positions = np.concatenate([np.arange(TILE), steps])
    turns = positions[:, None] * frequency[None, :]
    return jnp.asarray(np.stack([np.cos(turns), np.sin(turns)]).astype(np.float32))


def forward_kernel(
    dp_size,
    turned,
    tokens,
    cotangent,
    segments,
    w_query,
    w_key,
    w_value,
    w_out,
    gate_shard,
    up_shard,
    w_down,
    attn_gain,
    ffn_gain,
    query_gain,
    key_gain,
    angles,
    out_qkv_full,
    out_back_full,
    out_gate_full,
    out_up_full,
    out_down_full,
    out_normed,
    out_ffn,
    out_cot,
    out_gate_slope,
    out_up_slope,
    out_hidden,
    out_grad_down,
    out_query,
    out_key,
    out_value,
    out_attended,
    out_proj,
    out_middle,
    out_tables,
    qkv_shard,
    back_shard,
    down_shard,
    tables,
    query_marks,
    key_marks,
    mixer,
    normed,
    ffn_all,
    cot_all,
    qkv_full,
    back_full,
    gate_full,
    up_full,
    slopes,
    hidden,
    grad_down,
    query,
    key,
    value,
    attended,
    proj,
    middle,
    staged,
    from_twin,
    from_across,
    outer_send,
    outer_recv,
    inner_send,
    inner_recv,
    group_send,
    group_recv,
    local_sems,
    slope_sems,
):
    place = Place(dp_size)
    micro_count = tokens.shape[0]
    block_count = normed.shape[1] // TILE
    outer_size = place.outer_size
    group_sems = (group_send, group_recv)
    outer_sems = (outer_send, outer_recv)
    inner_sems = (inner_send, inner_recv)
    own = tile(place.tensor)
    first_cut = 1 + (outer_size - 1) // 3
    second_cut = 1 + 2 * (outer_size - 1) // 3
    qkv_w = Weights(place, qkv_shard, qkv_full, outer_sems, inner_sems, 0)
    back_w = Weights(place, back_shard, back_full, outer_sems, inner_sems, 1)
    gate_w = Weights(place, gate_shard, gate_full, outer_sems, inner_sems, 2)
    up_w = Weights(place, up_shard, up_full, outer_sems, inner_sems, 3)
    down_w = Weights(place, down_shard, out_down_full, outer_sems, inner_sems, 4)
    normed_g = [Gather(place, normed, m, group_sems, 3 * m) for m in range(micro_count)]
    cot_g = [
        Gather(place, cot_all, m, group_sems, 6 + 3 * m, cotangent.at[m])
        for m in range(micro_count)
    ]
    ffn_g = [Gather(place, ffn_all, m, group_sems, 12 + 3 * m) for m in range(micro_count)]

    def branch_s(m):
        return Scatter(
            place, staged.at[m], from_twin.at[m], from_across.at[m], group_sems, 18 + 3 * m
        )

    saves = []

    def save(src, dst):
        copy = pltpu.make_async_copy(src, dst, local_sems.at[len(saves)])
        copy.start()
        saves.append(copy)
        return copy

    def save_columns(src, dst, m):
        for block in range(dst.shape[0]):
            save(src.at[m, :, TILE * block : TILE * block + TILE], dst.at[block, m])

    lane = lax.broadcasted_iota(jnp.int32, (TILE, 128), 1)
    front = lane < 64
    place_in = rem(lane, 64)

    value_end = w_query.shape[1] + w_key.shape[1]
    qkv_shard[:, : w_query.shape[1]] = w_query[...]
    qkv_shard[:, w_query.shape[1] : value_end] = w_key[...]
    qkv_shard[:, value_end:] = w_value[...]
    for m in range(micro_count):
        normed[m, own] = norm_rows(tokens[m].astype(F32), attn_gain[...]).astype(BF16)
    if turned:
        back_shard[...] = w_out[...]
        down_shard[...] = w_down[...]
    else:
        back_shard[...] = w_out[...].T
        down_shard[...] = w_down[...].T
    place.greet(False)
    cuts = (1, first_cut, second_cut, outer_size)
    order = (qkv_w, back_w, gate_w, up_w, down_w)

    def take(item):
        part = item % 3
        order[item // 3].relay(cuts[part], cuts[part + 1])

    qkv_w.begin()
    normed_g[0].start()

    def prepare():
        fill_mixer(mixer)
        sign = jnp.where(place_in < 32, -1.0, 1.0)
        for kind, (gain_ref, scale) in enumerate(((query_gain, DH**-0.5 / LN2), (key_gain, 1.0))):
            gain = jnp.broadcast_to(
                jnp.concatenate([gain_ref[...], gain_ref[...]], axis=1) * scale, (TILE, 128)
            )
            crossed = swap_halves(gain) * sign
            for block in range(block_count):
                rows = slice(block * TILE, (block + 1) * TILE)
                cos_step = angles[0, TILE + block : TILE + block + 1]
                sin_step = angles[1, TILE + block : TILE + block + 1]
                cosine = angles[0, 0:TILE] * cos_step - angles[1, 0:TILE] * sin_step
                sine = angles[1, 0:TILE] * cos_step + angles[0, 0:TILE] * sin_step
                tables[2 * kind, rows] = cosine * gain
                tables[2 * kind + 1, rows] = sine * crossed
        row = lax.broadcasted_iota(jnp.int32, (16, 128), 0)
        mark_lane = lax.broadcasted_iota(jnp.int32, (16, 128), 1)
        spread = jnp.where(mark_lane == row + 8, 1.0, 0.0).astype(BF16)
        used = (lane >= 8) & (lane < 11)
        for m in range(micro_count):
            for block in range(block_count):
                rows = slice(block * TILE, (block + 1) * TILE)
                ids = jnp.broadcast_to(segments[m, :, rows], (16, TILE))
                match = lax.broadcasted_iota(jnp.int32, (16, TILE), 0) == ids
                marks = tn(jnp.where(match, 1.0, 0.0).astype(BF16), spread)
                query_marks[m, rows] = marks.astype(BF16)
                apart = jnp.where(used, APART * (1.0 - marks), 0.0)
                for head in range(2):
                    chosen = (lane >= 64 * head) & (lane < 64 * head + 3)
                    key_marks[head, m, rows] = jnp.where(chosen, 1.0, apart).astype(BF16)
        qkv_w.at(place.dp)[...] = qkv_shard[...]
        back_w.at(place.dp)[...] = back_shard[...]
        gate_w.at(place.dp)[...] = gate_shard[...]
        up_w.at(place.dp)[...] = up_shard[...]
        for m in range(micro_count):
            cot_all[m, own] = cotangent[m]

    prepare()
    save(down_shard, down_w.at(place.dp))
    save(tables, out_tables)
    take(0)
    back_w.begin()
    take(1)
    normed_g[1].start()
    take(2)
    take(3)
    gate_w.begin()

    later = lax.broadcasted_iota(jnp.int32, (TILE, TILE), 1) > lax.broadcasted_iota(
        jnp.int32, (TILE, TILE), 0
    )
    causal = jnp.where(later, APART, 0.0)

    def project(m):
        @pl.loop(0, block_count)
        def _(block):
            rows = tile(block)
            product = nn(normed[m, rows], qkv_full[...])
            proj[m, rows] = product[:, :384]
            heads = product[:, :256]
            inverse = lax.rsqrt(head_mean(heads * heads, mixer[...]) + NORM_EPS)
            for group in range(2):
                lanes = slice(128 * group, 128 * group + 128)
                part = heads[:, lanes]
                turned = part * tables[0, rows] + swap_halves(part) * tables[1, rows]
                query[m, group, rows, 0:128] = (turned * inverse[:, lanes]).astype(BF16)
                query[m, group, rows, 128:256] = query_marks[m, rows]
            part = product[:, 256:384]
            inverse = lax.rsqrt(head_mean(part * part, mixer[0:128, 0:128]) + NORM_EPS)
            turned = (part * tables[2, rows] + swap_halves(part) * tables[3, rows]) * inverse
            moved = pltpu.roll(turned, 64, 1)
            val = product[:, 384:512]
            val_moved = pltpu.roll(val, 64, 1)
            for group in range(2):
                first, second = (turned, moved) if group == 0 else (moved, turned)
                key[m, group, 0, rows, 0:128] = jnp.where(front, first, 0.0).astype(BF16)
                key[m, group, 1, rows, 0:128] = jnp.where(front, 0.0, second).astype(BF16)
                first, second = (val, val_moved) if group == 0 else (val_moved, val)
                value[m, group, 0, rows, 0:128] = jnp.where(front, first, 0.0).astype(BF16)
                value[m, group, 1, rows, 0:128] = jnp.where(front, 0.0, second).astype(BF16)
                for head in range(2):
                    key[m, group, head, rows, 128:256] = key_marks[head, m, rows]
                value[m, group, 0, rows, 128:256] = jnp.where(front, 1.0, 0.0).astype(BF16)
                value[m, group, 1, rows, 128:256] = jnp.where(front, 0.0, 1.0).astype(BF16)

    def attend(m):
        @pl.loop(0, 2)
        def _(group):
            for block in range(block_count):
                rows = slice(block * TILE, (block + 1) * TILE)
                query_block = query[m, group, rows]
                total = jnp.zeros((TILE, 256), F32)
                for head in range(2):
                    if block > 0:
                        before = slice(0, block * TILE)
                        scores = nt(query_block, key[m, group, head, before])
                        weights = jnp.exp2(scores).astype(BF16)
                        total = total + nn(weights, value[m, group, head, before])
                    scores = nt(query_block, key[m, group, head, rows]) + causal
                    weights = jnp.exp2(scores).astype(BF16)
                    total = total + nn(weights, value[m, group, head, rows])
                sums = total[:, 128:256]
                attended[m, group, rows] = (total[:, 0:128] / sums).astype(BF16)
                shift = -jnp.log2(sums)
                high = shift.astype(BF16)
                middle_part = (shift - high.astype(F32)).astype(BF16)
                last = (shift - high.astype(F32) - middle_part.astype(F32)).astype(BF16)
                marks = jnp.where(
                    place_in == 0,
                    high.astype(F32),
                    jnp.where(
                        place_in == 1,
                        middle_part.astype(F32),
                        jnp.where(
                            place_in == 2,
                            last.astype(F32),
                            query_block[:, 128:256].astype(F32),
                        ),
                    ),
                )
                query[m, group, rows, 128:256] = marks.astype(BF16)

    def branch_block(m, step):
        rows = tile(place.block(step))
        heads = jnp.concatenate([attended[m, 0, rows], attended[m, 1, rows]], axis=1)
        return nt(heads, back_full[...])

    def branch(m):
        for step in range(3):
            branch_s(m).give(step, branch_block(m, step))

    def enter_ffn(m):
        total = branch_s(m).result(branch_block(m, 3))
        middle[m] = tokens[m].astype(F32) + total
        save(middle.at[m], out_middle.at[m])
        ffn_all[m, own] = norm_rows(middle[m], ffn_gain[...]).astype(BF16)
        ffn_g[m].start()

    @pl.loop(0, micro_count)
    def _(m):
        @pl.when(m == 0)
        def _():
            normed_g[0].relay()
            take(4)
            normed_g[0].finish()
            qkv_w.finish()

        @pl.when(m == 1)
        def _():
            normed_g[1].finish()

        project(m)

        @pl.when(m == 0)
        def _():
            take(5)
            cot_g[0].start()

        attend(m)

        @pl.when(m == 0)
        def _():
            normed_g[1].relay()
            back_w.finish()

        branch(m)

        @pl.when(m == 0)
        def _():
            take(6)

        branch_s(m).cross()

        @pl.when(m == 0)
        def _():
            take(7)

        @pl.when(m == 1)
        def _():
            take(8)
            up_w.begin()

    save(qkv_full, out_qkv_full)
    save(back_full, out_back_full)
    for m in range(micro_count):
        save(query.at[m], out_query.at[m])
        save(key.at[m], out_key.at[m])
        save(value.at[m], out_value.at[m])
        save(attended.at[m], out_attended.at[m])
        save(proj.at[m], out_proj.at[m])
        save_columns(normed, out_normed, m)
    cot_g[0].relay()
    enter_ffn(0)
    take(9)
    enter_ffn(1)
    take(10)
    gate_w.finish()
    save(gate_full, out_gate_full)
    take(11)
    down_w.begin()
    cot_g[0].finish()
    save(cot_all.at[0], out_cot.at[0])
    ffn_g[0].relay()
    cot_g[1].start()
    ffn_g[0].finish()
    save_columns(ffn_all, out_ffn, 0)
    tile_count = micro_count * block_count

    @pl.loop(0, tile_count)
    def _(index):
        m = index // block_count
        rows = tile(rem(index, block_count))

        @pl.when(index == block_count)
        def _():
            take(12)
            ffn_g[1].relay()
            ffn_g[1].finish()

        hidden[m, rows] = nn(ffn_all[m, rows], gate_full[...]).astype(BF16)

    take(13)
    save_columns(ffn_all, out_ffn, 1)
    up_w.finish()
    save(up_full, out_up_full)

    def slope_copies(index):
        m = index // block_count
        rows = tile(rem(index, block_count))
        slot = rem(index, 2)
        return [
            pltpu.make_async_copy(
                slopes.at[slot, kind], out.at[m, rows], slope_sems.at[slot, kind]
            )
            for kind, out in enumerate((out_gate_slope, out_up_slope))
        ]

    @pl.loop(0, tile_count)
    def _(index):
        m = index // block_count
        rows = tile(rem(index, block_count))
        slot = rem(index, 2)

        @pl.when(index >= 2)
        def _():
            for copy in slope_copies(index - 2):
                copy.wait()

        gate = hidden[m, rows].astype(F32)
        up = nn(ffn_all[m, rows], up_full[...])
        sig = 1.0 / (1.0 + jnp.exp(-gate))
        act = gate * sig
        hidden[m, rows] = (act * up).astype(BF16)
        slopes[slot, 0] = (up * (sig + act * (1.0 - sig))).astype(BF16)
        slopes[slot, 1] = act.astype(BF16)
        for copy in slope_copies(index):
            copy.start()

    save(hidden, out_hidden)
    for index in (tile_count - 2, tile_count - 1):
        for copy in slope_copies(index):
            copy.wait()
    take(14)

    @pl.loop(0, block_count)
    def _(block):
        columns = tile(block)
        grad_down[columns] = tn(cot_all[0, :, columns], hidden[0]).astype(BF16)

    cot_g[1].relay()
    cot_g[1].finish()
    save(cot_all.at[1], out_cot.at[1])

    @pl.loop(0, block_count)
    def _(block):
        columns = tile(block)
        grad_down[columns] = (
            grad_down[columns].astype(F32) + tn(cot_all[1, :, columns], hidden[1])
        ).astype(BF16)

    save(grad_down, out_grad_down)
    down_w.finish()
    for piece in (qkv_w, back_w, gate_w, up_w, down_w):
        piece.drain()
    for m in range(micro_count):
        normed_g[m].drain()
        cot_g[m].drain()
        ffn_g[m].drain()
        branch_s(m).drain()
    for copy in saves:
        copy.wait()


def forward(dp_size, tokens, cotangent, segments, weights, gains):
    w_query, w_key, w_value, w_out, w_gate, w_up, w_down = weights
    micro, rows, width = tokens.shape
    length = segments.shape[2]
    share, hidden_width = w_gate.shape
    qkv_width = w_query.shape[1] + w_key.shape[1] + w_value.shape[1]
    back_width = w_out.shape[0]
    turned = share % 128 != 0
    if turned:
        w_out, w_down = w_out.T, w_down.T
    outer_size = dp_size // 2
    whole = pl.BlockSpec(memory_space=pltpu.VMEM)
    anywhere = pl.BlockSpec(memory_space=pl.ANY)
    shape = jax.ShapeDtypeStruct
    out_shape = [
        shape((width, qkv_width), BF16),
        shape((width, back_width), BF16),
        shape((width, hidden_width), BF16),
        shape((width, hidden_width), BF16),
        shape((width, hidden_width), BF16),
        shape((width // TILE, micro, length, TILE), BF16),
        shape((width // TILE, micro, length, TILE), BF16),
        shape((micro, length, width), BF16),
        shape((micro, length, hidden_width), BF16),
        shape((micro, length, hidden_width), BF16),
        shape((micro, length, hidden_width), BF16),
        shape((width, hidden_width), BF16),
        shape((micro, 2, length, 256), BF16),
        shape((micro, 2, 2, length, 256), BF16),
        shape((micro, 2, 2, length, 256), BF16),
        shape((micro, 2, length, 128), BF16),
        shape((micro, length, 384), F32),
        shape((micro, rows, width), F32),
        shape((4, length, 128), F32),
    ]
    scratch = [
        pltpu.VMEM((share, qkv_width), BF16),
        pltpu.VMEM((share, back_width), BF16),
        pltpu.VMEM((share, hidden_width), BF16),
        pltpu.VMEM((4, length, 128), F32),
        pltpu.VMEM((micro, length, 128), BF16),
        pltpu.VMEM((2, micro, length, 128), BF16),
        pltpu.VMEM((256, 256), BF16),
        pltpu.VMEM((micro, length, width), BF16),
        pltpu.VMEM((micro, length, width), BF16),
        pltpu.VMEM((micro, length, width), BF16),
        pltpu.VMEM((width, qkv_width), BF16),
        pltpu.VMEM((width, back_width), BF16),
        pltpu.VMEM((width, hidden_width), BF16),
        pltpu.VMEM((width, hidden_width), BF16),
        pltpu.VMEM((2, 2, TILE, hidden_width), BF16),
        pltpu.VMEM((micro, length, hidden_width), BF16),
        pltpu.VMEM((width, hidden_width), BF16),
        pltpu.VMEM((micro, 2, length, 256), BF16),
        pltpu.VMEM((micro, 2, 2, length, 256), BF16),
        pltpu.VMEM((micro, 2, 2, length, 256), BF16),
        pltpu.VMEM((micro, 2, length, 128), BF16),
        pltpu.VMEM((micro, length, 384), F32),
        pltpu.VMEM((micro, rows, width), F32),
        pltpu.VMEM((micro, 3, rows, width), BF16),
        pltpu.VMEM((micro, 2, rows, width), BF16),
        pltpu.VMEM((micro, rows, width), BF16),
        pltpu.SemaphoreType.DMA((5, 2, outer_size)),
        pltpu.SemaphoreType.DMA((5, 2, outer_size)),
        pltpu.SemaphoreType.DMA((5, outer_size)),
        pltpu.SemaphoreType.DMA((5, outer_size)),
        pltpu.SemaphoreType.DMA((24,)),
        pltpu.SemaphoreType.DMA((24,)),
        pltpu.SemaphoreType.DMA((48,)),
        pltpu.SemaphoreType.DMA((2, 2)),
    ]
    operands = (
        tokens,
        cotangent,
        segments,
        w_query,
        w_key,
        w_value,
        w_out,
        w_gate,
        w_up,
        w_down,
        *gains,
        rotation_angles(length),
    )
    return pl.pallas_call(
        functools.partial(forward_kernel, dp_size, turned),
        out_shape=out_shape,
        in_specs=[whole] * len(operands),
        out_specs=[anywhere] * len(out_shape),
        scratch_shapes=scratch,
        compiler_params=pltpu.CompilerParams(
            collective_id=0, has_side_effects=True, vmem_limit_bytes=VMEM_LIMIT
        ),
        name="forward_pass",
    )(*operands)


class Shares:
    def __init__(self, place, partial, kept, from_inner, from_outer, outer_sems, inner_sems, piece):
        self.place = place
        self.partial = partial
        self.kept = kept
        self.from_inner = from_inner
        self.from_outer = from_outer
        self.outer_sems = outer_sems
        self.inner_sems = inner_sems
        self.piece = piece
        self.rows = from_inner.shape[1]

    def at(self, index):
        return self.partial.at[pl.ds(pl.multiple_of(index * self.rows, self.rows), self.rows), :]

    def mine(self, shift):
        if self.kept is not None:
            return self.kept.at[shift]
        return self.at(self.place.ahead(shift))

    def inner_copy(self, shift):
        place = self.place
        return place.copy(
            self.at(place.ahead(shift, 1 - place.inner)),
            self.from_inner.at[shift],
            self.inner_sems,
            (self.piece, shift),
            dp=place.other,
        )

    def outer_copy(self, shift):
        place = self.place
        return place.copy(
            self.mine(shift),
            self.from_outer.at[shift - 1],
            self.outer_sems,
            (self.piece, shift),
            dp=place.ahead(shift),
        )

    def give(self, first, last):
        @pl.loop(first, last)
        def _(shift):
            self.inner_copy(shift).start()

    def turn(self, first, last):
        @pl.loop(first, last)
        def _(shift):
            self.inner_copy(shift).wait_recv()
            mine = self.mine(shift)
            mine[...] = (mine[...].astype(F32) + self.from_inner[shift].astype(F32)).astype(BF16)
            self.outer_copy(shift).start()

    def keep(self, total):
        self.inner_copy(0).wait_recv()
        total[...] = self.mine(0)[...].astype(F32) + self.from_inner[0].astype(F32)

    def finish(self, total):
        @pl.loop(1, self.place.outer_size)
        def _(shift):
            self.outer_copy(shift).wait_recv()
            total[...] += self.from_outer[shift - 1].astype(F32)

    def drain(self):
        self.inner_copy(0).wait_send()

        @pl.loop(1, self.place.outer_size)
        def _(shift):
            self.inner_copy(shift).wait_send()
            self.outer_copy(shift).wait_send()


def backward_kernel(
    dp_size,
    cotangent,
    attn_gain,
    ffn_gain,
    tokens,
    qkv_full,
    back_full,
    gate_full,
    up_full,
    down_full,
    normed,
    ffn_all,
    cot_all,
    gate_slope,
    up_slope,
    hidden,
    grad_down,
    query,
    key,
    value,
    attended,
    proj,
    middle_in,
    tables,
    out_mixed,
    out_tokens,
    gain_sums,
    out_qkv,
    out_back,
    out_gate,
    out_up,
    out_down,
    mixed,
    mid_all,
    mixer,
    ffn_w,
    down_w,
    qkv_w,
    att,
    qry,
    ky,
    val,
    prj,
    down_kept,
    qkv_inner,
    back_inner,
    ffn_inner,
    down_inner,
    qkv_outer,
    back_outer,
    ffn_outer,
    down_outer,
    staged,
    part_twin,
    part_across,
    out_twin,
    out_across,
    middle,
    gain_parts,
    gain_packed,
    gain_group,
    gain_dp,
    outer_send,
    outer_recv,
    inner_send,
    inner_recv,
    group_send,
    group_recv,
    gain_send,
    gain_recv,
    local_sems,
    tile_sems,
):
    place = Place(dp_size)
    micro_count = mixed.shape[0]
    length = mid_all.shape[1]
    width = mid_all.shape[2]
    hidden_width = down_w.shape[1]
    block_count = length // TILE
    tile_count = micro_count * block_count
    outer_size = place.outer_size
    group_sems = (group_send, group_recv)
    outer_sems = (outer_send, outer_recv)
    inner_sems = (inner_send, inner_recv)
    own = tile(place.tensor)
    first_cut = 1 + (outer_size - 1) // 3
    second_cut = 1 + 2 * (outer_size - 1) // 3
    outers = outer_size // 4
    own_outer_block = place.outer // outers
    counter = []

    def load(src, dst):
        copy = pltpu.make_async_copy(src, dst, local_sems.at[len(counter) + (8 if len(counter) >= 8 else 0)])
        counter.append(copy)
        copy.start()
        return copy

    down_s = Shares(place, grad_down, down_kept, down_inner, down_outer, outer_sems, inner_sems, 4)

    def ffn_shares(kind):
        return Shares(
            place,
            ffn_w.at[kind],
            None,
            ffn_inner.at[kind],
            ffn_outer.at[kind],
            outer_sems,
            inner_sems,
            2 + kind,
        )

    gate_s, up_s = ffn_shares(0), ffn_shares(1)
    mid_g = [Gather(place, mid_all, m, group_sems, 3 * m) for m in range(micro_count)]

    def turn_block(step):
        return rem(step + 1 + own_outer_block, 4)

    cuts = (1, first_cut, second_cut, outer_size)

    def issue(share, part):
        share.give(*((0, 1) if part == 3 else (cuts[part], cuts[part + 1])))

    def take(share, part):
        share.turn(cuts[part], cuts[part + 1])

    def twin_copy(kind, m, half):
        from_twin = (part_twin, out_twin, part_twin)[kind]
        return place.copy(
            staged.at[m, half],
            from_twin.at[m, half],
            group_sems,
            6 + 6 * kind + 3 * m + half,
            tensor=place.twin,
        )

    def across_copy(kind, m):
        from_across = (part_across, out_across, part_across)[kind]
        return place.copy(
            staged.at[m, 2],
            from_across.at[m],
            group_sems,
            6 + 6 * kind + 3 * m + 2,
            tensor=place.across,
        )

    def block_of(step):
        side = jnp.where(step < 2, 1 - place.side, place.side)
        core = jnp.where(rem(step, 2) == 0, 1 - place.core, place.core)
        return side * 2 + core

    def hand_out(m, step, values):
        staged[m, rem(step, 2) * 2 + step // 2] = values.astype(BF16)

    def send_twin(kind, m, step):
        @pl.when(rem(step, 2) == 0)
        def _():
            twin_copy(kind, m, step // 2).start()

    def cross(kind, m):
        from_twin = (part_twin, out_twin, part_twin)[kind]
        twin_copy(kind, m, 0).wait_recv()
        staged[m, 2] = (staged[m, 2].astype(F32) + from_twin[m, 0].astype(F32)).astype(BF16)
        across_copy(kind, m).start()

    def collect(kind, m):
        from_twin = (part_twin, out_twin, part_twin)[kind]
        from_across = (part_across, out_across, part_across)[kind]
        twin_copy(kind, m, 1).wait_recv()
        across_copy(kind, m).wait_recv()
        return staged[m, 3].astype(F32) + from_twin[m, 1].astype(F32) + from_across[m].astype(F32)

    def drain(kind, m):
        twin_copy(kind, m, 0).wait_send()
        twin_copy(kind, m, 1).wait_send()
        across_copy(kind, m).wait_send()

    def leave_ffn(m):
        upstream = collect(0, m)
        back, term = norm_rows_back(middle[m], ffn_gain[...], upstream)
        mid_all[m, own] = (mixed[m].astype(F32) + back).astype(BF16)
        mid_g[m].start()
        gain_parts[1:2, :] += term

    def leave_out(m):
        mixed[m] = (middle[m] + collect(1, m)).astype(BF16)

    def attn_copies():
        pairs = (
            (back_full, qkv_w.at[:, 512:768]),
            (attended, att),
            (value.at[0], val),
            (key.at[0], ky),
            (query.at[0], qry),
            (proj.at[0], prj),
            (qkv_full, qkv_w.at[:, 0:512]),
        )
        return [
            pltpu.make_async_copy(src, dst, local_sems.at[30 + index])
            for index, (src, dst) in enumerate(pairs)
        ]

    def rows_of(index):
        return index // block_count, tile(block_of(rem(index, block_count)))

    def ffn_phase(grads, rows_buf, ffn_cols):
        def rows_copy(index):
            m, rows = rows_of(index)
            slot = rem(index, 2)
            return pltpu.make_async_copy(cot_all.at[m, rows], rows_buf.at[slot], tile_sems.at[0, slot])

        def cols_copy(index):
            slot = rem(index, 2)
            return pltpu.make_async_copy(
                ffn_all.at[turn_block(rem(index, block_count))], ffn_cols.at[slot], tile_sems.at[2, slot]
            )

        loads = [load(down_full, down_w)]
        rows_copy(0).start()
        loads += [load(gate_slope.at[0], grads.at[0, 0]), load(up_slope.at[0], grads.at[1, 0])]
        loads += [load(gate_full, ffn_w.at[0]), load(up_full, ffn_w.at[1])]
        others = [
            load(gate_slope.at[1], grads.at[0, 1]),
            load(up_slope.at[1], grads.at[1, 1]),
            load(middle_in, middle),
            load(cotangent, mixed),
        ]

        def kept_copy(shift):
            return pltpu.make_async_copy(
                down_s.at(place.ahead(shift)), down_kept.at[shift], local_sems.at[40 + shift]
            )

        @pl.loop(0, outer_size)
        def _(shift):
            kept_copy(shift).start()

        fill_mixer(mixer)
        gain_parts[...] = jnp.zeros_like(gain_parts)
        gain_packed[...] = jnp.zeros_like(gain_packed)
        place.greet(True)
        issue(down_s, 0)
        issue(down_s, 1)
        for copy in loads:
            copy.wait()

        @pl.loop(0, tile_count)
        def _(index):
            m, rows = rows_of(index)
            step = rem(index, block_count)
            slot = rem(index, 2)

            @pl.when(index + 1 < tile_count)
            def _():
                rows_copy(index + 1).start()

            @pl.when(index == block_count)
            def _():
                pltpu.make_async_copy(gate_slope.at[1], grads.at[0, 1], local_sems.at[5]).wait()
                pltpu.make_async_copy(up_slope.at[1], grads.at[1, 1], local_sems.at[6]).wait()

            @pl.when(index == 2)
            def _():
                @pl.loop(0, outer_size)
                def _(shift):
                    kept_copy(shift).wait()

                take(down_s, 0)
                issue(down_s, 2)

            @pl.when(index == block_count + 1)
            def _():
                take(down_s, 1)
                issue(down_s, 3)

            rows_copy(index).wait()
            hidden_grad = nn(rows_buf[slot], down_w[...])
            gate_low = (hidden_grad * grads[0, m, rows].astype(F32)).astype(BF16)
            up_low = (hidden_grad * grads[1, m, rows].astype(F32)).astype(BF16)
            grads[0, m, rows] = gate_low
            grads[1, m, rows] = up_low
            hand_out(m, step, nt(gate_low, ffn_w[0]) + nt(up_low, ffn_w[1]))

            send_twin(0, m, step)

            @pl.when(index == 2)
            def _():
                cross(0, 0)

        for copy in attn_copies():
            copy.start()
        cols_copy(0).start()
        for copy in others[2:]:
            copy.wait()
        leave_ffn(0)
        cross(0, 1)

        @pl.loop(0, 2 * block_count)
        def _(index):
            kind = index // block_count
            block = turn_block(rem(index, block_count))
            slot = rem(index, 2)
            cols_copy(index).wait()

            @pl.when(index + 1 < 2 * block_count)
            def _():
                cols_copy(index + 1).start()

            ffn_w[kind, tile(block)] = (
                tn(ffn_cols[slot, 0], grads[kind, 0]) + tn(ffn_cols[slot, 1], grads[kind, 1])
            ).astype(BF16)

            @pl.when(index == 1)
            def _():
                take(down_s, 2)
                if outers == 1:
                    issue(gate_s, 0)

            @pl.when(index == block_count - 1)
            def _():
                if outers > 1:
                    issue(gate_s, 0)
                issue(gate_s, 1)

            @pl.when(index == block_count + 3)
            def _():
                take(gate_s, 0)
                issue(gate_s, 2)

    pl.run_scoped(
        ffn_phase,
        pltpu.VMEM((2, micro_count, length, hidden_width), BF16),
        pltpu.VMEM((2, TILE, width), BF16),
        pltpu.VMEM((2, micro_count, length, TILE), BF16),
    )

    def attn_phase(
        toks,
        tabs,
        hidden_buf,
        grad_att,
        grad_q,
        grad_k,
        grad_v,
        grad_qkv,
        qkv_total,
        back_total,
        gate_total,
        up_total,
        down_total,
    ):
        qkv_part = down_w.at[:, 0:512]
        back_part = down_w.at[:, 512:768]
        qkv_s = Shares(place, qkv_part, None, qkv_inner, qkv_outer, outer_sems, inner_sems, 0)
        back_s = Shares(place, back_part, None, back_inner, back_outer, outer_sems, inner_sems, 1)
        lane = lax.broadcasted_iota(jnp.int32, (TILE, 128), 1)
        front = lane < 64
        place_in = rem(lane, 64)
        later = lax.broadcasted_iota(jnp.int32, (TILE, TILE), 0) > lax.broadcasted_iota(
            jnp.int32, (TILE, TILE), 1
        )
        causal = jnp.where(later, APART, 0.0)
        small = mixer[0:128, 0:128]
        table_load = load(tables, tabs)
        token_load = load(tokens, toks)

        def score_ready(m):
            @pl.loop(0, block_count)
            def _(block):
                rows = tile(block)
                low = nn(mid_all[m, rows], qkv_w[:, 512:768]).astype(BF16)
                for group in range(2):
                    part = low[:, 128 * group : 128 * group + 128]
                    both = part.astype(F32) * att[m, group, rows].astype(F32)
                    shift = head_mean(both, small) * -64.0
                    high = shift.astype(BF16)
                    rest = shift - high.astype(F32)
                    mid = rest.astype(BF16)
                    last = (rest - mid.astype(F32)).astype(BF16)
                    marks = jnp.where(
                        place_in == 0,
                        high.astype(F32),
                        jnp.where(
                            place_in == 1,
                            mid.astype(F32),
                            jnp.where(place_in == 2, last.astype(F32), 0.0),
                        ),
                    )
                    grad_att[group, rows, 0:128] = part
                    grad_att[group, rows, 128:256] = marks.astype(BF16)

        def attend_back(m, between):
            @pl.loop(0, 2)
            def _(group):
                for block in range(block_count):
                    rows = slice(block * TILE, (block + 1) * TILE)
                    spans = [(rows, True)]
                    if block + 1 < block_count:
                        spans.append((slice((block + 1) * TILE, length), False))
                    sums_k = []
                    sums_v = []
                    for head in range(2):
                        key_block = ky[group, head, rows]
                        value_block = val[group, head, rows]
                        sum_k = None
                        sum_v = None
                        for span, masked in spans:
                            query_span = qry[group, span]
                            grad_span = grad_att[group, span]
                            scores = nt(key_block, query_span)
                            if masked:
                                scores = scores + causal
                            probs = jnp.exp2(scores)
                            score_grad = (probs * nt(value_block, grad_span)).astype(BF16)
                            probs_low = probs.astype(BF16)
                            part_v = nn(probs_low, grad_span[:, 0:128])
                            part_k = nn(score_grad, query_span[:, 0:128])
                            sum_v = part_v if sum_v is None else sum_v + part_v
                            sum_k = part_k if sum_k is None else sum_k + part_k
                            part_q = tn(score_grad, key_block[:, 0:128])
                            if block == 0 and head == 0:
                                grad_q[group, span] = part_q
                            else:
                                grad_q[group, span] += part_q
                        sums_k.append(sum_k)
                        sums_v.append(sum_v)
                    both_k = jnp.where(front, sums_k[0], sums_k[1])
                    both_v = jnp.where(front, sums_v[0], sums_v[1])
                    grad_k[group, rows] = both_k + pltpu.roll(both_k, 64, 1)
                    grad_v[group, rows] = both_v + pltpu.roll(both_v, 64, 1)

                between(group)

        def normalize_back(grads, values, cosine, sine):
            scaled = grads * LN2
            weighted = scaled * cosine + swap_halves(scaled * sine)
            inverse = lax.rsqrt(head_mean(values * values, small) + NORM_EPS)
            unit = values * inverse
            both = weighted * unit
            back = inverse * (weighted - unit * head_mean(both, small))
            return back.astype(BF16), jnp.sum(both, axis=0, keepdims=True)

        def leave_heads(m):
            @pl.loop(0, block_count)
            def _(block):
                rows = tile(block)
                cosine, sine = tabs[0, rows], tabs[1, rows]
                for group in range(2):
                    lanes = slice(128 * group, 128 * group + 128)
                    back, term = normalize_back(grad_q[group, rows], prj[rows, lanes], cosine, sine)
                    grad_qkv[m, rows, lanes] = back
                    gain_parts[2:3, 0:128] += term
                back, term = normalize_back(
                    jnp.where(front, grad_k[0, rows], grad_k[1, rows]),
                    prj[rows, 256:384],
                    tabs[2, rows],
                    tabs[3, rows],
                )
                grad_qkv[m, rows, 256:384] = back
                gain_parts[2:3, 128:256] += term
                grad_qkv[m, rows, 384:512] = jnp.where(
                    front, grad_v[0, rows], grad_v[1, rows]
                ).astype(BF16)

        def enter_norm(m):
            drain(1, m)

            @pl.loop(0, block_count)
            def _(step):
                rows = tile(block_of(step))
                hand_out(m, step, nt(grad_qkv[m, rows], qkv_w[:, 0:512]))
                send_twin(2, m, step)

            cross(2, m)

        def leave_attn(m):
            upstream = collect(2, m)
            back, term = norm_rows_back(toks[m].astype(F32), attn_gain[...], upstream)
            middle[m] = mid_all[m, own].astype(F32) + back
            gain_parts[0:1, :] += term

        def norm_copies():
            return [
                pltpu.make_async_copy(
                    normed.at[turn_block(step)], norm_cols.at[step % 2], local_sems.at[24 + step]
                )
                for step, norm_cols in enumerate((ky, ky, val, val))
            ]

        reloads = ((value, val), (key, ky), (query, qry), (proj, prj))

        def reload_copy(index):
            src, dst = reloads[index]
            return pltpu.make_async_copy(src.at[1], dst, local_sems.at[10 + index])

        def mixed_save(m):
            return pltpu.make_async_copy(mixed.at[m], out_mixed.at[m], local_sems.at[14 + m])

        def enter_back():
            @pl.loop(0, block_count)
            def _(step):
                block = turn_block(step)
                columns = tile(block)
                total = jnp.zeros((TILE, 256), F32)
                for m in range(micro_count):
                    heads = jnp.concatenate([att[m, 0], att[m, 1]], axis=1)
                    total = total + tn(mid_all[m, :, columns], heads)
                back_part[columns] = total.astype(BF16)

        def hidden_copy(index):
            m, rows = rows_of(index)
            slot = rem(index, block_count)
            return pltpu.make_async_copy(
                hidden.at[m, rows], hidden_buf.at[slot], local_sems.at[24 + slot]
            )

        def enter_out():
            drain(0, 0)

            @pl.loop(0, tile_count)
            def _(index):
                m = index // block_count
                step = rem(index, block_count)

                @pl.when(index == block_count)
                def _():
                    take(gate_s, 1)
                    issue(gate_s, 3)
                    leave_ffn(1)
                    drain(0, 1)

                hidden_copy(index).wait()
                hand_out(m, step, nt(hidden_buf[step], down_w[...]))
                send_twin(1, m, step)

                @pl.when(index + block_count < tile_count)
                def _():
                    hidden_copy(index + block_count).start()

        for slot in range(block_count):
            hidden_copy(slot).start()
        for copy in attn_copies():
            copy.wait()
        down_s.keep(down_total)
        mid_g[0].relay()
        enter_out()
        cross(1, 0)
        mid_g[0].finish()

        @pl.loop(0, micro_count)
        def _(m):
            score_ready(m)

            @pl.when(m == 1)
            def _():
                leave_out(0)
                mixed_save(0).start()
                enter_norm(0)
                take(up_s, 1)
                issue(up_s, 3)
                enter_back()

            def between(group):
                @pl.when((m == 0) & (group == 0))
                def _():
                    take(gate_s, 2)
                    issue(up_s, 0)

                @pl.when((m == 0) & (group == 1))
                def _():
                    gate_s.keep(gate_total)
                    issue(up_s, 1)
                    cross(1, 1)
                    mid_g[1].relay()

                @pl.when((m == 1) & (group == 0))
                def _():
                    take(up_s, 2)
                    issue(back_s, 0)
                    issue(back_s, 1)

                @pl.when((m == 1) & (group == 1))
                def _():
                    up_s.keep(up_total)
                    issue(back_s, 2)
                    issue(back_s, 3)

            attend_back(m, between)

            @pl.when(m == 0)
            def _():
                for index in range(3):
                    reload_copy(index).start()
                table_load.wait()

            @pl.when(m == 1)
            def _():
                for copy in norm_copies():
                    copy.start()

            leave_heads(m)

            @pl.when(m == 0)
            def _():
                reload_copy(3).start()
                take(up_s, 0)
                issue(up_s, 2)

            @pl.when(m == 0)
            def _():
                mid_g[1].finish()
                for index in range(4):
                    reload_copy(index).wait()

        for half, norm_cols in enumerate((ky, val)):

            @pl.loop(2 * half, 2 * half + 2)
            def _(step):
                slot = step - 2 * half
                pltpu.make_async_copy(
                    normed.at[turn_block(step)], norm_cols.at[slot], local_sems.at[24 + step]
                ).wait()
                qkv_part[tile(turn_block(step))] = (
                    tn(norm_cols[slot, 0], grad_qkv[0]) + tn(norm_cols[slot, 1], grad_qkv[1])
                ).astype(BF16)
                if outers == 1:
                    qkv_s.inner_copy(rem(step + 1, outer_size)).start()

        if outers > 1:
            for part in range(4):
                issue(qkv_s, part)
        leave_out(1)
        mixed_save(1).start()
        enter_norm(1)
        token_load.wait()
        saves = [mixed_save(m) for m in range(micro_count)]
        down_s.finish(down_total)
        saves.append(load(down_total, out_down))
        gate_s.finish(gate_total)
        saves.append(load(gate_total, out_gate))

        for part in range(3):
            take(back_s, part)
        leave_attn(0)
        saves.append(load(middle.at[0], out_tokens.at[0]))
        back_s.keep(back_total)
        for part in range(3):
            take(qkv_s, part)
        leave_attn(1)
        saves.append(load(middle.at[1], out_tokens.at[1]))

        def group_gain(shift):
            return place.copy(
                gain_packed,
                gain_group.at[shift - 1],
                (gain_send, gain_recv),
                shift - 1,
                tensor=rem(place.tensor + shift, 4),
            )

        pack_gains(gain_packed, gain_parts)
        for shift in range(1, 4):
            group_gain(shift).start()
        qkv_s.keep(qkv_total)
        up_s.finish(up_total)
        saves.append(load(up_total, out_up))
        back_s.finish(back_total)
        saves.append(load(back_total, out_back))
        for shift in range(1, 4):
            group_gain(shift).wait_recv()
        gain_dp[0] = gain_packed[...] + gain_group[0] + gain_group[1] + gain_group[2]

        def dp_gain(shift):
            return place.copy(
                gain_dp.at[0],
                gain_dp.at[shift],
                (gain_send, gain_recv),
                2 + shift,
                dp=rem(place.dp + shift, dp_size),
            )

        @pl.loop(1, dp_size)
        def _(shift):
            dp_gain(shift).start()

        qkv_s.finish(qkv_total)
        saves.append(load(qkv_total, out_qkv))
        gain_sums[...] = gain_dp[0]

        @pl.loop(1, dp_size)
        def _(shift):
            dp_gain(shift).wait_recv()
            gain_sums[...] += gain_dp[shift]

        for shift in range(1, 4):
            group_gain(shift).wait_send()

        @pl.loop(1, dp_size)
        def _(shift):
            dp_gain(shift).wait_send()

        qkv_s.drain()
        back_s.drain()
        for copy in saves:
            copy.wait()

    pl.run_scoped(
        attn_phase,
        pltpu.VMEM(tokens.shape, BF16),
        pltpu.VMEM(tables.shape, F32),
        pltpu.VMEM((block_count, TILE, hidden_width), BF16),
        pltpu.VMEM((2, length, 256), BF16),
        pltpu.VMEM((2, length, 128), F32),
        pltpu.VMEM((2, length, 128), F32),
        pltpu.VMEM((2, length, 128), F32),
        pltpu.VMEM((micro_count, length, 512), BF16),
        *[
            pltpu.VMEM((width // dp_size, w), F32)
            for w in (512, 256, hidden_width, hidden_width, hidden_width)
        ],
    )
    for share in (down_s, gate_s, up_s):
        share.drain()
    for m in range(micro_count):
        mid_g[m].drain()
        drain(2, m)


def backward(dp_size, cotangent, attn_gain, ffn_gain, tokens, saved):
    micro, rows, width = tokens.shape
    length = saved[7].shape[1]
    hidden_width = saved[2].shape[1]
    outer_size = dp_size // 2
    share = width // dp_size
    whole = pl.BlockSpec(memory_space=pltpu.VMEM)
    anywhere = pl.BlockSpec(memory_space=pl.ANY)
    shape = jax.ShapeDtypeStruct
    widths = (512, 256, hidden_width, hidden_width, hidden_width)
    out_shape = [
        shape((micro, rows, width), BF16),
        shape((micro, rows, width), F32),
        shape((8, 384), F32),
    ] + [shape((share, w), F32) for w in widths]
    scratch = (
        [pltpu.VMEM((micro, rows, width), BF16)]
        + [
            pltpu.VMEM((micro, length, width), BF16),
            pltpu.VMEM((256, 256), BF16),
            pltpu.VMEM((2, width, hidden_width), BF16),
            pltpu.VMEM((width, hidden_width), BF16),
            pltpu.VMEM((width, 768), BF16),
            pltpu.VMEM((micro, 2, length, 128), BF16),
            pltpu.VMEM((2, length, 256), BF16),
            pltpu.VMEM((2, 2, length, 256), BF16),
            pltpu.VMEM((2, 2, length, 256), BF16),
            pltpu.VMEM((length, 384), F32),
            pltpu.VMEM((outer_size, share, hidden_width), BF16),
            pltpu.VMEM((outer_size, share, 512), BF16),
            pltpu.VMEM((outer_size, share, 256), BF16),
            pltpu.VMEM((2, outer_size, share, hidden_width), BF16),
            pltpu.VMEM((outer_size, share, hidden_width), BF16),
            pltpu.VMEM((outer_size - 1, share, 512), BF16),
            pltpu.VMEM((outer_size - 1, share, 256), BF16),
            pltpu.VMEM((2, outer_size - 1, share, hidden_width), BF16),
            pltpu.VMEM((outer_size - 1, share, hidden_width), BF16),
            pltpu.VMEM((micro, 4, rows, width), BF16),
            pltpu.VMEM((micro, 2, rows, width), BF16),
            pltpu.VMEM((micro, rows, width), BF16),
            pltpu.VMEM((micro, 2, rows, width), BF16),
            pltpu.VMEM((micro, rows, width), BF16),
            pltpu.VMEM((micro, rows, width), F32),
            pltpu.VMEM((8, width), F32),
            pltpu.VMEM((8, 384), F32),
            pltpu.VMEM((3, 8, 384), F32),
            pltpu.VMEM((dp_size, 8, 384), F32),
        ]
        + [pltpu.SemaphoreType.DMA((5, outer_size))] * 4
        + [pltpu.SemaphoreType.DMA((24,))] * 2
        + [pltpu.SemaphoreType.DMA((dp_size + 2,))] * 2
        + [pltpu.SemaphoreType.DMA((40 + outer_size,)), pltpu.SemaphoreType.DMA((4, 2))]
    )
    return pl.pallas_call(
        functools.partial(backward_kernel, dp_size),
        out_shape=out_shape,
        in_specs=[anywhere, whole, whole] + [anywhere] * (1 + len(saved)),
        out_specs=[anywhere, anywhere, whole] + [anywhere] * 5,
        scratch_shapes=scratch,
        compiler_params=pltpu.CompilerParams(
            collective_id=1, has_side_effects=True, vmem_limit_bytes=VMEM_LIMIT
        ),
        name="backward_pass",
    )(cotangent, attn_gain, ffn_gain, tokens, *saved)


def deliver_kernel(
    turned,
    in_mixed,
    in_tokens,
    gains,
    query_gain,
    key_gain,
    in_qkv,
    in_back,
    in_gate,
    in_up,
    in_down,
    mixed,
    grad_tokens,
    attn_gain,
    ffn_gain,
    query_term,
    key_term,
    grad_query,
    grad_key,
    grad_value,
    grad_out,
    grad_gate,
    grad_up,
    grad_down,
    buf_mixed,
    buf_tokens,
    buf_gate,
    buf_up,
    buf_qkv,
    buf_back,
    buf_down,
    turned_out,
    turned_down,
    sems,
):
    flows = [
        (in_down, buf_down, ()),
        (in_back, buf_back, ()),
        (in_mixed, buf_mixed, ((buf_mixed, mixed),)),
        (in_tokens.at[0], buf_tokens.at[0], ((buf_tokens.at[0], grad_tokens.at[0]),)),
        (in_tokens.at[1], buf_tokens.at[1], ((buf_tokens.at[1], grad_tokens.at[1]),)),
        (in_gate, buf_gate, ((buf_gate, grad_gate),)),
        (in_up, buf_up, ((buf_up, grad_up),)),
        (
            in_qkv,
            buf_qkv,
            (
                (buf_qkv.at[:, 0:256], grad_query),
                (buf_qkv.at[:, 256:384], grad_key),
                (buf_qkv.at[:, 384:512], grad_value),
            ),
        ),
    ]
    arrivals = [
        pltpu.make_async_copy(src, buf, sems.at[0, index]) for index, (src, buf, _) in enumerate(flows)
    ]
    departures = []

    def depart(src, dst):
        copy = pltpu.make_async_copy(src, dst, sems.at[1, len(departures)])
        copy.start()
        departures.append(copy)

    for copy in arrivals:
        copy.start()
    part = 0
    for out in (attn_gain, ffn_gain):
        for start in range(0, out.shape[1], 128):
            out[:, start : start + 128] = gains[
                part // 3 : part // 3 + 1, 128 * (part % 3) : 128 * (part % 3) + 128
            ]
            part += 1
    for out, gain in ((query_term, query_gain), (key_term, key_gain)):
        term = gains[part // 3 : part // 3 + 1, 128 * (part % 3) : 128 * (part % 3) + 128]
        out[...] = term[:, :DH] / gain[...] + term[:, DH:] / gain[...]
        part += 1
    for index in range(2, len(flows)):
        arrivals[index].wait()
        for src, dst in flows[index][2]:
            depart(src, dst)
    for index, (buf, facing, dst) in enumerate(
        ((buf_down, turned_down, grad_down), (buf_back, turned_out, grad_out))
    ):
        arrivals[index].wait()
        if turned:
            depart(buf, dst)
        else:
            facing[...] = buf[...].T
            depart(facing, dst)
    for copy in departures:
        copy.wait()


def deliver(results, query_gain, key_gain):
    mixed, grad_tokens, gains, qkv, back, gate, up, down = results
    turned = qkv.shape[0] % 128 != 0
    whole = pl.BlockSpec(memory_space=pltpu.VMEM)
    anywhere = pl.BlockSpec(memory_space=pl.ANY)
    stored = pl.BlockSpec(memory_space=pltpu.HBM)
    shape = jax.ShapeDtypeStruct
    share, width = qkv.shape[0], mixed.shape[2]

    def facing(array):
        return array.shape if turned else array.shape[::-1]

    out_shape = [
        shape(mixed.shape, BF16),
        shape(grad_tokens.shape, F32),
        shape((1, width), F32),
        shape((1, width), F32),
        shape((1, DH), F32),
        shape((1, DH), F32),
        shape((share, 256), F32),
        shape((share, 128), F32),
        shape((share, 128), F32),
        shape(facing(back), F32),
        shape(gate.shape, F32),
        shape(up.shape, F32),
        shape(facing(down), F32),
    ]
    out = pl.pallas_call(
        functools.partial(deliver_kernel, turned),
        out_shape=out_shape,
        in_specs=[stored, stored] + [whole] * 3 + [stored] * 5,
        out_specs=[anywhere] * 2 + [whole] * 4 + [anywhere] * 7,
        scratch_shapes=[
            pltpu.VMEM(mixed.shape, BF16),
            pltpu.VMEM(grad_tokens.shape, F32),
            pltpu.VMEM(gate.shape, F32),
            pltpu.VMEM(up.shape, F32),
            pltpu.VMEM(qkv.shape, F32),
            pltpu.VMEM(back.shape, F32),
            pltpu.VMEM(down.shape, F32),
            pltpu.VMEM(facing(back), F32),
            pltpu.VMEM(facing(down), F32),
            pltpu.SemaphoreType.DMA((2, 16)),
        ],
        compiler_params=pltpu.CompilerParams(vmem_limit_bytes=VMEM_LIMIT),
        name="deliver_pass",
    )(mixed, grad_tokens, gains, query_gain, key_gain, qkv, back, gate, up, down)
    out = list(out)
    if turned:
        out[9], out[12] = out[9].T, out[12].T
    return out


def shards(
    dp_size,
    tokens,
    segment_ids,
    attn_gain,
    query_gain,
    key_gain,
    w_query,
    w_key,
    w_value,
    w_out,
    ffn_gain,
    w_gate,
    w_up,
    w_down,
    cotangent,
):
    own_tokens, own_cot = tokens[:, 0], cotangent[:, 0]
    attn_row, ffn_row = attn_gain[None], ffn_gain[None]
    saved = forward(
        dp_size,
        own_tokens,
        own_cot,
        segment_ids,
        (w_query, w_key, w_value, w_out, w_gate, w_up, w_down),
        (attn_row, ffn_row, query_gain[None], key_gain[None]),
    )
    results = backward(dp_size, own_cot, attn_row, ffn_row, own_tokens, saved)
    (
        mixed,
        grad_tokens,
        attn_term,
        ffn_term,
        query_term,
        key_term,
        grad_query,
        grad_key,
        grad_value,
        grad_out,
        grad_gate,
        grad_up,
        grad_down,
    ) = deliver(results, query_gain[None], key_gain[None])
    return (
        mixed[:, None],
        grad_tokens[:, None],
        attn_term[0],
        query_term[0],
        key_term[0],
        grad_query,
        grad_key,
        grad_value,
        grad_out,
        ffn_term[0],
        grad_gate,
        grad_up,
        grad_down,
    )


def solution(mesh):
    sequence = P(None, "dp", "tensor", None)
    rows = P("dp", "tensor")
    columns = P("tensor", "dp")
    return jax.shard_map(
        functools.partial(shards, mesh.shape["dp"]),
        mesh=mesh,
        in_specs=(sequence, P(None, "dp", None), P(), P(), P(), rows, rows, rows, columns, P(), rows, rows, columns, sequence),
        out_specs=(sequence, sequence, P(), P(), P(), rows, rows, rows, columns, P(), rows, rows, columns),
        check_vma=False,
    )
```

```python
import functools
import math

import jax
import jax.numpy as jnp
import numpy as np
from jax import lax
from jax.experimental import pallas as pl
from jax.experimental.pallas import tpu as pltpu
from jax.sharding import PartitionSpec as P

MESH = pl.DeviceIdType.MESH
VMEM_LIMIT = 67000000
NORM_EPS = 1e-05
ROPE_BASE = 1000000.0
DH = 64
TILE = 256
LN2 = math.log(2.0)
APART = -32768.0
BF16 = jnp.bfloat16
F32 = jnp.float32


def nn(left, right):
    return lax.dot_general(left, right, (((1,), (0,)), ((), ())), preferred_element_type=F32)


def nt(left, right):
    return lax.dot_general(left, right, (((1,), (1,)), ((), ())), preferred_element_type=F32)


def tn(left, right):
    return lax.dot_general(left, right, (((0,), (0,)), ((), ())), preferred_element_type=F32)


def tile(index, size=TILE):
    return pl.ds(pl.multiple_of(index * size, size), size)


def rem(value, divisor):
    return value % divisor if isinstance(value, int) else lax.rem(value, divisor)


def low_parts(values):
    high = values.astype(BF16)
    return high, (values - high.astype(F32)).astype(BF16)


def head_mean(values, mixer):
    high, rest = low_parts(values)
    return nn(high, mixer) + nn(rest, mixer)


def swap_halves(values):
    lane = lax.broadcasted_iota(jnp.int32, values.shape, 1)
    ahead = pltpu.roll(values, 96, 1)
    behind = pltpu.roll(values, 32, 1)
    return jnp.where(lax.rem(lane, 64) < 32, ahead, behind)


def norm_rows(values, gain):
    inverse = lax.rsqrt(jnp.mean(values * values, axis=-1, keepdims=True) + NORM_EPS)
    return values * inverse * gain


def norm_rows_back(values, gain, upstream):
    inverse = lax.rsqrt(jnp.mean(values * values, axis=-1, keepdims=True) + NORM_EPS)
    scaled = values * inverse
    weighted = upstream * gain
    back = inverse * (weighted - scaled * jnp.mean(weighted * scaled, axis=-1, keepdims=True))
    return back, jnp.sum(upstream * scaled, axis=0, keepdims=True)


class Place:
    def __init__(self, dp_size):
        self.dp_size = dp_size
        self.dp = lax.axis_index("dp")
        self.tensor = lax.axis_index("tensor")
        self.outer_size = dp_size // 2
        self.outer = self.dp // 2
        self.inner = lax.rem(self.dp, 2)
        self.other = self.outer * 2 + 1 - self.inner
        self.side = self.tensor // 2
        self.core = lax.rem(self.tensor, 2)
        self.across = (1 - self.side) * 2 + self.core
        self.twin = self.side * 2 + 1 - self.core

    def ahead(self, shift, inner=None):
        inner = self.inner if inner is None else inner
        return lax.rem(self.outer + shift, self.outer_size) * 2 + inner

    def behind(self, shift):
        return lax.rem(self.outer - shift + self.outer_size, self.outer_size) * 2 + self.inner

    def block(self, step):
        side = 1 - self.side if step < 2 else self.side
        core = 1 - self.core if step % 2 == 0 else self.core
        return side * 2 + core

    def copy(self, src, dst, sems, index, dp=None, tensor=None):
        return pltpu.make_async_remote_copy(
            src_ref=src,
            dst_ref=dst,
            send_sem=sems[0].at[index],
            recv_sem=sems[1].at[index],
            device_id=(
                self.dp if dp is None else dp,
                self.tensor if tensor is None else tensor,
            ),
            device_id_type=MESH,
        )

    def greet(self, everyone):
        barrier = pltpu.get_barrier_semaphore()

        def signal(dp, tensor):
            pl.semaphore_signal(barrier, inc=1, device_id=(dp, tensor), device_id_type=MESH)

        if everyone:

            @pl.loop(1, self.dp_size)
            def _(shift):
                signal(lax.rem(self.dp + shift, self.dp_size), self.tensor)

            for shift in range(1, 4):
                signal(self.dp, lax.rem(self.tensor + shift, 4))
            pl.semaphore_wait(barrier, self.dp_size + 2)
        else:

            @pl.loop(1, self.outer_size)
            def _(shift):
                signal(self.ahead(shift), self.tensor)

            signal(self.other, self.tensor)
            signal(self.dp, self.across)
            signal(self.dp, self.twin)
            pl.semaphore_wait(barrier, self.outer_size + 2)


def pack_gains(packed, terms):
    part = 0
    for row, width in enumerate((terms.shape[1], terms.shape[1], 256)):
        for start in range(0, width, 128):
            packed[part // 3 : part // 3 + 1, 128 * (part % 3) : 128 * (part % 3) + 128] = terms[
                row : row + 1, start : start + 128
            ]
            part += 1


class Gather:
    def __init__(self, place, ref, micro, sems, index, source=None):
        own = ref.at[micro, tile(place.tensor)]
        source = own if source is None else source
        theirs = ref.at[micro, tile(place.across)]
        self.to_across = place.copy(source, own, sems, index, tensor=place.across)
        self.to_twin = place.copy(source, own, sems, index + 1, tensor=place.twin)
        self.on_to_twin = place.copy(theirs, theirs, sems, index + 2, tensor=place.twin)

    def start(self):
        self.to_across.start()
        self.to_twin.start()

    def relay(self):
        self.to_across.wait_recv()
        self.on_to_twin.start()

    def finish(self):
        self.to_twin.wait_recv()
        self.on_to_twin.wait_recv()

    def drain(self):
        self.to_across.wait_send()
        self.to_twin.wait_send()
        self.on_to_twin.wait_send()


class Scatter:
    def __init__(self, place, staged, from_twin, from_across, sems, index):
        self.place = place
        self.staged = staged
        self.from_twin = from_twin
        self.from_across = from_across
        self.sems = sems
        self.index = index

    def twin(self, half):
        return self.place.copy(
            self.staged.at[half],
            self.from_twin.at[half],
            self.sems,
            self.index + half,
            tensor=self.place.twin,
        )

    def crossing(self):
        return self.place.copy(
            self.staged.at[2],
            self.from_across,
            self.sems,
            self.index + 2,
            tensor=self.place.across,
        )

    def give(self, step, values):
        if step == 0 or step == 2:
            half = step // 2
            self.staged[half] = values.astype(BF16)
            self.twin(half).start()
        elif step == 1:
            self.staged[2] = values.astype(BF16)

    def cross(self):
        self.twin(0).wait_recv()
        self.staged[2] = (self.staged[2].astype(F32) + self.from_twin[0].astype(F32)).astype(BF16)
        self.crossing().start()

    def result(self, values):
        self.twin(1).wait_recv()
        self.crossing().wait_recv()
        return values + self.from_twin[1].astype(F32) + self.from_across[...].astype(F32)

    def drain(self):
        self.twin(0).wait_send()
        self.twin(1).wait_send()
        self.crossing().wait_send()


def fill_mixer(mixer):
    row = lax.broadcasted_iota(jnp.int32, mixer.shape, 0) // DH
    column = lax.broadcasted_iota(jnp.int32, mixer.shape, 1) // DH
    mixer[...] = jnp.where(row == column, 1.0 / DH, 0.0).astype(BF16)


class Weights:
    def __init__(self, place, shard, full, outer_sems, inner_sems, piece):
        self.place = place
        self.shard = shard
        self.full = full
        self.outer_sems = outer_sems
        self.inner_sems = inner_sems
        self.piece = piece
        self.rows = shard.shape[0]

    def at(self, index):
        return self.full.at[pl.ds(pl.multiple_of(index * self.rows, self.rows), self.rows), :]

    def hop(self, way, distance, own=False):
        place = self.place
        step = 1 - 2 * way
        rows = self.at((place.outer - step * (distance - 1)) * 2 + place.inner)
        return place.copy(
            self.shard if own else rows,
            rows,
            self.outer_sems,
            (self.piece, way, distance),
            dp=(place.outer + step) * 2 + place.inner,
        )

    def inner_copy(self, source, own=False):
        place = self.place
        rows = self.at(source * 2 + place.inner)
        return place.copy(
            self.shard if own else rows,
            rows,
            self.inner_sems,
            (self.piece, source),
            dp=place.other,
        )

    def arrival(self, way, distance):
        place = self.place
        rows = self.at(place.dp)
        return place.copy(
            rows, rows, self.outer_sems, (self.piece, way, distance), dp=place.other
        )

    def goes(self, way):
        place = self.place
        return place.outer > 0 if way else place.outer + 1 < place.outer_size

    def begin(self):
        for way in range(2):

            @pl.when(self.goes(way))
            def _():
                self.hop(way, 1, own=True).start()

        self.inner_copy(self.place.outer, own=True).start()

    def relay(self, first, last):
        place = self.place

        @pl.loop(first, last)
        def _(distance):
            for way in range(2):
                source = place.outer + distance if way else place.outer - distance

                @pl.when((source >= 0) & (source < place.outer_size))
                def _():
                    self.arrival(way, distance).wait_recv()

                    @pl.when(self.goes(way))
                    def _():
                        self.hop(way, distance + 1).start()

                    self.inner_copy(source).start()

    def finish(self):
        @pl.loop(0, self.place.outer_size)
        def _(source):
            self.inner_copy(source).wait_recv()

    def drain(self):
        place = self.place

        @pl.loop(0, place.outer_size)
        def _(source):
            self.inner_copy(source).wait_send()
            for way in range(2):
                distance = source - place.outer + 1 if way else place.outer - source + 1

                @pl.when(self.goes(way) & (distance >= 1))
                def _():
                    self.hop(way, distance).wait_send()


def rotation_angles(length):
    frequency = ROPE_BASE ** (-2.0 * (np.arange(128) % (DH // 2)) / DH)
    steps = np.arange(8) * TILE if length <= 8 * TILE else np.arange(0, length, TILE)
    positions = np.concatenate([np.arange(TILE), steps])
    turns = positions[:, None] * frequency[None, :]
    return jnp.asarray(np.stack([np.cos(turns), np.sin(turns)]).astype(np.float32))


def forward_kernel(
    dp_size,
    turned,
    tokens,
    cotangent,
    segments,
    w_query,
    w_key,
    w_value,
    w_out,
    gate_shard,
    up_shard,
    w_down,
    attn_gain,
    ffn_gain,
    query_gain,
    key_gain,
    angles,
    out_qkv_full,
    out_back_full,
    out_gate_full,
    out_up_full,
    out_down_full,
    out_normed,
    out_ffn,
    out_cot,
    out_gate_slope,
    out_up_slope,
    out_hidden,
    out_grad_down,
    out_query,
    out_key,
    out_value,
    out_attended,
    out_proj,
    out_middle,
    out_tables,
    qkv_shard,
    back_shard,
    down_shard,
    tables,
    query_marks,
    key_marks,
    mixer,
    normed,
    ffn_all,
    cot_all,
    qkv_full,
    back_full,
    gate_full,
    up_full,
    slopes,
    hidden,
    grad_down,
    query,
    key,
    value,
    attended,
    proj,
    middle,
    staged,
    from_twin,
    from_across,
    outer_send,
    outer_recv,
    inner_send,
    inner_recv,
    group_send,
    group_recv,
    local_sems,
    slope_sems,
):
    place = Place(dp_size)
    micro_count = tokens.shape[0]
    block_count = normed.shape[1] // TILE
    outer_size = place.outer_size
    group_sems = (group_send, group_recv)
    outer_sems = (outer_send, outer_recv)
    inner_sems = (inner_send, inner_recv)
    own = tile(place.tensor)
    first_cut = 1 + (outer_size - 1) // 3
    second_cut = 1 + 2 * (outer_size - 1) // 3
    qkv_w = Weights(place, qkv_shard, qkv_full, outer_sems, inner_sems, 0)
    back_w = Weights(place, back_shard, back_full, outer_sems, inner_sems, 1)
    gate_w = Weights(place, gate_shard, gate_full, outer_sems, inner_sems, 2)
    up_w = Weights(place, up_shard, up_full, outer_sems, inner_sems, 3)
    down_w = Weights(place, down_shard, out_down_full, outer_sems, inner_sems, 4)
    normed_g = [Gather(place, normed, m, group_sems, 3 * m) for m in range(micro_count)]
    cot_g = [
        Gather(place, cot_all, m, group_sems, 6 + 3 * m, cotangent.at[m])
        for m in range(micro_count)
    ]
    ffn_g = [Gather(place, ffn_all, m, group_sems, 12 + 3 * m) for m in range(micro_count)]

    def branch_s(m):
        return Scatter(
            place, staged.at[m], from_twin.at[m], from_across.at[m], group_sems, 18 + 3 * m
        )

    saves = []
    used = []

    def save(src, dst):
        copy = pltpu.make_async_copy(src, dst, local_sems.at[len(used)])
        copy.start()
        saves.append(copy)
        used.append(copy)
        return copy

    def save_columns(src, dst, m):
        for block in range(dst.shape[0]):
            save(src.at[m, :, TILE * block : TILE * block + TILE], dst.at[block, m])

    lane = lax.broadcasted_iota(jnp.int32, (TILE, 128), 1)
    front = lane < 64
    place_in = rem(lane, 64)

    value_end = w_query.shape[1] + w_key.shape[1]
    qkv_shard[:, : w_query.shape[1]] = w_query[...]
    qkv_shard[:, w_query.shape[1] : value_end] = w_key[...]
    qkv_shard[:, value_end:] = w_value[...]
    for m in range(micro_count):
        normed[m, own] = norm_rows(tokens[m].astype(F32), attn_gain[...]).astype(BF16)
    if turned:
        back_shard[...] = w_out[...]
        down_shard[...] = w_down[...]
    else:
        back_shard[...] = w_out[...].T
        down_shard[...] = w_down[...].T
    place.greet(False)
    cuts = (1, first_cut, second_cut, outer_size)
    order = (qkv_w, back_w, gate_w, up_w, down_w)

    def take(item):
        part = item % 3
        order[item // 3].relay(cuts[part], cuts[part + 1])

    qkv_w.begin()
    normed_g[0].start()

    def prepare():
        fill_mixer(mixer)
        sign = jnp.where(place_in < 32, -1.0, 1.0)
        for kind, (gain_ref, scale) in enumerate(((query_gain, DH**-0.5 / LN2), (key_gain, 1.0))):
            gain = jnp.broadcast_to(
                jnp.concatenate([gain_ref[...], gain_ref[...]], axis=1) * scale, (TILE, 128)
            )
            crossed = swap_halves(gain) * sign
            for block in range(block_count):
                rows = slice(block * TILE, (block + 1) * TILE)
                cos_step = angles[0, TILE + block : TILE + block + 1]
                sin_step = angles[1, TILE + block : TILE + block + 1]
                cosine = angles[0, 0:TILE] * cos_step - angles[1, 0:TILE] * sin_step
                sine = angles[1, 0:TILE] * cos_step + angles[0, 0:TILE] * sin_step
                tables[2 * kind, rows] = cosine * gain
                tables[2 * kind + 1, rows] = sine * crossed
        row = lax.broadcasted_iota(jnp.int32, (16, 128), 0)
        mark_lane = lax.broadcasted_iota(jnp.int32, (16, 128), 1)
        spread = jnp.where(mark_lane == row + 8, 1.0, 0.0).astype(BF16)
        used = (lane >= 8) & (lane < 11)
        for m in range(micro_count):
            for block in range(block_count):
                rows = slice(block * TILE, (block + 1) * TILE)
                ids = jnp.broadcast_to(segments[m, :, rows], (16, TILE))
                match = lax.broadcasted_iota(jnp.int32, (16, TILE), 0) == ids
                marks = tn(jnp.where(match, 1.0, 0.0).astype(BF16), spread)
                query_marks[m, rows] = marks.astype(BF16)
                apart = jnp.where(used, APART * (1.0 - marks), 0.0)
                for head in range(2):
                    chosen = (lane >= 64 * head) & (lane < 64 * head + 3)
                    key_marks[head, m, rows] = jnp.where(chosen, 1.0, apart).astype(BF16)
        qkv_w.at(place.dp)[...] = qkv_shard[...]
        back_w.at(place.dp)[...] = back_shard[...]

    own_loads = [
        save(gate_shard, gate_w.at(place.dp)),
        save(up_shard, up_w.at(place.dp)),
        save(cotangent.at[0], cot_all.at[0, own]),
        save(cotangent.at[1], cot_all.at[1, own]),
    ]
    prepare()
    save(down_shard, down_w.at(place.dp))
    save(tables, out_tables)
    take(0)
    back_w.begin()
    take(1)
    normed_g[1].start()
    take(2)
    take(3)
    gate_w.begin()

    later = lax.broadcasted_iota(jnp.int32, (TILE, TILE), 1) > lax.broadcasted_iota(
        jnp.int32, (TILE, TILE), 0
    )
    causal = jnp.where(later, APART, 0.0)

    def project(m):
        @pl.loop(0, block_count)
        def _(block):
            rows = tile(block)
            product = nn(normed[m, rows], qkv_full[...])
            proj[m, rows] = product[:, :384]
            heads = product[:, :256]
            inverse = lax.rsqrt(head_mean(heads * heads, mixer[...]) + NORM_EPS)
            for group in range(2):
                lanes = slice(128 * group, 128 * group + 128)
                part = heads[:, lanes]
                turned = part * tables[0, rows] + swap_halves(part) * tables[1, rows]
                query[m, group, rows, 0:128] = (turned * inverse[:, lanes]).astype(BF16)
                query[m, group, rows, 128:256] = query_marks[m, rows]
            part = product[:, 256:384]
            inverse = lax.rsqrt(head_mean(part * part, mixer[0:128, 0:128]) + NORM_EPS)
            turned = (part * tables[2, rows] + swap_halves(part) * tables[3, rows]) * inverse
            moved = pltpu.roll(turned, 64, 1)
            val = product[:, 384:512]
            val_moved = pltpu.roll(val, 64, 1)
            for group in range(2):
                first, second = (turned, moved) if group == 0 else (moved, turned)
                key[m, group, 0, rows, 0:128] = jnp.where(front, first, 0.0).astype(BF16)
                key[m, group, 1, rows, 0:128] = jnp.where(front, 0.0, second).astype(BF16)
                first, second = (val, val_moved) if group == 0 else (val_moved, val)
                value[m, group, 0, rows, 0:128] = jnp.where(front, first, 0.0).astype(BF16)
                value[m, group, 1, rows, 0:128] = jnp.where(front, 0.0, second).astype(BF16)
                for head in range(2):
                    key[m, group, head, rows, 128:256] = key_marks[head, m, rows]
                value[m, group, 0, rows, 128:256] = jnp.where(front, 1.0, 0.0).astype(BF16)
                value[m, group, 1, rows, 128:256] = jnp.where(front, 0.0, 1.0).astype(BF16)

    def attend(m):
        @pl.loop(0, 2)
        def _(group):
            for block in range(block_count):
                rows = slice(block * TILE, (block + 1) * TILE)
                query_block = query[m, group, rows]
                total = jnp.zeros((TILE, 256), F32)
                for head in range(2):
                    if block > 0:
                        before = slice(0, block * TILE)
                        scores = nt(query_block, key[m, group, head, before])
                        weights = jnp.exp2(scores).astype(BF16)
                        total = total + nn(weights, value[m, group, head, before])
                    scores = nt(query_block, key[m, group, head, rows]) + causal
                    weights = jnp.exp2(scores).astype(BF16)
                    total = total + nn(weights, value[m, group, head, rows])
                sums = total[:, 128:256]
                attended[m, group, rows] = (total[:, 0:128] / sums).astype(BF16)
                shift = -jnp.log2(sums)
                high = shift.astype(BF16)
                middle_part = (shift - high.astype(F32)).astype(BF16)
                last = (shift - high.astype(F32) - middle_part.astype(F32)).astype(BF16)
                marks = jnp.where(
                    place_in == 0,
                    high.astype(F32),
                    jnp.where(
                        place_in == 1,
                        middle_part.astype(F32),
                        jnp.where(
                            place_in == 2,
                            last.astype(F32),
                            query_block[:, 128:256].astype(F32),
                        ),
                    ),
                )
                query[m, group, rows, 128:256] = marks.astype(BF16)

    def branch_block(m, step):
        rows = tile(place.block(step))
        heads = jnp.concatenate([attended[m, 0, rows], attended[m, 1, rows]], axis=1)
        return nt(heads, back_full[...])

    def branch(m):
        for step in range(3):
            branch_s(m).give(step, branch_block(m, step))

    def enter_ffn(m):
        total = branch_s(m).result(branch_block(m, 3))
        middle[m] = tokens[m].astype(F32) + total
        save(middle.at[m], out_middle.at[m])
        ffn_all[m, own] = norm_rows(middle[m], ffn_gain[...]).astype(BF16)
        ffn_g[m].start()

    @pl.loop(0, micro_count)
    def _(m):
        @pl.when(m == 0)
        def _():
            normed_g[0].relay()
            take(4)
            normed_g[0].finish()
            qkv_w.finish()

        @pl.when(m == 1)
        def _():
            normed_g[1].finish()

        project(m)

        @pl.when(m == 0)
        def _():
            take(5)
            cot_g[0].start()

        attend(m)

        @pl.when(m == 0)
        def _():
            normed_g[1].relay()
            back_w.finish()

        branch(m)

        @pl.when(m == 0)
        def _():
            take(6)

        branch_s(m).cross()

        @pl.when(m == 0)
        def _():
            take(7)

        @pl.when(m == 1)
        def _():
            take(8)
            up_w.begin()

    save(qkv_full, out_qkv_full)
    save(back_full, out_back_full)
    for m in range(micro_count):
        save(query.at[m], out_query.at[m])
        save(key.at[m], out_key.at[m])
        save(value.at[m], out_value.at[m])
        save(attended.at[m], out_attended.at[m])
        save(proj.at[m], out_proj.at[m])
        save_columns(normed, out_normed, m)
    cot_g[0].relay()
    enter_ffn(0)
    take(9)
    enter_ffn(1)
    take(10)
    gate_w.finish()
    for copy in own_loads:
        saves.remove(copy)
        copy.wait()
    save(gate_full, out_gate_full)
    take(11)
    down_w.begin()
    cot_g[0].finish()
    save(cot_all.at[0], out_cot.at[0])
    ffn_g[0].relay()
    cot_g[1].start()
    ffn_g[0].finish()
    save_columns(ffn_all, out_ffn, 0)
    tile_count = micro_count * block_count

    @pl.loop(0, tile_count)
    def _(index):
        m = index // block_count
        rows = tile(rem(index, block_count))

        @pl.when(index == block_count)
        def _():
            take(12)
            ffn_g[1].relay()
            ffn_g[1].finish()

        hidden[m, rows] = nn(ffn_all[m, rows], gate_full[...]).astype(BF16)

    take(13)
    save_columns(ffn_all, out_ffn, 1)
    up_w.finish()
    save(up_full, out_up_full)

    def slope_copies(index):
        m = index // block_count
        rows = tile(rem(index, block_count))
        slot = rem(index, 2)
        return [
            pltpu.make_async_copy(
                slopes.at[slot, kind], out.at[m, rows], slope_sems.at[slot, kind]
            )
            for kind, out in enumerate((out_gate_slope, out_up_slope))
        ]

    @pl.loop(0, tile_count)
    def _(index):
        m = index // block_count
        rows = tile(rem(index, block_count))
        slot = rem(index, 2)

        @pl.when(index >= 2)
        def _():
            for copy in slope_copies(index - 2):
                copy.wait()

        gate = hidden[m, rows].astype(F32)
        up = nn(ffn_all[m, rows], up_full[...])
        sig = 1.0 / (1.0 + jnp.exp(-gate))
        act = gate * sig
        hidden[m, rows] = (act * up).astype(BF16)
        slopes[slot, 0] = (up * (sig + act * (1.0 - sig))).astype(BF16)
        slopes[slot, 1] = act.astype(BF16)
        for copy in slope_copies(index):
            copy.start()

    save(hidden, out_hidden)

    def down_copy(block):
        rows = tile(block)
        return pltpu.make_async_copy(
            grad_down.at[rows], out_grad_down.at[rows], slope_sems.at[2 + block // 2, rem(block, 2)]
        )

    for index in (tile_count - 2, tile_count - 1):
        for copy in slope_copies(index):
            copy.wait()
    take(14)

    @pl.loop(0, block_count)
    def _(block):
        columns = tile(block)
        grad_down[columns] = tn(cot_all[0, :, columns], hidden[0]).astype(BF16)

        @pl.when(block == block_count // 2)
        def _():
            cot_g[1].relay()

    cot_g[1].finish()
    save(cot_all.at[1], out_cot.at[1])

    @pl.loop(0, block_count)
    def _(block):
        columns = tile(block)
        grad_down[columns] = (
            grad_down[columns].astype(F32) + tn(cot_all[1, :, columns], hidden[1])
        ).astype(BF16)
        down_copy(block).start()

    down_w.finish()
    for piece in (qkv_w, back_w, gate_w, up_w, down_w):
        piece.drain()
    for m in range(micro_count):
        normed_g[m].drain()
        cot_g[m].drain()
        ffn_g[m].drain()
        branch_s(m).drain()
    for block in range(block_count):
        down_copy(block).wait()
    for copy in saves:
        copy.wait()


def forward(dp_size, tokens, cotangent, segments, weights, gains):
    w_query, w_key, w_value, w_out, w_gate, w_up, w_down = weights
    micro, rows, width = tokens.shape
    length = segments.shape[2]
    share, hidden_width = w_gate.shape
    qkv_width = w_query.shape[1] + w_key.shape[1] + w_value.shape[1]
    back_width = w_out.shape[0]
    turned = share % 128 != 0
    if turned:
        w_out, w_down = w_out.T, w_down.T
    outer_size = dp_size // 2
    whole = pl.BlockSpec(memory_space=pltpu.VMEM)
    anywhere = pl.BlockSpec(memory_space=pl.ANY)
    shape = jax.ShapeDtypeStruct
    out_shape = [
        shape((width, qkv_width), BF16),
        shape((width, back_width), BF16),
        shape((width, hidden_width), BF16),
        shape((width, hidden_width), BF16),
        shape((width, hidden_width), BF16),
        shape((width // TILE, micro, length, TILE), BF16),
        shape((width // TILE, micro, length, TILE), BF16),
        shape((micro, length, width), BF16),
        shape((micro, length, hidden_width), BF16),
        shape((micro, length, hidden_width), BF16),
        shape((micro, length, hidden_width), BF16),
        shape((width, hidden_width), BF16),
        shape((micro, 2, length, 256), BF16),
        shape((micro, 2, 2, length, 256), BF16),
        shape((micro, 2, 2, length, 256), BF16),
        shape((micro, 2, length, 128), BF16),
        shape((micro, length, 384), F32),
        shape((micro, rows, width), F32),
        shape((4, length, 128), F32),
    ]
    scratch = [
        pltpu.VMEM((share, qkv_width), BF16),
        pltpu.VMEM((share, back_width), BF16),
        pltpu.VMEM((share, hidden_width), BF16),
        pltpu.VMEM((4, length, 128), F32),
        pltpu.VMEM((micro, length, 128), BF16),
        pltpu.VMEM((2, micro, length, 128), BF16),
        pltpu.VMEM((256, 256), BF16),
        pltpu.VMEM((micro, length, width), BF16),
        pltpu.VMEM((micro, length, width), BF16),
        pltpu.VMEM((micro, length, width), BF16),
        pltpu.VMEM((width, qkv_width), BF16),
        pltpu.VMEM((width, back_width), BF16),
        pltpu.VMEM((width, hidden_width), BF16),
        pltpu.VMEM((width, hidden_width), BF16),
        pltpu.VMEM((2, 2, TILE, hidden_width), BF16),
        pltpu.VMEM((micro, length, hidden_width), BF16),
        pltpu.VMEM((width, hidden_width), BF16),
        pltpu.VMEM((micro, 2, length, 256), BF16),
        pltpu.VMEM((micro, 2, 2, length, 256), BF16),
        pltpu.VMEM((micro, 2, 2, length, 256), BF16),
        pltpu.VMEM((micro, 2, length, 128), BF16),
        pltpu.VMEM((micro, length, 384), F32),
        pltpu.VMEM((micro, rows, width), F32),
        pltpu.VMEM((micro, 3, rows, width), BF16),
        pltpu.VMEM((micro, 2, rows, width), BF16),
        pltpu.VMEM((micro, rows, width), BF16),
        pltpu.SemaphoreType.DMA((5, 2, outer_size)),
        pltpu.SemaphoreType.DMA((5, 2, outer_size)),
        pltpu.SemaphoreType.DMA((5, outer_size)),
        pltpu.SemaphoreType.DMA((5, outer_size)),
        pltpu.SemaphoreType.DMA((24,)),
        pltpu.SemaphoreType.DMA((24,)),
        pltpu.SemaphoreType.DMA((48,)),
        pltpu.SemaphoreType.DMA((4, 2)),
    ]
    operands = (
        tokens,
        cotangent,
        segments,
        w_query,
        w_key,
        w_value,
        w_out,
        w_gate,
        w_up,
        w_down,
        *gains,
        rotation_angles(length),
    )
    return pl.pallas_call(
        functools.partial(forward_kernel, dp_size, turned),
        out_shape=out_shape,
        in_specs=[anywhere if index in (1, 7, 8) else whole for index in range(len(operands))],
        out_specs=[anywhere] * len(out_shape),
        scratch_shapes=scratch,
        compiler_params=pltpu.CompilerParams(
            collective_id=0, has_side_effects=True, vmem_limit_bytes=VMEM_LIMIT
        ),
        name="forward_pass",
    )(*operands)


class Shares:
    def __init__(self, place, partial, kept, from_inner, from_outer, outer_sems, inner_sems, piece):
        self.place = place
        self.partial = partial
        self.kept = kept
        self.from_inner = from_inner
        self.from_outer = from_outer
        self.outer_sems = outer_sems
        self.inner_sems = inner_sems
        self.piece = piece
        self.rows = from_inner.shape[1]

    def at(self, index):
        return self.partial.at[pl.ds(pl.multiple_of(index * self.rows, self.rows), self.rows), :]

    def mine(self, shift):
        if self.kept is not None:
            return self.kept.at[shift]
        return self.at(self.place.ahead(shift))

    def inner_copy(self, shift):
        place = self.place
        return place.copy(
            self.at(place.ahead(shift, 1 - place.inner)),
            self.from_inner.at[shift],
            self.inner_sems,
            (self.piece, shift),
            dp=place.other,
        )

    def outer_copy(self, shift):
        place = self.place
        return place.copy(
            self.mine(shift),
            self.from_outer.at[shift - 1],
            self.outer_sems,
            (self.piece, shift),
            dp=place.ahead(shift),
        )

    def give(self, first, last):
        @pl.loop(first, last)
        def _(shift):
            self.inner_copy(shift).start()

    def turn(self, first, last):
        @pl.loop(first, last)
        def _(shift):
            self.inner_copy(shift).wait_recv()
            mine = self.mine(shift)
            mine[...] = (mine[...].astype(F32) + self.from_inner[shift].astype(F32)).astype(BF16)
            self.outer_copy(shift).start()

    def keep(self, total):
        self.inner_copy(0).wait_recv()
        total[...] = self.mine(0)[...].astype(F32) + self.from_inner[0].astype(F32)

    def finish(self, total):
        @pl.loop(1, self.place.outer_size)
        def _(shift):
            self.outer_copy(shift).wait_recv()
            total[...] += self.from_outer[shift - 1].astype(F32)

    def drain(self):
        self.inner_copy(0).wait_send()

        @pl.loop(1, self.place.outer_size)
        def _(shift):
            self.inner_copy(shift).wait_send()
            self.outer_copy(shift).wait_send()


def backward_kernel(
    dp_size,
    cotangent,
    attn_gain,
    ffn_gain,
    tokens,
    qkv_full,
    back_full,
    gate_full,
    up_full,
    down_full,
    normed,
    ffn_all,
    cot_all,
    gate_slope,
    up_slope,
    hidden,
    grad_down,
    query,
    key,
    value,
    attended,
    proj,
    middle_in,
    tables,
    out_mixed,
    out_tokens,
    gain_sums,
    out_qkv,
    out_back,
    out_gate,
    out_up,
    out_down,
    mixed,
    mid_all,
    mixer,
    ffn_w,
    down_w,
    qkv_w,
    att,
    qry,
    ky,
    val,
    prj,
    down_kept,
    qkv_inner,
    back_inner,
    ffn_inner,
    down_inner,
    qkv_outer,
    back_outer,
    ffn_outer,
    down_outer,
    staged,
    part_twin,
    part_across,
    out_twin,
    out_across,
    middle,
    gain_parts,
    gain_packed,
    gain_group,
    gain_dp,
    outer_send,
    outer_recv,
    inner_send,
    inner_recv,
    group_send,
    group_recv,
    gain_send,
    gain_recv,
    local_sems,
    tile_sems,
):
    place = Place(dp_size)
    micro_count = mixed.shape[0]
    length = mid_all.shape[1]
    width = mid_all.shape[2]
    hidden_width = down_w.shape[1]
    block_count = length // TILE
    tile_count = micro_count * block_count
    outer_size = place.outer_size
    group_sems = (group_send, group_recv)
    outer_sems = (outer_send, outer_recv)
    inner_sems = (inner_send, inner_recv)
    own = tile(place.tensor)
    first_cut = 1 + (outer_size - 1) // 3
    second_cut = 1 + 2 * (outer_size - 1) // 3
    outers = outer_size // 4
    own_outer_block = place.outer // outers
    counter = []

    def load(src, dst):
        copy = pltpu.make_async_copy(src, dst, local_sems.at[len(counter) + (8 if len(counter) >= 8 else 0)])
        counter.append(copy)
        copy.start()
        return copy

    down_s = Shares(place, grad_down, down_kept, down_inner, down_outer, outer_sems, inner_sems, 4)

    def ffn_shares(kind):
        return Shares(
            place,
            ffn_w.at[kind],
            None,
            ffn_inner.at[kind],
            ffn_outer.at[kind],
            outer_sems,
            inner_sems,
            2 + kind,
        )

    gate_s, up_s = ffn_shares(0), ffn_shares(1)
    mid_g = [Gather(place, mid_all, m, group_sems, 3 * m) for m in range(micro_count)]

    def turn_block(step):
        return rem(step + 1 + own_outer_block, 4)

    cuts = (1, first_cut, second_cut, outer_size)

    def issue(share, part):
        share.give(*((0, 1) if part == 3 else (cuts[part], cuts[part + 1])))

    def take(share, part):
        share.turn(cuts[part], cuts[part + 1])

    def twin_copy(kind, m, half):
        from_twin = (part_twin, out_twin, part_twin)[kind]
        return place.copy(
            staged.at[m, half],
            from_twin.at[m, half],
            group_sems,
            6 + 6 * kind + 3 * m + half,
            tensor=place.twin,
        )

    def across_copy(kind, m):
        from_across = (part_across, out_across, part_across)[kind]
        return place.copy(
            staged.at[m, 2],
            from_across.at[m],
            group_sems,
            6 + 6 * kind + 3 * m + 2,
            tensor=place.across,
        )

    def block_of(step):
        side = jnp.where(step < 2, 1 - place.side, place.side)
        core = jnp.where(rem(step, 2) == 0, 1 - place.core, place.core)
        return side * 2 + core

    def hand_out(m, step, values):
        staged[m, rem(step, 2) * 2 + step // 2] = values.astype(BF16)

    def send_twin(kind, m, step):
        @pl.when(rem(step, 2) == 0)
        def _():
            twin_copy(kind, m, step // 2).start()

    def cross(kind, m):
        from_twin = (part_twin, out_twin, part_twin)[kind]
        twin_copy(kind, m, 0).wait_recv()
        staged[m, 2] = (staged[m, 2].astype(F32) + from_twin[m, 0].astype(F32)).astype(BF16)
        across_copy(kind, m).start()

    def collect(kind, m):
        from_twin = (part_twin, out_twin, part_twin)[kind]
        from_across = (part_across, out_across, part_across)[kind]
        twin_copy(kind, m, 1).wait_recv()
        across_copy(kind, m).wait_recv()
        return staged[m, 3].astype(F32) + from_twin[m, 1].astype(F32) + from_across[m].astype(F32)

    def drain(kind, m):
        twin_copy(kind, m, 0).wait_send()
        twin_copy(kind, m, 1).wait_send()
        across_copy(kind, m).wait_send()

    def leave_ffn(m):
        upstream = collect(0, m)
        back, term = norm_rows_back(middle[m], ffn_gain[...], upstream)
        mid_all[m, own] = (mixed[m].astype(F32) + back).astype(BF16)
        mid_g[m].start()
        gain_parts[1:2, :] += term

    def leave_out(m):
        mixed[m] = (middle[m] + collect(1, m)).astype(BF16)

    def attn_copies():
        pairs = (
            (back_full, qkv_w.at[:, 512:768]),
            (attended, att),
            (value.at[0], val),
            (key.at[0], ky),
            (query.at[0], qry),
            (proj.at[0], prj),
            (qkv_full, qkv_w.at[:, 0:512]),
        )
        return [
            pltpu.make_async_copy(src, dst, local_sems.at[30 + index])
            for index, (src, dst) in enumerate(pairs)
        ]

    def rows_of(index):
        return index // block_count, tile(block_of(rem(index, block_count)))

    def ffn_phase(grads, rows_buf, ffn_cols):
        def rows_copy(index):
            m, rows = rows_of(index)
            slot = rem(index, 2)
            return pltpu.make_async_copy(cot_all.at[m, rows], rows_buf.at[slot], tile_sems.at[0, slot])

        def cols_copy(index):
            slot = rem(index, 2)
            return pltpu.make_async_copy(
                ffn_all.at[turn_block(rem(index, block_count))], ffn_cols.at[slot], tile_sems.at[2, slot]
            )

        loads = [load(down_full, down_w)]
        rows_copy(0).start()
        loads += [load(gate_slope.at[0], grads.at[0, 0]), load(up_slope.at[0], grads.at[1, 0])]
        loads += [load(gate_full, ffn_w.at[0]), load(up_full, ffn_w.at[1])]
        others = [
            load(gate_slope.at[1], grads.at[0, 1]),
            load(up_slope.at[1], grads.at[1, 1]),
            load(middle_in, middle),
            load(cotangent, mixed),
        ]

        def kept_copy(shift):
            return pltpu.make_async_copy(
                down_s.at(place.ahead(shift)), down_kept.at[shift], local_sems.at[40 + shift]
            )

        @pl.loop(0, outer_size)
        def _(shift):
            kept_copy(shift).start()

        fill_mixer(mixer)
        gain_parts[...] = jnp.zeros_like(gain_parts)
        gain_packed[...] = jnp.zeros_like(gain_packed)
        place.greet(True)
        issue(down_s, 0)
        issue(down_s, 1)
        for copy in loads:
            copy.wait()

        @pl.loop(0, tile_count)
        def _(index):
            m, rows = rows_of(index)
            step = rem(index, block_count)
            slot = rem(index, 2)

            @pl.when(index + 1 < tile_count)
            def _():
                rows_copy(index + 1).start()

            @pl.when(index == block_count)
            def _():
                pltpu.make_async_copy(gate_slope.at[1], grads.at[0, 1], local_sems.at[5]).wait()
                pltpu.make_async_copy(up_slope.at[1], grads.at[1, 1], local_sems.at[6]).wait()

            @pl.when(index == 2)
            def _():
                @pl.loop(0, outer_size)
                def _(shift):
                    kept_copy(shift).wait()

                take(down_s, 0)
                issue(down_s, 2)

            @pl.when(index == block_count + 1)
            def _():
                take(down_s, 1)
                issue(down_s, 3)

            rows_copy(index).wait()
            hidden_grad = nn(rows_buf[slot], down_w[...])
            gate_low = (hidden_grad * grads[0, m, rows].astype(F32)).astype(BF16)
            up_low = (hidden_grad * grads[1, m, rows].astype(F32)).astype(BF16)
            grads[0, m, rows] = gate_low
            grads[1, m, rows] = up_low
            hand_out(m, step, nt(gate_low, ffn_w[0]) + nt(up_low, ffn_w[1]))

            send_twin(0, m, step)

            @pl.when(index == 2)
            def _():
                cross(0, 0)

        for copy in attn_copies():
            copy.start()
        cols_copy(0).start()
        for copy in others[2:]:
            copy.wait()
        leave_ffn(0)
        cross(0, 1)

        @pl.loop(0, 2 * block_count)
        def _(index):
            kind = index // block_count
            block = turn_block(rem(index, block_count))
            slot = rem(index, 2)
            cols_copy(index).wait()

            @pl.when(index + 1 < 2 * block_count)
            def _():
                cols_copy(index + 1).start()

            ffn_w[kind, tile(block)] = (
                tn(
                    ffn_cols[slot].reshape(micro_count * length, TILE),
                    grads[kind].reshape(micro_count * length, hidden_width),
                )
            ).astype(BF16)

            @pl.when(index == 1)
            def _():
                take(down_s, 2)
                if outers == 1:
                    issue(gate_s, 0)

            @pl.when(index == block_count - 1)
            def _():
                if outers > 1:
                    issue(gate_s, 0)
                issue(gate_s, 1)

            @pl.when(index == block_count + 3)
            def _():
                take(gate_s, 0)
                issue(gate_s, 2)

    pl.run_scoped(
        ffn_phase,
        pltpu.VMEM((2, micro_count, length, hidden_width), BF16),
        pltpu.VMEM((2, TILE, width), BF16),
        pltpu.VMEM((2, micro_count, length, TILE), BF16),
    )

    def attn_phase(
        toks,
        tabs,
        hidden_buf,
        grad_att,
        grad_q,
        grad_k,
        grad_v,
        grad_qkv,
        qkv_total,
        back_total,
        gate_total,
        up_total,
        down_total,
    ):
        qkv_part = down_w.at[:, 0:512]
        back_part = down_w.at[:, 512:768]
        qkv_s = Shares(place, qkv_part, None, qkv_inner, qkv_outer, outer_sems, inner_sems, 0)
        back_s = Shares(place, back_part, None, back_inner, back_outer, outer_sems, inner_sems, 1)
        lane = lax.broadcasted_iota(jnp.int32, (TILE, 128), 1)
        front = lane < 64
        place_in = rem(lane, 64)
        later = lax.broadcasted_iota(jnp.int32, (TILE, TILE), 0) > lax.broadcasted_iota(
            jnp.int32, (TILE, TILE), 1
        )
        causal = jnp.where(later, APART, 0.0)
        small = mixer[0:128, 0:128]
        table_load = load(tables, tabs)
        token_load = load(tokens, toks)

        def score_ready(m):
            @pl.loop(0, block_count)
            def _(block):
                rows = tile(block)
                low = nn(mid_all[m, rows], qkv_w[:, 512:768]).astype(BF16)
                for group in range(2):
                    part = low[:, 128 * group : 128 * group + 128]
                    both = part.astype(F32) * att[m, group, rows].astype(F32)
                    shift = head_mean(both, small) * -64.0
                    high = shift.astype(BF16)
                    rest = shift - high.astype(F32)
                    mid = rest.astype(BF16)
                    last = (rest - mid.astype(F32)).astype(BF16)
                    marks = jnp.where(
                        place_in == 0,
                        high.astype(F32),
                        jnp.where(
                            place_in == 1,
                            mid.astype(F32),
                            jnp.where(place_in == 2, last.astype(F32), 0.0),
                        ),
                    )
                    grad_att[group, rows, 0:128] = part
                    grad_att[group, rows, 128:256] = marks.astype(BF16)

        def attend_back(m, between):
            @pl.loop(0, 2)
            def _(group):
                for block in range(block_count):
                    rows = slice(block * TILE, (block + 1) * TILE)
                    spans = [(rows, True)]
                    if block + 1 < block_count:
                        spans.append((slice((block + 1) * TILE, length), False))
                    sums_k = []
                    sums_v = []
                    for head in range(2):
                        key_block = ky[group, head, rows]
                        value_block = val[group, head, rows]
                        sum_k = None
                        sum_v = None
                        for span, masked in spans:
                            query_span = qry[group, span]
                            grad_span = grad_att[group, span]
                            scores = nt(key_block, query_span)
                            if masked:
                                scores = scores + causal
                            probs = jnp.exp2(scores)
                            score_grad = (probs * nt(value_block, grad_span)).astype(BF16)
                            probs_low = probs.astype(BF16)
                            part_v = nn(probs_low, grad_span[:, 0:128])
                            part_k = nn(score_grad, query_span[:, 0:128])
                            sum_v = part_v if sum_v is None else sum_v + part_v
                            sum_k = part_k if sum_k is None else sum_k + part_k
                            part_q = tn(score_grad, key_block[:, 0:128])
                            if block == 0 and head == 0:
                                grad_q[group, span] = part_q
                            else:
                                grad_q[group, span] += part_q
                        sums_k.append(sum_k)
                        sums_v.append(sum_v)
                    both_k = jnp.where(front, sums_k[0], sums_k[1])
                    both_v = jnp.where(front, sums_v[0], sums_v[1])
                    grad_k[group, rows] = both_k + pltpu.roll(both_k, 64, 1)
                    grad_v[group, rows] = both_v + pltpu.roll(both_v, 64, 1)

                between(group)

        def normalize_back(grads, values, cosine, sine):
            scaled = grads * LN2
            weighted = scaled * cosine + swap_halves(scaled * sine)
            inverse = lax.rsqrt(head_mean(values * values, small) + NORM_EPS)
            unit = values * inverse
            both = weighted * unit
            back = inverse * (weighted - unit * head_mean(both, small))
            return back.astype(BF16), jnp.sum(both, axis=0, keepdims=True)

        def leave_heads(m):
            @pl.loop(0, block_count)
            def _(block):
                rows = tile(block)
                cosine, sine = tabs[0, rows], tabs[1, rows]
                for group in range(2):
                    lanes = slice(128 * group, 128 * group + 128)
                    back, term = normalize_back(grad_q[group, rows], prj[rows, lanes], cosine, sine)
                    grad_qkv[m, rows, lanes] = back
                    gain_parts[2:3, 0:128] += term
                back, term = normalize_back(
                    jnp.where(front, grad_k[0, rows], grad_k[1, rows]),
                    prj[rows, 256:384],
                    tabs[2, rows],
                    tabs[3, rows],
                )
                grad_qkv[m, rows, 256:384] = back
                gain_parts[2:3, 128:256] += term
                grad_qkv[m, rows, 384:512] = jnp.where(
                    front, grad_v[0, rows], grad_v[1, rows]
                ).astype(BF16)

        def enter_norm(m):
            drain(1, m)

            @pl.loop(0, block_count)
            def _(step):
                rows = tile(block_of(step))
                hand_out(m, step, nt(grad_qkv[m, rows], qkv_w[:, 0:512]))
                send_twin(2, m, step)

            cross(2, m)

        def leave_attn(m):
            upstream = collect(2, m)
            back, term = norm_rows_back(toks[m].astype(F32), attn_gain[...], upstream)
            middle[m] = mid_all[m, own].astype(F32) + back
            gain_parts[0:1, :] += term

        def norm_copies():
            return [
                pltpu.make_async_copy(
                    normed.at[turn_block(step)], norm_cols.at[step % 2], local_sems.at[24 + step]
                )
                for step, norm_cols in enumerate((ky, ky, val, val))
            ]

        reloads = ((value, val), (key, ky), (query, qry), (proj, prj))

        def reload_copy(index):
            src, dst = reloads[index]
            return pltpu.make_async_copy(src.at[1], dst, local_sems.at[10 + index])

        def mixed_save(m):
            return pltpu.make_async_copy(mixed.at[m], out_mixed.at[m], local_sems.at[14 + m])

        def enter_back():
            @pl.loop(0, block_count)
            def _(step):
                block = turn_block(step)
                columns = tile(block)
                total = jnp.zeros((TILE, 256), F32)
                for m in range(micro_count):
                    heads = jnp.concatenate([att[m, 0], att[m, 1]], axis=1)
                    total = total + tn(mid_all[m, :, columns], heads)
                back_part[columns] = total.astype(BF16)

        def hidden_copy(index):
            m, rows = rows_of(index)
            slot = rem(index, block_count)
            return pltpu.make_async_copy(
                hidden.at[m, rows], hidden_buf.at[slot], local_sems.at[24 + slot]
            )

        def enter_out():
            drain(0, 0)

            @pl.loop(0, tile_count)
            def _(index):
                m = index // block_count
                step = rem(index, block_count)

                @pl.when(index == block_count)
                def _():
                    take(gate_s, 1)
                    issue(gate_s, 3)
                    leave_ffn(1)
                    drain(0, 1)

                hidden_copy(index).wait()
                hand_out(m, step, nt(hidden_buf[step], down_w[...]))
                send_twin(1, m, step)

                @pl.when(index + block_count < tile_count)
                def _():
                    hidden_copy(index + block_count).start()

        for slot in range(block_count):
            hidden_copy(slot).start()
        for copy in attn_copies():
            copy.wait()
        down_s.keep(down_total)
        mid_g[0].relay()
        enter_out()
        cross(1, 0)
        mid_g[0].finish()

        @pl.loop(0, micro_count)
        def _(m):
            score_ready(m)

            @pl.when(m == 1)
            def _():
                leave_out(0)
                mixed_save(0).start()
                enter_norm(0)
                take(up_s, 1)
                issue(up_s, 3)
                enter_back()

            def between(group):
                @pl.when((m == 0) & (group == 0))
                def _():
                    take(gate_s, 2)
                    issue(up_s, 0)

                @pl.when((m == 0) & (group == 1))
                def _():
                    gate_s.keep(gate_total)
                    issue(up_s, 1)
                    cross(1, 1)
                    mid_g[1].relay()

                @pl.when((m == 1) & (group == 0))
                def _():
                    take(up_s, 2)
                    issue(back_s, 0)
                    issue(back_s, 1)

                @pl.when((m == 1) & (group == 1))
                def _():
                    up_s.keep(up_total)
                    issue(back_s, 2)
                    issue(back_s, 3)

            attend_back(m, between)

            @pl.when(m == 0)
            def _():
                for index in range(3):
                    reload_copy(index).start()
                table_load.wait()

            @pl.when(m == 1)
            def _():
                for copy in norm_copies():
                    copy.start()

            leave_heads(m)

            @pl.when(m == 0)
            def _():
                reload_copy(3).start()
                take(up_s, 0)
                issue(up_s, 2)

            @pl.when(m == 0)
            def _():
                mid_g[1].finish()
                for index in range(4):
                    reload_copy(index).wait()

        for half, norm_cols in enumerate((ky, val)):

            @pl.loop(2 * half, 2 * half + 2)
            def _(step):
                slot = step - 2 * half
                pltpu.make_async_copy(
                    normed.at[turn_block(step)], norm_cols.at[slot], local_sems.at[24 + step]
                ).wait()
                qkv_part[tile(turn_block(step))] = (
                    tn(
                        norm_cols[slot].reshape(micro_count * length, TILE),
                        grad_qkv[...].reshape(micro_count * length, 512),
                    )
                ).astype(BF16)
                if outers == 1:
                    qkv_s.inner_copy(rem(step + 1, outer_size)).start()

        if outers > 1:
            for part in range(4):
                issue(qkv_s, part)
        leave_out(1)
        mixed_save(1).start()
        enter_norm(1)
        token_load.wait()
        saves = [mixed_save(m) for m in range(micro_count)]
        down_s.finish(down_total)
        saves.append(load(down_total, out_down))
        gate_s.finish(gate_total)
        saves.append(load(gate_total, out_gate))

        for part in range(3):
            take(back_s, part)
        leave_attn(0)
        saves.append(load(middle.at[0], out_tokens.at[0]))
        back_s.keep(back_total)
        for part in range(3):
            take(qkv_s, part)
        leave_attn(1)
        saves.append(load(middle.at[1], out_tokens.at[1]))

        def group_gain(shift):
            return place.copy(
                gain_packed,
                gain_group.at[shift - 1],
                (gain_send, gain_recv),
                shift - 1,
                tensor=rem(place.tensor + shift, 4),
            )

        pack_gains(gain_packed, gain_parts)
        for shift in range(1, 4):
            group_gain(shift).start()
        qkv_s.keep(qkv_total)
        up_s.finish(up_total)
        saves.append(load(up_total, out_up))
        back_s.finish(back_total)
        saves.append(load(back_total, out_back))
        for shift in range(1, 4):
            group_gain(shift).wait_recv()
        gain_dp[0] = gain_packed[...] + gain_group[0] + gain_group[1] + gain_group[2]

        def dp_gain(shift):
            return place.copy(
                gain_dp.at[0],
                gain_dp.at[shift],
                (gain_send, gain_recv),
                2 + shift,
                dp=rem(place.dp + shift, dp_size),
            )

        @pl.loop(1, dp_size)
        def _(shift):
            dp_gain(shift).start()

        qkv_s.finish(qkv_total)
        saves.append(load(qkv_total, out_qkv))
        gain_sums[...] = gain_dp[0]

        @pl.loop(1, dp_size)
        def _(shift):
            dp_gain(shift).wait_recv()
            gain_sums[...] += gain_dp[shift]

        for shift in range(1, 4):
            group_gain(shift).wait_send()

        @pl.loop(1, dp_size)
        def _(shift):
            dp_gain(shift).wait_send()

        qkv_s.drain()
        back_s.drain()
        for copy in saves:
            copy.wait()

    pl.run_scoped(
        attn_phase,
        pltpu.VMEM(tokens.shape, BF16),
        pltpu.VMEM(tables.shape, F32),
        pltpu.VMEM((block_count, TILE, hidden_width), BF16),
        pltpu.VMEM((2, length, 256), BF16),
        pltpu.VMEM((2, length, 128), F32),
        pltpu.VMEM((2, length, 128), F32),
        pltpu.VMEM((2, length, 128), F32),
        pltpu.VMEM((micro_count, length, 512), BF16),
        *[
            pltpu.VMEM((width // dp_size, w), F32)
            for w in (512, 256, hidden_width, hidden_width, hidden_width)
        ],
    )
    for share in (down_s, gate_s, up_s):
        share.drain()
    for m in range(micro_count):
        mid_g[m].drain()
        drain(2, m)


def backward(dp_size, cotangent, attn_gain, ffn_gain, tokens, saved):
    micro, rows, width = tokens.shape
    length = saved[7].shape[1]
    hidden_width = saved[2].shape[1]
    outer_size = dp_size // 2
    share = width // dp_size
    whole = pl.BlockSpec(memory_space=pltpu.VMEM)
    anywhere = pl.BlockSpec(memory_space=pl.ANY)
    shape = jax.ShapeDtypeStruct
    widths = (512, 256, hidden_width, hidden_width, hidden_width)
    out_shape = [
        shape((micro, rows, width), BF16),
        shape((micro, rows, width), F32),
        shape((8, 384), F32),
    ] + [shape((share, w), F32) for w in widths]
    scratch = (
        [pltpu.VMEM((micro, rows, width), BF16)]
        + [
            pltpu.VMEM((micro, length, width), BF16),
            pltpu.VMEM((256, 256), BF16),
            pltpu.VMEM((2, width, hidden_width), BF16),
            pltpu.VMEM((width, hidden_width), BF16),
            pltpu.VMEM((width, 768), BF16),
            pltpu.VMEM((micro, 2, length, 128), BF16),
            pltpu.VMEM((2, length, 256), BF16),
            pltpu.VMEM((2, 2, length, 256), BF16),
            pltpu.VMEM((2, 2, length, 256), BF16),
            pltpu.VMEM((length, 384), F32),
            pltpu.VMEM((outer_size, share, hidden_width), BF16),
            pltpu.VMEM((outer_size, share, 512), BF16),
            pltpu.VMEM((outer_size, share, 256), BF16),
            pltpu.VMEM((2, outer_size, share, hidden_width), BF16),
            pltpu.VMEM((outer_size, share, hidden_width), BF16),
            pltpu.VMEM((outer_size - 1, share, 512), BF16),
            pltpu.VMEM((outer_size - 1, share, 256), BF16),
            pltpu.VMEM((2, outer_size - 1, share, hidden_width), BF16),
            pltpu.VMEM((outer_size - 1, share, hidden_width), BF16),
            pltpu.VMEM((micro, 4, rows, width), BF16),
            pltpu.VMEM((micro, 2, rows, width), BF16),
            pltpu.VMEM((micro, rows, width), BF16),
            pltpu.VMEM((micro, 2, rows, width), BF16),
            pltpu.VMEM((micro, rows, width), BF16),
            pltpu.VMEM((micro, rows, width), F32),
            pltpu.VMEM((8, width), F32),
            pltpu.VMEM((8, 384), F32),
            pltpu.VMEM((3, 8, 384), F32),
            pltpu.VMEM((dp_size, 8, 384), F32),
        ]
        + [pltpu.SemaphoreType.DMA((5, outer_size))] * 4
        + [pltpu.SemaphoreType.DMA((24,))] * 2
        + [pltpu.SemaphoreType.DMA((dp_size + 2,))] * 2
        + [pltpu.SemaphoreType.DMA((40 + outer_size,)), pltpu.SemaphoreType.DMA((4, 2))]
    )
    return pl.pallas_call(
        functools.partial(backward_kernel, dp_size),
        out_shape=out_shape,
        in_specs=[anywhere, whole, whole] + [anywhere] * (1 + len(saved)),
        out_specs=[anywhere, anywhere, whole] + [anywhere] * 5,
        scratch_shapes=scratch,
        compiler_params=pltpu.CompilerParams(
            collective_id=1, has_side_effects=True, vmem_limit_bytes=VMEM_LIMIT
        ),
        name="backward_pass",
    )(cotangent, attn_gain, ffn_gain, tokens, *saved)


def deliver_kernel(
    turned,
    in_mixed,
    in_tokens,
    gains,
    query_gain,
    key_gain,
    in_qkv,
    in_back,
    in_gate,
    in_up,
    in_down,
    mixed,
    grad_tokens,
    attn_gain,
    ffn_gain,
    query_term,
    key_term,
    grad_query,
    grad_key,
    grad_value,
    grad_out,
    grad_gate,
    grad_up,
    grad_down,
    buf_mixed,
    buf_tokens,
    buf_gate,
    buf_up,
    buf_qkv,
    buf_back,
    buf_down,
    turned_out,
    turned_down,
    sems,
):
    flows = [
        (in_down, buf_down, ()),
        (in_back, buf_back, ()),
        (in_mixed, buf_mixed, ((buf_mixed, mixed),)),
        (in_tokens.at[0], buf_tokens.at[0], ((buf_tokens.at[0], grad_tokens.at[0]),)),
        (in_tokens.at[1], buf_tokens.at[1], ((buf_tokens.at[1], grad_tokens.at[1]),)),
        (in_gate, buf_gate, ((buf_gate, grad_gate),)),
        (in_up, buf_up, ((buf_up, grad_up),)),
        (
            in_qkv,
            buf_qkv,
            (
                (buf_qkv.at[:, 0:256], grad_query),
                (buf_qkv.at[:, 256:384], grad_key),
                (buf_qkv.at[:, 384:512], grad_value),
            ),
        ),
    ]
    arrivals = [
        pltpu.make_async_copy(src, buf, sems.at[0, index]) for index, (src, buf, _) in enumerate(flows)
    ]
    departures = []

    def depart(src, dst):
        copy = pltpu.make_async_copy(src, dst, sems.at[1, len(departures)])
        copy.start()
        departures.append(copy)

    for copy in arrivals:
        copy.start()
    part = 0
    for out in (attn_gain, ffn_gain):
        for start in range(0, out.shape[1], 128):
            out[:, start : start + 128] = gains[
                part // 3 : part // 3 + 1, 128 * (part % 3) : 128 * (part % 3) + 128
            ]
            part += 1
    for out, gain in ((query_term, query_gain), (key_term, key_gain)):
        term = gains[part // 3 : part // 3 + 1, 128 * (part % 3) : 128 * (part % 3) + 128]
        out[...] = term[:, :DH] / gain[...] + term[:, DH:] / gain[...]
        part += 1
    for index in range(2, len(flows)):
        arrivals[index].wait()
        for src, dst in flows[index][2]:
            depart(src, dst)
    for index, (buf, facing, dst) in enumerate(
        ((buf_down, turned_down, grad_down), (buf_back, turned_out, grad_out))
    ):
        arrivals[index].wait()
        if turned:
            depart(buf, dst)
        else:
            facing[...] = buf[...].T
            depart(facing, dst)
    for copy in departures:
        copy.wait()


def deliver(results, query_gain, key_gain):
    mixed, grad_tokens, gains, qkv, back, gate, up, down = results
    turned = qkv.shape[0] % 128 != 0
    whole = pl.BlockSpec(memory_space=pltpu.VMEM)
    anywhere = pl.BlockSpec(memory_space=pl.ANY)
    stored = pl.BlockSpec(memory_space=pltpu.HBM)
    shape = jax.ShapeDtypeStruct
    share, width = qkv.shape[0], mixed.shape[2]

    def facing(array):
        return array.shape if turned else array.shape[::-1]

    out_shape = [
        shape(mixed.shape, BF16),
        shape(grad_tokens.shape, F32),
        shape((1, width), F32),
        shape((1, width), F32),
        shape((1, DH), F32),
        shape((1, DH), F32),
        shape((share, 256), F32),
        shape((share, 128), F32),
        shape((share, 128), F32),
        shape(facing(back), F32),
        shape(gate.shape, F32),
        shape(up.shape, F32),
        shape(facing(down), F32),
    ]
    out = pl.pallas_call(
        functools.partial(deliver_kernel, turned),
        out_shape=out_shape,
        in_specs=[stored, stored] + [whole] * 3 + [stored] * 5,
        out_specs=[anywhere] * 2 + [whole] * 4 + [anywhere] * 7,
        scratch_shapes=[
            pltpu.VMEM(mixed.shape, BF16),
            pltpu.VMEM(grad_tokens.shape, F32),
            pltpu.VMEM(gate.shape, F32),
            pltpu.VMEM(up.shape, F32),
            pltpu.VMEM(qkv.shape, F32),
            pltpu.VMEM(back.shape, F32),
            pltpu.VMEM(down.shape, F32),
            pltpu.VMEM(facing(back), F32),
            pltpu.VMEM(facing(down), F32),
            pltpu.SemaphoreType.DMA((2, 16)),
        ],
        compiler_params=pltpu.CompilerParams(vmem_limit_bytes=VMEM_LIMIT),
        name="deliver_pass",
    )(mixed, grad_tokens, gains, query_gain, key_gain, qkv, back, gate, up, down)
    out = list(out)
    if turned:
        out[9], out[12] = out[9].T, out[12].T
    return out


def shards(
    dp_size,
    tokens,
    segment_ids,
    attn_gain,
    query_gain,
    key_gain,
    w_query,
    w_key,
    w_value,
    w_out,
    ffn_gain,
    w_gate,
    w_up,
    w_down,
    cotangent,
):
    own_tokens, own_cot = tokens[:, 0], cotangent[:, 0]
    attn_row, ffn_row = attn_gain[None], ffn_gain[None]
    saved = forward(
        dp_size,
        own_tokens,
        own_cot,
        segment_ids,
        (w_query, w_key, w_value, w_out, w_gate, w_up, w_down),
        (attn_row, ffn_row, query_gain[None], key_gain[None]),
    )
    results = backward(dp_size, own_cot, attn_row, ffn_row, own_tokens, saved)
    (
        mixed,
        grad_tokens,
        attn_term,
        ffn_term,
        query_term,
        key_term,
        grad_query,
        grad_key,
        grad_value,
        grad_out,
        grad_gate,
        grad_up,
        grad_down,
    ) = deliver(results, query_gain[None], key_gain[None])
    return (
        mixed[:, None],
        grad_tokens[:, None],
        attn_term[0],
        query_term[0],
        key_term[0],
        grad_query,
        grad_key,
        grad_value,
        grad_out,
        ffn_term[0],
        grad_gate,
        grad_up,
        grad_down,
    )


def solution(mesh):
    sequence = P(None, "dp", "tensor", None)
    rows = P("dp", "tensor")
    columns = P("tensor", "dp")
    return jax.shard_map(
        functools.partial(shards, mesh.shape["dp"]),
        mesh=mesh,
        in_specs=(sequence, P(None, "dp", None), P(), P(), P(), rows, rows, rows, columns, P(), rows, rows, columns, sequence),
        out_specs=(sequence, sequence, P(), P(), P(), rows, rows, rows, columns, P(), rows, rows, columns),
        check_vma=False,
    )
```
